32 devices in a mesh: dp: 8 (over z, x), fsdp: 4 (over y, core).
Axes of the slice: x: 2, y: 2, z: 4, core: 2. Of those that a mesh axis runs over, the one named last changes fastest.
Arguments:
- hidden: bfloat16 [16384, 1536], P(('dp', 'fsdp')), may hold values from -6 to 6
- cotangent: bfloat16 [16384, 1536], P(('dp', 'fsdp')), may hold values from -6 to 6
- lengths: int32 [32], P(('dp', 'fsdp')), may hold values from 1 to 512, 12288 in all
- norm_gain: bfloat16 [1536], P(('dp', 'fsdp')), may hold values from 0.5 to 1.5
- in_proj: bfloat16 [1536, 6400], P(('dp', 'fsdp')), may hold values from -0.15625 to 0.15625
- dt_proj: bfloat16 [1536, 48], P(('dp', 'fsdp')), may hold values from -0.15625 to 0.15625
- conv_weight: bfloat16 [4, 3328], P(None, ('dp', 'fsdp')), may hold values from -3 to 3
- conv_bias: bfloat16 [3328], P(('dp', 'fsdp')), may hold values from -3 to 3
- dt_bias: bfloat16 [48], replicated, may hold values from -6 to -3
- a_log: bfloat16 [48], replicated, may hold values from 0 to 2.5
- skip_gain: bfloat16 [48], replicated, may hold values from 0.5 to 1.5
- gate_gain: bfloat16 [3072], P(('dp', 'fsdp')), may hold values from 0.5 to 1.5
- out_proj: bfloat16 [3072, 1536], P(('dp', 'fsdp')), may hold values from -0.109375 to 0.109375
Outputs:
- output: bfloat16 [16384, 1536], P(('dp', 'fsdp'))
- input_grad: float32 [16384, 1536], P(('dp', 'fsdp'))
- grad_norm_gain: float32 [1536], P(('dp', 'fsdp'))
- grad_in_proj: float32 [1536, 6400], P(('dp', 'fsdp'))
- grad_dt_proj: float32 [1536, 48], P(('dp', 'fsdp'))
- grad_conv_weight: float32 [4, 3328], P(None, ('dp', 'fsdp'))
- grad_conv_bias: float32 [3328], P(('dp', 'fsdp'))
- grad_dt_bias: float32 [48], replicated
- grad_a_log: float32 [48], replicated
- grad_skip_gain: float32 [48], replicated
- grad_gate_gain: float32 [3072], P(('dp', 'fsdp'))
- grad_out_proj: float32 [3072, 1536], P(('dp', 'fsdp'))
The draws below stay inside these ranges and needn't reach their ends.
Inputs may be any that keep to these rules, and one draw needn't show every extreme that they name: `lengths`: each slot has 1 to 512 live tokens, the longest slot is full, and all slots hold 12288 live tokens together.
All inputs are finite; a program needn't handle non-finite values. No bound on the sum of `lengths` on one device may be relied on, other than what follows from the above.
Results may differ from the reference program's by a relative error of at most 0.0078.
Values may be sent and summed in bfloat16 or wider, within the bound.
A program may use at most 320 MiB of HBM per device.

```python
import math
from functools import partial
import jax
import jax.numpy as jnp
import numpy as np
from jax import lax

D = 1536
HEADS = 48
CONV = 4
SPAN = 256
SLOT = 512
INNER = 3072
XBC = 3328
IN_WIDTH = 6400
SEQS = 32
TOKENS = 16384


def with_spikes(array, stream_key, source, target, parts, factor):
    owner, partner = [(jnp.arange(array.shape[dim]) // (array.shape[dim] // parts)).reshape([-1 if axis == dim else 1 for axis in range(array.ndim)]) for dim in (source, target)]
    chosen = jax.random.permutation(stream_key, parts)[partner]
    strong = (owner == chosen) | (owner == (partner + parts // 2) % parts)
    return jnp.where(strong, factor * array, array)


def levels(stream_key, dims, shards, least, high):
    level = 1.0
    for position, blocks in shards:
        steps = jax.random.uniform(jax.random.fold_in(jax.random.fold_in(stream_key, 6), position), (blocks,), jnp.float32, least / len(shards), high / len(shards))
        level = level * jnp.repeat(jnp.exp(steps), dims[position] // blocks).reshape((-1,) + (1,) * (len(dims) - 1 - position))
    return level


def length_profile(count, total, reach, lean):
    weights = [(1 << 20) // math.isqrt(grade ** lean) + 1 for grade in range(2, count + 1)]
    spare, holding = total - reach - (count - 1), [1] * (count - 1)
    while spare > 0:
        free = [i for i in range(count - 1) if holding[i] < reach]
        pool, remaining = sum([weights[i] for i in free]), spare
        for i in free:
            more = min(reach - holding[i], max(1, remaining * weights[i] // pool), spare)
            holding[i] = holding[i] + more
            spare = spare - more
    return np.array([reach] + holding)


def uneven_parts(stream_key, amount, total, reach, lean):
    if amount == 2:
        one = jax.random.randint(stream_key, (), max(1, total - reach), min(reach, total - 1) + 1)
        return jnp.stack([one, total - one])
    sizes = jnp.asarray(length_profile(amount, total, reach, lean), jnp.int32)
    pairs = (amount - 1) // 2
    giver, receiver = sizes[1:1 + 2 * pairs:2], sizes[2:2 + 2 * pairs:2]
    room = jnp.minimum(giver - 1, reach - receiver)
    moved = jax.random.randint(jax.random.fold_in(stream_key, 1), (pairs,), 0, 1 << 20) % (room + 1)
    sizes = sizes.at[1:1 + 2 * pairs:2].set(giver - moved).at[2:2 + 2 * pairs:2].set(receiver + moved)
    return sizes[jax.random.permutation(jax.random.fold_in(stream_key, 2), amount)]


def gaussian(key, dims, scale, limit, shards=(), kind=jnp.bfloat16):
    drawn = scale * jax.random.normal(key, dims, jnp.float32)
    if shards:
        drawn = drawn * levels(key, dims, shards, -0.22, 0.18)
    return jnp.clip(drawn, -limit, limit).astype(kind)


def heavy_noise(stream_key, extent, deviation, reach, pieces, heavy, kind=jnp.bfloat16):
    array = deviation * jax.random.normal(stream_key, extent, jnp.float32)
    if pieces:
        array = array * levels(stream_key, extent, pieces, -0.22, 0.18)
    return jnp.clip(with_spikes(array, jax.random.fold_in(stream_key, 3), *heavy), -reach, reach).astype(kind)


def setup_inputs(seed: int = 0) -> dict:
    arg_keys = jax.random.split(jax.random.key(seed), 14)
    return {
        "hidden": heavy_noise(arg_keys[0], (TOKENS, D), 1.0, 6.0, ((0, 32),), (0, 1, 32, 2.75)),
        "cotangent": gaussian(arg_keys[1], (TOKENS, D), 1.0, 6.0, ((0, 32),)),
        "lengths": uneven_parts(arg_keys[2], SEQS, SEQS * SLOT * 3 // 4, SLOT, 2).astype(jnp.int32),
        "norm_gain": jnp.clip(1.0 + 0.1 * jax.random.normal(arg_keys[3], (D,), jnp.float32), 0.5, 1.5).astype(jnp.bfloat16),
        "in_proj": gaussian(arg_keys[4], (D, IN_WIDTH), D ** -0.5, 0.15625, ((0, 32),)),
        "dt_proj": gaussian(arg_keys[5], (D, HEADS), D ** -0.5, 0.15625, ((0, 32),)),
        "conv_weight": gaussian(arg_keys[6], (CONV, XBC), CONV ** -0.5, 3.0, ((1, 32),)),
        "conv_bias": gaussian(arg_keys[7], (XBC,), 0.5, 3.0, ((0, 32),)),
        "dt_bias": jnp.clip(jax.random.uniform(arg_keys[8], (HEADS,), jnp.float32, -6.0, -3.0), -6.0, -3.0).astype(jnp.bfloat16),
        "a_log": jnp.clip(jax.random.uniform(arg_keys[9], (HEADS,), jnp.float32, 0.0, 2.5), 0.0, 2.5).astype(jnp.bfloat16),
        "skip_gain": jnp.clip(jax.random.uniform(arg_keys[10], (HEADS,), jnp.float32, 0.5, 1.5), 0.5, 1.5).astype(jnp.bfloat16),
        "gate_gain": jnp.clip(1.0 + 0.1 * jax.random.normal(arg_keys[11], (INNER,), jnp.float32), 0.5, 1.5).astype(jnp.bfloat16),
        "out_proj": gaussian(arg_keys[12], (INNER, D), INNER ** -0.5, 0.109375, ((0, 32),)),
    }


highest = lax.Precision.HIGHEST
epsilon = 1e-05

def pre_norm(row_values, gain_values):
    inverse = lax.rsqrt(lax.optimization_barrier(jnp.mean(row_values * row_values, axis=1, keepdims=True)) + epsilon)
    return row_values * inverse * gain_values[None, :]

def state_space(values, step_size, log_decay, input_keys, read_keys, span_len):
    length, head_count, head_dim = values.shape
    blocks = length // span_len
    scaled = (values * step_size[:, :, None]).reshape(blocks, span_len, head_count, head_dim)
    scaled = jnp.transpose(scaled, (0, 2, 1, 3))
    decays = jnp.transpose(log_decay.reshape(blocks, span_len, head_count), (0, 2, 1))
    summed = jnp.cumsum(decays, axis=2)
    in_keys = input_keys.reshape(blocks, span_len, -1)
    out_keys = read_keys.reshape(blocks, span_len, -1)
    scores = jnp.einsum('kin,kjn->kij', out_keys, in_keys, precision=highest)
    causal = jnp.arange(span_len)[:, None] >= jnp.arange(span_len)[None, :]
    spread = summed[:, :, :, None] - summed[:, :, None, :]
    decay_matrix = jnp.where(causal, jnp.exp(jnp.where(causal, spread, 0.0)), 0.0)
    mixing = decay_matrix * scores[:, None, :, :]
    inner_part = jnp.einsum('khij,khjp->khip', mixing, scaled, precision=highest)
    ending = summed[:, :, -1]
    tail_decay = jnp.exp(ending[:, :, None] - summed)
    states = jnp.einsum('kjn,khjp->khpn', in_keys, scaled * tail_decay[:, :, :, None], precision=highest)

    def advance(carried, inputs):
        block_state, block_end = inputs
        return (jnp.exp(block_end)[:, None, None] * carried + block_state, carried)
    _, entering = lax.scan(advance, jnp.zeros(states.shape[1:], states.dtype), (states, ending))
    outer_part = jnp.einsum('kin,khpn->khip', out_keys, entering, precision=highest) * jnp.exp(summed)[:, :, :, None]
    result = jnp.transpose(inner_part + outer_part, (0, 2, 1, 3))
    return result.reshape(length, head_count, head_dim)

def mixer_block(projected, dt_raw, conv_w, conv_b, dt_shift, a_log, skip_gain, gate_gain, span_len):
    length = projected.shape[0]
    inner_width = gate_gain.shape[0]
    head_count = dt_shift.shape[0]
    state_dim = (projected.shape[1] - 2 * inner_width) // 2
    gate_part = projected[:, :inner_width]
    raw_part = projected[:, inner_width:]
    kernel = conv_w.shape[0]
    padded = jnp.pad(raw_part, ((kernel - 1, 0), (0, 0)))
    conv_out = conv_b[None, :] + conv_w[kernel - 1][None, :] * raw_part
    for offset in range(kernel - 1):
        conv_out = conv_out + conv_w[offset][None, :] * padded[offset:offset + length]
    active = jax.nn.silu(conv_out)
    values = active[:, :inner_width].reshape(length, head_count, inner_width // head_count)
    input_keys = active[:, inner_width:inner_width + state_dim]
    read_keys = active[:, inner_width + state_dim:]
    step_size = jax.nn.softplus(dt_raw + dt_shift[None, :])
    log_decay = -step_size * jnp.exp(a_log)[None, :]
    mixed_out = state_space(values, step_size, log_decay, input_keys, read_keys, span_len) + skip_gain[None, :, None] * values
    product = mixed_out.reshape(length, inner_width) * jax.nn.silu(gate_part)
    return pre_norm(product, gate_gain)

def row_dot(left, right):
    return lax.dot_general(left, right, (((0,), (0,)), ((), ())), preferred_element_type=jnp.float32)

def back_dot(left, weight):
    return lax.dot_general(left, weight, (((1,), (1,)), ((), ())), preferred_element_type=jnp.float32)

def reference(hidden, cotangent, lengths, norm_gain, in_proj, dt_proj, conv_weight, conv_bias, dt_bias, a_log, skip_gain, gate_gain, out_proj):
    gain_one = norm_gain.astype(jnp.float32)
    conv_taps = conv_weight.astype(jnp.float32)
    conv_shift = conv_bias.astype(jnp.float32)
    dt_shift = dt_bias.astype(jnp.float32)
    rates_log = a_log.astype(jnp.float32)
    skip_vals = skip_gain.astype(jnp.float32)
    gain_two = gate_gain.astype(jnp.float32)
    mixer_fn = partial(mixer_block, span_len=SPAN)

    def process(totals, item):
        row_values, cot_values, seq_len = item
        rows_wide = row_values.astype(jnp.float32)
        live = (jnp.arange(SLOT) < seq_len).astype(jnp.float32)
        normed_wide, norm_back = jax.vjp(pre_norm, rows_wide, gain_one)
        normed = normed_wide.astype(jnp.bfloat16)
        projected = jnp.dot(normed, in_proj, preferred_element_type=jnp.float32)
        dt_raw = jnp.dot(normed, dt_proj, preferred_element_type=jnp.float32)
        gated_wide, mixer_back = jax.vjp(mixer_fn, projected, dt_raw, conv_taps, conv_shift, dt_shift, rates_log, skip_vals, gain_two)
        gated = gated_wide.astype(jnp.bfloat16)
        branch = jnp.dot(gated, out_proj, preferred_element_type=jnp.float32)
        output = (rows_wide + live[:, None] * branch).astype(jnp.bfloat16)
        upstream = (cot_values.astype(jnp.float32) * live[:, None]).astype(jnp.bfloat16)
        grad_out = row_dot(gated, upstream)
        grad_gated = back_dot(upstream, out_proj)
        g_proj, g_dtraw, g_conv, g_convb, g_dtb, g_alog, g_skip, g_ggain = mixer_back(grad_gated)
        proj_low = g_proj.astype(jnp.bfloat16)
        dtraw_low = g_dtraw.astype(jnp.bfloat16)
        grad_in = row_dot(normed, proj_low)
        grad_dt = row_dot(normed, dtraw_low)
        grad_normed = back_dot(proj_low, in_proj) + back_dot(dtraw_low, dt_proj)
        grad_rows, grad_gain = norm_back(grad_normed)
        input_grad = cot_values.astype(jnp.float32) + grad_rows
        terms = (grad_gain, grad_in, grad_dt, g_conv, g_convb, g_dtb, g_alog, g_skip, g_ggain, grad_out)
        totals = tuple((left + right for left, right in zip(totals, terms)))
        return (totals, (output, input_grad))
    shapes = (norm_gain, in_proj, dt_proj, conv_weight, conv_bias, dt_bias, a_log, skip_gain, gate_gain, out_proj)
    start = tuple((jnp.zeros(entry.shape, jnp.float32) for entry in shapes))
    items = (hidden.reshape(SEQS, SLOT, D), cotangent.reshape(SEQS, SLOT, D), lengths)
    totals, (outputs, in_grads) = lax.scan(process, start, items)
    return (outputs.reshape(TOKENS, D), in_grads.reshape(TOKENS, D), totals[0], totals[1], totals[2], totals[3], totals[4], totals[5], totals[6], totals[7], totals[8], totals[9])
```

```python
from functools import partial

import jax
import jax.numpy as jnp
from jax import lax
from jax.experimental import pallas as pl
from jax.experimental.pallas import tpu as pltpu
from jax.sharding import PartitionSpec as P

f32 = jnp.float32
bf16 = jnp.bfloat16
epsilon = 1e-05
highest = lax.Precision.HIGHEST
BLK = 128
GH = 8
HD = 64
GC = GH * HD
KEY = 128
NEG = -1e30


def sigmoid(v):
    return 0.5 * jnp.tanh(0.5 * v) + 0.5


def mm(a, b):
    return lax.dot_general(a, b, (((1,), (0,)), ((), ())), preferred_element_type=f32)


def mm_nt(a, b):
    return lax.dot_general(a, b, (((1,), (1,)), ((), ())), preferred_element_type=f32)


def mm_tn(a, b):
    return lax.dot_general(a, b, (((0,), (0,)), ((), ())), preferred_element_type=f32)


def mm_hi(a, b, dims=((1,), (0,))):
    return lax.dot_general(a, b, (dims, ((), ())), preferred_element_type=f32, precision=highest)


def split(v):
    hi = v.astype(bf16)
    lo = (v - hi.astype(f32)).astype(bf16)
    return jnp.concatenate([hi, lo], axis=1)


def iota(shape, dim):
    return lax.broadcasted_iota(jnp.int32, shape, dim)


def expander(g):
    rows = iota((2 * KEY, GC), 0)
    cols = iota((2 * KEY, GC), 1)
    return jnp.where(lax.rem(rows, KEY) == cols // HD + g * GH, 1.0, 0.0).astype(bf16)


def reducer(g):
    rows = iota((GC, KEY), 0)
    cols = iota((GC, KEY), 1)
    return jnp.where(rows // HD + g * GH == cols, 1.0, 0.0).astype(bf16)


def taps_of(window, par, cols):
    out = par[4:5, cols] + par[3:4, cols] * window[8:136]
    for k in range(3):
        out = out + par[k : k + 1, cols] * window[5 + k : 133 + k]
    return out


def fwd_kernel(
    gate_ref, rawv_ref, rawk_ref, dtr_ref, pv_ref, pk_ref, ph_ref,
    y_ref, p_ref, hst_ref, r_ref, s_ref, st_ref, hl_ref, ehl_ref, kb_ref, kt_ref, sc_ref,
    pad, padk, sg, hcar, ssq,
):
    g = pl.program_id(0)
    length = gate_ref.shape[0]
    blocks = length // BLK
    inner = HD * GH * pl.num_programs(0)

    @pl.when(g == 0)
    def _():
        dt = jax.nn.softplus(dtr_ref[...] + ph_ref[0:1, :])
        la = -dt * jnp.exp(ph_ref[1:2, :])
        tri = jnp.where(iota((BLK, BLK), 0) >= iota((BLK, BLK), 1), 1.0, 0.0).astype(f32)
        hl_ref[0] = split(dt)
        ehl_ref[...] = jnp.zeros_like(ehl_ref)
        for k in range(blocks):
            rows = slice(k * BLK, (k + 1) * BLK)
            s = mm_hi(tri, la[rows])
            s_ref[rows] = s
            st_ref[:, rows] = s.T
            hl_ref[1, rows] = split(jnp.exp(s))
            hl_ref[2, rows] = split(jnp.exp(s[BLK - 1 :] - s))
            ehl_ref[k : k + 1] = split(jnp.exp(s[BLK - 1 :]))
        padk[0:8] = jnp.zeros((8, 2 * KEY), f32)
        padk[8:] = rawk_ref[...]
        pad[0:8] = jnp.zeros((8, GC), f32)
        for k in range(blocks):
            rows = slice(k * BLK, (k + 1) * BLK)
            u = taps_of(padk[k * BLK : k * BLK + BLK + 8], pk_ref, slice(0, 2 * KEY))
            v = u * sigmoid(u)
            kb_ref[rows] = v.astype(bf16)
            kt_ref[:, rows] = v.T.astype(bf16)
            sc_ref[k] = mm_hi(v[:, KEY:], v[:, :KEY], ((1,), (1,)))
        ssq[...] = jnp.zeros_like(ssq)

    pad[8:] = rawv_ref[...]
    sg[...] = pltpu.roll(s_ref[...], lax.rem(KEY - g * GH, KEY), 1)
    ex = expander(g)
    bias = jnp.where(iota((BLK, BLK), 0) >= iota((BLK, BLK), 1), 0.0, NEG).astype(f32)
    low = iota((BLK, KEY), 1) < HD
    eend = mm(ehl_ref[...], ex)
    hcar[...] = jnp.zeros_like(hcar)
    for k in range(blocks):
        rows = slice(k * BLK, (k + 1) * BLK)
        dtx = mm(hl_ref[0, rows], ex)
        exx = mm(hl_ref[1, rows], ex)
        txx = mm(hl_ref[2, rows], ex)
        hb = hcar[...].astype(bf16)
        hst_ref[k] = hb
        outer = mm(kb_ref[rows, KEY:], hb)
        across = st_ref[pl.ds(pl.multiple_of(g * GH, GH), GH), rows]
        xts = []
        for q in range(GC // KEY):
            cols = slice(q * KEY, (q + 1) * KEY)
            u = taps_of(pad[k * BLK : k * BLK + BLK + 8, cols], pv_ref, cols)
            v = u * sigmoid(u)
            x = v * dtx[:, cols]
            xts.append((x * txx[:, cols]).astype(bf16))
            xb = x.astype(bf16)
            zero = jnp.zeros_like(xb)
            x2 = jnp.concatenate([jnp.where(low, xb, zero), jnp.where(low, zero, xb)], axis=0)
            ms = []
            for half in range(2):
                j = 2 * q + half
                spread = sg[rows, j : j + 1] - across[j : j + 1]
                ms.append((jnp.exp(spread + bias) * sc_ref[k]).astype(bf16))
            y = mm(jnp.concatenate(ms, axis=1), x2)
            y = y + outer[:, cols] * exx[:, cols] + pv_ref[6:7, cols] * v
            y_ref[rows, cols] = y
            gate = gate_ref[rows, cols]
            p = y * (gate * sigmoid(gate))
            p_ref[rows, cols] = p
            ssq[rows] += p * p
        if k + 1 < blocks:
            hcar[...] = eend[k : k + 1] * hcar[...] + mm(kt_ref[:KEY, rows], jnp.concatenate(xts, axis=1))

    @pl.when(g == pl.num_programs(0) - 1)
    def _():
        mean = jnp.sum(ssq[...], axis=1, keepdims=True) / inner
        r_ref[...] = jnp.broadcast_to(lax.rsqrt(mean + epsilon), r_ref.shape)


def bwd_kernel(
    gate_ref, rawv_ref, rawk_ref, dtr_ref, pv_ref, pk_ref, ph_ref,
    y_ref, gg_ref, hst_ref, r_ref, c_ref, s_ref, st_ref, hl_ref, ehl_ref, kb_ref, kt_ref, sc_ref,
    dproj_ref, sv_ref, sk_ref, sh_ref,
    pad, padk, dpad, dpadk, sg, dhcar, dsc, dkb, dsrow, dscol, ddt,
):
    g = pl.program_id(0)
    length = gate_ref.shape[0]
    blocks = length // BLK
    groups = gate_ref.shape[1] // GC
    inner = dproj_ref.shape[1] // 2 - 3 * KEY // 2
    groups = pl.num_programs(0)

    @pl.when(g == 0)
    def _():
        pad[0:8] = jnp.zeros((8, GC), f32)
        padk[0:8] = jnp.zeros((8, 2 * KEY), f32)
        padk[8:] = rawk_ref[...]
        dpad[length:] = jnp.zeros((8, GC), f32)
        dpadk[length:] = jnp.zeros((8, 2 * KEY), f32)
        dsc[...] = jnp.zeros_like(dsc)
        dkb[...] = jnp.zeros_like(dkb)
        dsrow[...] = jnp.zeros_like(dsrow)
        dscol[...] = jnp.zeros_like(dscol)
        ddt[...] = jnp.zeros_like(ddt)

    pad[8:] = rawv_ref[...]
    sg[...] = pltpu.roll(s_ref[...], lax.rem(KEY - g * GH, KEY), 1)
    ex = expander(g)
    red = reducer(g)
    row = iota((BLK, BLK), 0)
    col = iota((BLK, BLK), 1)
    bias = jnp.where(row >= col, 0.0, NEG).astype(f32)
    strict = row > col
    low = iota((BLK, KEY), 1) < HD
    eend = mm(ehl_ref[...], ex)
    dhcar[...] = jnp.zeros_like(dhcar)
    sv_ref[...] = jnp.zeros_like(sv_ref)
    for k in range(blocks - 1, -1, -1):
        rows = slice(k * BLK, (k + 1) * BLK)
        dtx = mm(hl_ref[0, rows], ex)
        exx = mm(hl_ref[1, rows], ex)
        txx = mm(hl_ref[2, rows], ex)
        hb = hst_ref[k]
        dhb = dhcar[...].astype(bf16)
        ch = mm(kb_ref[rows, KEY:], hb)
        qq = mm(kb_ref[rows, :KEY], dhb)
        across = st_ref[pl.ds(pl.multiple_of(g * GH, GH), GH), rows]
        dyes, xts, zs, oys, ddts, ecols = [], [], [], [], [], []
        dsrow_k = jnp.zeros((BLK, KEY), f32)
        for q in range(GC // KEY):
            cols = slice(q * KEY, (q + 1) * KEY)
            window = pad[k * BLK : k * BLK + BLK + 8, cols]
            u = taps_of(window, pv_ref, cols)
            su = sigmoid(u)
            v = u * su
            x = v * dtx[:, cols]
            xb = x.astype(bf16)
            gate = gate_ref[rows, cols]
            y = y_ref[rows, cols]
            gg = gg_ref[rows, cols]
            sgt = sigmoid(gate)
            silu_g = gate * sgt
            p = y * silu_g
            r = r_ref[rows]
            dgn = gg * r
            sv_ref[5:6, cols] += jnp.sum(dgn * p, axis=0, keepdims=True)
            dp = dgn * pv_ref[5:6, cols] - p * c_ref[rows]
            dgate = dp * y * (sgt + silu_g * (1.0 - sgt))
            off = pl.multiple_of(g * GC + q * KEY, KEY)
            dproj_ref[rows, pl.ds(off, KEY)] = dgate.astype(bf16)
            dy = dp * silu_g
            sv_ref[6:7, cols] += jnp.sum(dy * v, axis=0, keepdims=True)
            dyb = dy.astype(bf16)
            dye = dy * exx[:, cols]
            dyes.append(dye.astype(bf16))
            oys.append((dye * ch[:, cols]).astype(bf16))
            xt = x * txx[:, cols]
            xts.append(xt.astype(bf16))
            zs.append((xt * qq[:, cols]).astype(bf16))
            zero = jnp.zeros_like(dyb)
            dy2 = jnp.concatenate([jnp.where(low, dyb, zero), jnp.where(low, zero, dyb)], axis=0)
            dm2 = mm_nt(dy2, xb)
            ms = []
            for half in range(2):
                j = 2 * q + half
                spread = sg[rows, j : j + 1] - across[j : j + 1]
                decay = jnp.exp(spread + bias)
                m = decay * sc_ref[k]
                ms.append(m.astype(bf16))
                dm = dm2[half * BLK : (half + 1) * BLK]
                dsc[k] += decay * dm
                e = jnp.where(strict, m * dm, 0.0)
                dsrow_k = jnp.where(col == g * GH + j, jnp.sum(e, axis=1, keepdims=True), dsrow_k)
                ecols.append(jnp.sum(e, axis=0, keepdims=True))
            dx = mm_tn(jnp.concatenate(ms, axis=0), dy2) + qq[:, cols] * txx[:, cols]
            dv = dx * dtx[:, cols] + pv_ref[6:7, cols] * dy
            ddts.append((dx * v).astype(bf16))
            du = dv * (su + v * (1.0 - su))
            dpad[rows, cols] = du
            sv_ref[4:5, cols] += jnp.sum(du, axis=0, keepdims=True)
            for t in range(4):
                sv_ref[t : t + 1, cols] += jnp.sum(du * window[5 + t : 133 + t], axis=0, keepdims=True)
        dscol[pl.ds(pl.multiple_of(g * GH, GH), GH), rows] = jnp.concatenate(ecols, axis=0)
        dye = jnp.concatenate(dyes, axis=1)
        xt = jnp.concatenate(xts, axis=1)
        zsum = mm(jnp.concatenate(zs, axis=1), red)
        ddt[rows] += mm(jnp.concatenate(ddts, axis=1), red)
        hterm = eend[k : k + 1] * jnp.sum(dhcar[...] * hb.astype(f32), axis=0, keepdims=True)
        end = jnp.sum(zsum, axis=0, keepdims=True) + mm_hi(hterm, red.astype(f32))
        add = dsrow_k + mm(jnp.concatenate(oys, axis=1), red) - zsum
        dsrow[rows] += add + jnp.where(row == BLK - 1, end, 0.0)
        dkb[rows, KEY:] += mm_nt(dye, hb)
        dkb[rows, :KEY] += mm_nt(xt, dhb)
        if k:
            dhcar[...] = eend[k : k + 1] * dhcar[...] + mm(kt_ref[KEY:, rows], dye)

    inner_off = groups * GC
    for k in range(blocks):
        rows = slice(k * BLK, (k + 1) * BLK)
        for q in range(GC // KEY):
            cols = slice(q * KEY, (q + 1) * KEY)
            window = dpad[k * BLK : k * BLK + BLK + 8, cols]
            out = pv_ref[3:4, cols] * window[0:BLK]
            for t in range(3):
                out = out + pv_ref[t : t + 1, cols] * window[3 - t : 3 - t + BLK]
            off = pl.multiple_of(inner_off + g * GC + q * KEY, KEY)
            dproj_ref[rows, pl.ds(off, KEY)] = out.astype(bf16)

    @pl.when(g == groups - 1)
    def _():
        keys = dproj_ref.shape[1] - 3 * KEY
        sk_ref[...] = jnp.zeros_like(sk_ref)
        sh_ref[...] = jnp.zeros_like(sh_ref)
        upper = jnp.where(row <= col, 1.0, 0.0).astype(f32)
        for k in range(blocks):
            rows = slice(k * BLK, (k + 1) * BLK)
            window = padk[k * BLK : k * BLK + BLK + 8]
            u = taps_of(window, pk_ref, slice(0, 2 * KEY))
            su = sigmoid(u)
            ds = dsc[k].astype(bf16)
            db = dkb[rows, :KEY] + mm_tn(ds, kb_ref[rows, KEY:])
            dc = dkb[rows, KEY:] + mm(ds, kb_ref[rows, :KEY])
            du = jnp.concatenate([db, dc], axis=1) * (su + u * su * (1.0 - su))
            dpadk[rows] = du
            sk_ref[4:5] += jnp.sum(du, axis=0, keepdims=True)
            for t in range(4):
                sk_ref[t : t + 1] += jnp.sum(du * window[5 + t : 133 + t], axis=0, keepdims=True)
            dla = mm_hi(upper, dsrow[rows] - dscol[:, rows].T)
            z = dtr_ref[rows] + ph_ref[0:1, :]
            rate = jnp.exp(ph_ref[1:2, :])
            dt = jax.nn.softplus(z)
            sh_ref[1:2] += jnp.sum(dla * (-dt * rate), axis=0, keepdims=True)
            dz = (ddt[rows] - dla * rate) * sigmoid(z)
            sh_ref[0:1] += jnp.sum(dz, axis=0, keepdims=True)
            dproj_ref[rows, keys + 2 * KEY :] = dz.astype(bf16)
        for k in range(blocks):
            rows = slice(k * BLK, (k + 1) * BLK)
            window = dpadk[k * BLK : k * BLK + BLK + 8]
            out = pk_ref[3:4] * window[0:BLK]
            for t in range(3):
                out = out + pk_ref[t : t + 1] * window[3 - t : 3 - t + BLK]
            dproj_ref[rows, keys : keys + 2 * KEY] = out.astype(bf16)


def whole_spec(shape):
    return pl.BlockSpec(shape, lambda g: (0,) * len(shape))


def state_specs(length):
    return (
        ((length, KEY), f32),
        ((KEY, length), f32),
        ((3, length, 2 * KEY), bf16),
        ((8, 2 * KEY), bf16),
        ((length, 2 * KEY), bf16),
        ((2 * KEY, length), bf16),
        ((length // BLK, BLK, BLK), f32),
    )


def proj_specs(length, groups):
    wide = groups * GC
    return [
        pl.BlockSpec((length, GC), lambda g: (0, g)),
        pl.BlockSpec((length, GC), lambda g: (0, groups + g)),
        pl.BlockSpec((length, 2 * KEY), lambda g: (0, 2 * wide // (2 * KEY))),
        pl.BlockSpec((length, KEY), lambda g: (0, 2 * wide // KEY + 2)),
        pl.BlockSpec((8, GC), lambda g: (0, g)),
        whole_spec((8, 2 * KEY)),
        whole_spec((8, KEY)),
    ]


def mixer_forward(projected, pv, pk, ph):
    length = projected.shape[0]
    wide = pv.shape[1]
    groups = wide // GC
    blocks = length // BLK
    column = pl.BlockSpec((length, GC), lambda g: (0, g))
    shared = state_specs(length)
    return pl.pallas_call(
        fwd_kernel,
        grid=(groups,),
        in_specs=proj_specs(length, groups),
        out_specs=[
            column,
            column,
            pl.BlockSpec((blocks, KEY, GC), lambda g: (0, 0, g)),
            whole_spec((length, KEY)),
        ]
        + [whole_spec(shape) for shape, _ in shared],
        out_shape=[
            jax.ShapeDtypeStruct((length, wide), f32),
            jax.ShapeDtypeStruct((length, wide), f32),
            jax.ShapeDtypeStruct((blocks, KEY, wide), bf16),
            jax.ShapeDtypeStruct((length, KEY), f32),
        ]
        + [jax.ShapeDtypeStruct(shape, dtype) for shape, dtype in shared],
        scratch_shapes=[
            pltpu.VMEM((length + 8, GC), f32),
            pltpu.VMEM((length + 8, 2 * KEY), f32),
            pltpu.VMEM((length, KEY), f32),
            pltpu.VMEM((KEY, GC), f32),
            pltpu.VMEM((length, KEY), f32),
        ],
        name="mixer_forward",
    )(projected, projected, projected, projected, pv, pk, ph)


def mixer_backward(projected, pv, pk, ph, mixed, grad_gated, states, inverse, pull, shared):
    length, total = projected.shape
    wide = pv.shape[1]
    groups = wide // GC
    blocks = length // BLK
    column = pl.BlockSpec((length, GC), lambda g: (0, g))
    return pl.pallas_call(
        bwd_kernel,
        grid=(groups,),
        in_specs=proj_specs(length, groups)
        + [
            column,
            column,
            pl.BlockSpec((blocks, KEY, GC), lambda g: (0, 0, g)),
            whole_spec((length, KEY)),
            whole_spec((length, KEY)),
        ]
        + [whole_spec(shape) for shape, _ in state_specs(length)],
        out_specs=[
            whole_spec((length, total)),
            pl.BlockSpec((8, GC), lambda g: (0, g)),
            whole_spec((8, 2 * KEY)),
            whole_spec((8, KEY)),
        ],
        out_shape=[
            jax.ShapeDtypeStruct((length, total), bf16),
            jax.ShapeDtypeStruct((8, wide), f32),
            jax.ShapeDtypeStruct((8, 2 * KEY), f32),
            jax.ShapeDtypeStruct((8, KEY), f32),
        ],
        scratch_shapes=[
            pltpu.VMEM((length + 8, GC), f32),
            pltpu.VMEM((length + 8, 2 * KEY), f32),
            pltpu.VMEM((length + 8, GC), f32),
            pltpu.VMEM((length + 8, 2 * KEY), f32),
            pltpu.VMEM((length, KEY), f32),
            pltpu.VMEM((KEY, GC), f32),
            pltpu.VMEM((blocks, BLK, BLK), f32),
            pltpu.VMEM((length, 2 * KEY), f32),
            pltpu.VMEM((length, KEY), f32),
            pltpu.VMEM((KEY, length), f32),
            pltpu.VMEM((length, KEY), f32),
        ],
        name="mixer_backward",
    )(
        projected, projected, projected, projected, pv, pk, ph,
        mixed, grad_gated, states, inverse, pull, *shared,
    )


def pre_norm_inverse(rows):
    return lax.rsqrt(jnp.mean(rows * rows, axis=1, keepdims=True) + epsilon)


AXES = ("dp", "fsdp")
HEAD_LANES = KEY


def gather_rows(shard):
    return lax.all_gather(shard, AXES, axis=0, tiled=True)


def scatter_rows(whole):
    return lax.psum_scatter(whole, AXES, scatter_dimension=0, tiled=True)


def pack_columns(parts, rows, width):
    flat = jnp.concatenate([part.reshape(-1) for part in parts])
    return jnp.pad(flat, (0, rows * width - flat.shape[0])).reshape(rows, width)


def shards(
    hidden, cotangent, lengths, norm_gain, in_proj, dt_proj, conv_weight, conv_bias,
    dt_bias, a_log, skip_gain, gate_gain, out_proj,
):
    length, width = hidden.shape
    assert lengths.shape[0] == 1
    rows_in, columns = in_proj.shape
    heads = dt_bias.shape[0]
    parts = width // rows_in
    taps, conv_part = conv_weight.shape
    gate_part = gate_gain.shape[0]
    wide = gate_part * parts
    small_count = rows_in + taps * conv_part + conv_part + gate_part
    small_width = -(-small_count // (rows_in * 8)) * 8
    total = columns + KEY
    small_at = columns + heads

    small = pack_columns((norm_gain, conv_weight, conv_bias, gate_gain), rows_in, small_width)
    fill = jnp.zeros((rows_in, total - small_at - small_width), bf16)
    packed = jnp.concatenate([in_proj, dt_proj, small, fill], axis=1)
    w_in = gather_rows(packed)
    w_out = gather_rows(out_proj)
    small_all = w_in[:, small_at : small_at + small_width].astype(f32).reshape(parts, -1)
    ends = [rows_in, rows_in + taps * conv_part, small_count - gate_part, small_count]
    gain_one = small_all[:, : ends[0]].reshape(-1)
    conv_taps = jnp.transpose(small_all[:, ends[0] : ends[1]].reshape(parts, taps, conv_part), (1, 0, 2))
    conv_taps = conv_taps.reshape(taps, parts * conv_part)
    conv_shift = small_all[:, ends[1] : ends[2]].reshape(1, -1)
    gain_two = small_all[:, ends[2] : ends[3]].reshape(1, -1)

    rows_wide = hidden.astype(f32)
    live = (jnp.arange(length) < lengths[0]).astype(f32)[:, None]
    inverse_one = pre_norm_inverse(rows_wide)
    normed = (rows_wide * inverse_one * gain_one[None, :]).astype(bf16)
    projected = mm(normed, w_in)

    skip_wide = jnp.repeat(skip_gain.astype(f32), HD)[None]
    pv = jnp.concatenate(
        [conv_taps[:, :wide], conv_shift[:, :wide], gain_two, skip_wide, jnp.zeros((1, wide), f32)], axis=0
    )
    pk = jnp.concatenate([conv_taps[:, wide:], conv_shift[:, wide:], jnp.zeros((3, 2 * KEY), f32)], axis=0)
    ph = jnp.pad(jnp.stack([dt_bias, a_log]).astype(f32), ((0, 6), (0, KEY - heads)))
    mixed, product, states, inverse_two, *shared = mixer_forward(projected, pv, pk, ph)
    inv = inverse_two[:, :1]
    gated = (product * inv * gain_two).astype(bf16)
    output = (rows_wide + live * mm(gated, w_out)).astype(bf16)

    cot_wide = cotangent.astype(f32)
    upstream = (cot_wide * live).astype(bf16)
    grad_gated = mm_nt(upstream, w_out)
    pull = jnp.sum(grad_gated * gain_two * product, axis=1, keepdims=True)
    pull = jnp.broadcast_to(inv * inv * inv * pull / wide, inverse_two.shape)
    grad_proj, sums_v, sums_k, sums_h = mixer_backward(
        projected, pv, pk, ph, mixed, grad_gated, states, inverse_two, pull, shared
    )
    head_sums = lax.psum(
        jnp.concatenate([sums_h[:2, :heads], jnp.sum(sums_v[6].reshape(heads, HD), axis=1)[None]], axis=0), AXES
    )

    grad_normed = mm_nt(grad_proj, w_in)
    scaled = grad_normed * gain_one[None, :]
    dots = jnp.sum(scaled * rows_wide, axis=1, keepdims=True) / width
    grad_rows = inverse_one * scaled - rows_wide * (inverse_one * inverse_one * inverse_one * dots)
    input_grad = cot_wide + grad_rows
    grad_gain_one = jnp.sum(grad_normed * rows_wide * inverse_one, axis=0)

    conv_grad = jnp.concatenate([sums_v[:5], sums_k[:5]], axis=1)
    small_grad = jnp.concatenate(
        [
            grad_gain_one.reshape(parts, rows_in),
            jnp.transpose(conv_grad[:taps].reshape(taps, parts, conv_part), (1, 0, 2)).reshape(parts, -1),
            conv_grad[taps].reshape(parts, conv_part),
            sums_v[5].reshape(parts, gate_part),
            jnp.zeros((parts, rows_in * small_width - small_count), f32),
        ],
        axis=1,
    ).reshape(width, small_width)

    grad_out = scatter_rows(mm_tn(gated, upstream).astype(bf16)).astype(f32)
    grad_in = mm_tn(normed, grad_proj).astype(bf16)
    grad_in = lax.dynamic_update_slice(grad_in, small_grad.astype(bf16), (0, small_at))
    grad_in = scatter_rows(grad_in).astype(f32)
    small_sum = grad_in[:, small_at : small_at + small_width].reshape(-1)
    return (
        output,
        input_grad,
        small_sum[: ends[0]],
        grad_in[:, :columns],
        grad_in[:, columns:small_at],
        small_sum[ends[0] : ends[1]].reshape(taps, conv_part),
        small_sum[ends[1] : ends[2]],
        head_sums[0],
        head_sums[1],
        head_sums[2],
        small_sum[ends[2] : ends[3]],
        grad_out,
    )


def solution(mesh):
    rows = P(AXES, None)
    vector = P(AXES)
    last = P(None, AXES)
    return jax.shard_map(
        shards,
        mesh=mesh,
        in_specs=(rows, rows, vector, vector, rows, rows, last, vector, P(), P(), P(), vector, rows),
        out_specs=(rows, rows, vector, rows, rows, last, vector, P(), P(), P(), vector, rows),
        check_vma=False,
    )
```

```python
from functools import partial

import jax
import jax.numpy as jnp
from jax import lax
from jax.experimental import pallas as pl
from jax.experimental.pallas import tpu as pltpu
from jax.sharding import PartitionSpec as P

f32 = jnp.float32
bf16 = jnp.bfloat16
epsilon = 1e-05
highest = lax.Precision.HIGHEST
BLK = 128
GH = 8
HD = 64
GC = GH * HD
KEY = 128
NEG = -1e30


def sigmoid(v):
    return 0.5 * jnp.tanh(0.5 * v) + 0.5


def mm(a, b):
    return lax.dot_general(a, b, (((1,), (0,)), ((), ())), preferred_element_type=f32)


def mm_nt(a, b):
    return lax.dot_general(a, b, (((1,), (1,)), ((), ())), preferred_element_type=f32)


def mm_tn(a, b):
    return lax.dot_general(a, b, (((0,), (0,)), ((), ())), preferred_element_type=f32)


def mm_hi(a, b, dims=((1,), (0,))):
    return lax.dot_general(a, b, (dims, ((), ())), preferred_element_type=f32, precision=highest)


def split(v):
    hi = v.astype(bf16)
    lo = (v - hi.astype(f32)).astype(bf16)
    return jnp.concatenate([hi, lo], axis=1)


def iota(shape, dim):
    return lax.broadcasted_iota(jnp.int32, shape, dim)


def expander(g):
    rows = iota((2 * KEY, GC), 0)
    cols = iota((2 * KEY, GC), 1)
    return jnp.where(lax.rem(rows, KEY) == cols // HD + g * GH, 1.0, 0.0).astype(bf16)


def reducer(g):
    rows = iota((GC, KEY), 0)
    cols = iota((GC, KEY), 1)
    return jnp.where(rows // HD + g * GH == cols, 1.0, 0.0).astype(bf16)


def taps_of(window, par, cols):
    out = par[4:5, cols] + par[3:4, cols] * window[8:136]
    for k in range(3):
        out = out + par[k : k + 1, cols] * window[5 + k : 133 + k]
    return out


def fwd_kernel(
    gate_ref, rawv_ref, rawk_ref, dtr_ref, pv_ref, pk_ref, ph_ref,
    y_ref, p_ref, hst_ref, r_ref, s_ref, st_ref, hl_ref, ehl_ref, kb_ref, kt_ref, sc_ref,
    pad, padk, sg, hcar, ssq,
):
    g = pl.program_id(0)
    length = gate_ref.shape[0]
    blocks = length // BLK
    inner = HD * GH * pl.num_programs(0)

    @pl.when(g == 0)
    def _():
        dt = jax.nn.softplus(dtr_ref[...] + ph_ref[0:1, :])
        la = -dt * jnp.exp(ph_ref[1:2, :])
        tri = jnp.where(iota((BLK, BLK), 0) >= iota((BLK, BLK), 1), 1.0, 0.0).astype(f32)
        hl_ref[0] = split(dt)
        ehl_ref[...] = jnp.zeros_like(ehl_ref)
        for k in range(blocks):
            rows = slice(k * BLK, (k + 1) * BLK)
            s = mm_hi(tri, la[rows])
            s_ref[rows] = s
            st_ref[:, rows] = s.T
            hl_ref[1, rows] = split(jnp.exp(s))
            hl_ref[2, rows] = split(jnp.exp(s[BLK - 1 :] - s))
            ehl_ref[k : k + 1] = split(jnp.exp(s[BLK - 1 :]))
        padk[0:8] = jnp.zeros((8, 2 * KEY), f32)
        padk[8:] = rawk_ref[...]
        pad[0:8] = jnp.zeros((8, GC), f32)
        for k in range(blocks):
            rows = slice(k * BLK, (k + 1) * BLK)
            u = taps_of(padk[k * BLK : k * BLK + BLK + 8], pk_ref, slice(0, 2 * KEY))
            v = u * sigmoid(u)
            kb_ref[rows] = v.astype(bf16)
            kt_ref[:, rows] = v.T.astype(bf16)
            sc_ref[k] = mm_hi(v[:, KEY:], v[:, :KEY], ((1,), (1,)))
        ssq[...] = jnp.zeros_like(ssq)

    pad[8:] = rawv_ref[...]
    sg[...] = pltpu.roll(s_ref[...], lax.rem(KEY - g * GH, KEY), 1)
    ex = expander(g)
    bias = jnp.where(iota((BLK, BLK), 0) >= iota((BLK, BLK), 1), 0.0, NEG).astype(f32)
    low = iota((BLK, KEY), 1) < HD
    eend = mm(ehl_ref[...], ex)
    hcar[...] = jnp.zeros_like(hcar)
    for k in range(blocks):
        rows = slice(k * BLK, (k + 1) * BLK)
        dtx = mm(hl_ref[0, rows], ex)
        exx = mm(hl_ref[1, rows], ex)
        txx = mm(hl_ref[2, rows], ex)
        hb = hcar[...].astype(bf16)
        hst_ref[k] = hb
        outer = mm(kb_ref[rows, KEY:], hb)
        across = st_ref[pl.ds(pl.multiple_of(g * GH, GH), GH), rows]
        xts = []
        for q in range(GC // KEY):
            cols = slice(q * KEY, (q + 1) * KEY)
            u = taps_of(pad[k * BLK : k * BLK + BLK + 8, cols], pv_ref, cols)
            v = u * sigmoid(u)
            x = v * dtx[:, cols]
            xts.append((x * txx[:, cols]).astype(bf16))
            xb = x.astype(bf16)
            zero = jnp.zeros_like(xb)
            x2 = jnp.concatenate([jnp.where(low, xb, zero), jnp.where(low, zero, xb)], axis=0)
            ms = []
            for half in range(2):
                j = 2 * q + half
                spread = sg[rows, j : j + 1] - across[j : j + 1]
                ms.append((jnp.exp(spread + bias) * sc_ref[k]).astype(bf16))
            y = mm(jnp.concatenate(ms, axis=1), x2)
            y = y + outer[:, cols] * exx[:, cols] + pv_ref[6:7, cols] * v
            y_ref[rows, cols] = y
            gate = gate_ref[rows, cols]
            p = y * (gate * sigmoid(gate))
            p_ref[rows, cols] = p
            ssq[rows] += p * p
        if k + 1 < blocks:
            hcar[...] = eend[k : k + 1] * hcar[...] + mm(kt_ref[:KEY, rows], jnp.concatenate(xts, axis=1))

    @pl.when(g == pl.num_programs(0) - 1)
    def _():
        mean = jnp.sum(ssq[...], axis=1, keepdims=True) / inner
        r_ref[...] = jnp.broadcast_to(lax.rsqrt(mean + epsilon), r_ref.shape)


def bwd_kernel(
    gate_ref, rawv_ref, rawk_ref, dtr_ref, pv_ref, pk_ref, ph_ref,
    y_ref, gg_ref, hst_ref, r_ref, c_ref, s_ref, st_ref, hl_ref, ehl_ref, kb_ref, kt_ref, sc_ref,
    dproj_ref, sv_ref, sk_ref, sh_ref,
    pad, padk, dpad, dpadk, sg, dhcar, dsc, dkb, dsrow, dscol, ddt,
):
    g = pl.program_id(0)
    length = gate_ref.shape[0]
    blocks = length // BLK
    groups = pl.num_programs(0)

    @pl.when(g == 0)
    def _():
        pad[0:8] = jnp.zeros((8, GC), f32)
        padk[0:8] = jnp.zeros((8, 2 * KEY), f32)
        padk[8:] = rawk_ref[...]
        dpad[length:] = jnp.zeros((8, GC), f32)
        dpadk[length:] = jnp.zeros((8, 2 * KEY), f32)
        dsc[...] = jnp.zeros_like(dsc)
        dkb[...] = jnp.zeros_like(dkb)
        dsrow[...] = jnp.zeros_like(dsrow)
        dscol[...] = jnp.zeros_like(dscol)
        ddt[...] = jnp.zeros_like(ddt)

    pad[8:] = rawv_ref[...]
    sg[...] = pltpu.roll(s_ref[...], lax.rem(KEY - g * GH, KEY), 1)
    ex = expander(g)
    red = reducer(g)
    row = iota((BLK, BLK), 0)
    col = iota((BLK, BLK), 1)
    bias = jnp.where(row >= col, 0.0, NEG).astype(f32)
    strict = row > col
    low = iota((BLK, KEY), 1) < HD
    eend = mm(ehl_ref[...], ex)
    dhcar[...] = jnp.zeros_like(dhcar)
    sv_ref[...] = jnp.zeros_like(sv_ref)
    for k in range(blocks - 1, -1, -1):
        rows = slice(k * BLK, (k + 1) * BLK)
        dtx = mm(hl_ref[0, rows], ex)
        exx = mm(hl_ref[1, rows], ex)
        txx = mm(hl_ref[2, rows], ex)
        hb = hst_ref[k]
        dhb = dhcar[...].astype(bf16)
        ch = mm(kb_ref[rows, KEY:], hb)
        qq = mm(kb_ref[rows, :KEY], dhb)
        across = st_ref[pl.ds(pl.multiple_of(g * GH, GH), GH), rows]
        dyes, xts, zs, oys, ddts, ecols = [], [], [], [], [], []
        dsrow_k = jnp.zeros((BLK, KEY), f32)
        for q in range(GC // KEY):
            cols = slice(q * KEY, (q + 1) * KEY)
            window = pad[k * BLK : k * BLK + BLK + 8, cols]
            u = taps_of(window, pv_ref, cols)
            su = sigmoid(u)
            v = u * su
            x = v * dtx[:, cols]
            xb = x.astype(bf16)
            gate = gate_ref[rows, cols]
            y = y_ref[rows, cols]
            gg = gg_ref[rows, cols]
            sgt = sigmoid(gate)
            silu_g = gate * sgt
            p = y * silu_g
            r = r_ref[rows]
            dgn = gg * r
            sv_ref[5:6, cols] += jnp.sum(dgn * p, axis=0, keepdims=True)
            dp = dgn * pv_ref[5:6, cols] - p * c_ref[rows]
            dgate = dp * y * (sgt + silu_g * (1.0 - sgt))
            off = pl.multiple_of(g * GC + q * KEY, KEY)
            dproj_ref[rows, pl.ds(off, KEY)] = dgate.astype(bf16)
            dy = dp * silu_g
            sv_ref[6:7, cols] += jnp.sum(dy * v, axis=0, keepdims=True)
            dyb = dy.astype(bf16)
            dye = dy * exx[:, cols]
            dyes.append(dye.astype(bf16))
            oys.append((dye * ch[:, cols]).astype(bf16))
            xt = x * txx[:, cols]
            xts.append(xt.astype(bf16))
            zs.append((xt * qq[:, cols]).astype(bf16))
            zero = jnp.zeros_like(dyb)
            dy2 = jnp.concatenate([jnp.where(low, dyb, zero), jnp.where(low, zero, dyb)], axis=0)
            dm2 = mm_nt(dy2, xb)
            ms = []
            for half in range(2):
                j = 2 * q + half
                spread = sg[rows, j : j + 1] - across[j : j + 1]
                decay = jnp.exp(spread + bias)
                m = decay * sc_ref[k]
                ms.append(m.astype(bf16))
                dm = dm2[half * BLK : (half + 1) * BLK]
                dsc[k] += decay * dm
                e = jnp.where(strict, m * dm, 0.0)
                dsrow_k = jnp.where(col == g * GH + j, jnp.sum(e, axis=1, keepdims=True), dsrow_k)
                ecols.append(jnp.sum(e, axis=0, keepdims=True))
            dx = mm_tn(jnp.concatenate(ms, axis=0), dy2) + qq[:, cols] * txx[:, cols]
            dv = dx * dtx[:, cols] + pv_ref[6:7, cols] * dy
            ddts.append((dx * v).astype(bf16))
            du = dv * (su + v * (1.0 - su))
            dpad[rows, cols] = du
            sv_ref[4:5, cols] += jnp.sum(du, axis=0, keepdims=True)
            for t in range(4):
                sv_ref[t : t + 1, cols] += jnp.sum(du * window[5 + t : 133 + t], axis=0, keepdims=True)
        dscol[pl.ds(pl.multiple_of(g * GH, GH), GH), rows] = jnp.concatenate(ecols, axis=0)
        dye = jnp.concatenate(dyes, axis=1)
        xt = jnp.concatenate(xts, axis=1)
        zsum = mm(jnp.concatenate(zs, axis=1), red)
        ddt[rows] += mm(jnp.concatenate(ddts, axis=1), red)
        hterm = eend[k : k + 1] * jnp.sum(dhcar[...] * hb.astype(f32), axis=0, keepdims=True)
        end = jnp.sum(zsum, axis=0, keepdims=True) + mm_hi(hterm, red.astype(f32))
        add = dsrow_k + mm(jnp.concatenate(oys, axis=1), red) - zsum
        dsrow[rows] += add + jnp.where(row == BLK - 1, end, 0.0)
        dkb[rows, KEY:] += mm_nt(dye, hb)
        dkb[rows, :KEY] += mm_nt(xt, dhb)
        if k:
            dhcar[...] = eend[k : k + 1] * dhcar[...] + mm(kt_ref[KEY:, rows], dye)

    inner_off = groups * GC
    for k in range(blocks):
        rows = slice(k * BLK, (k + 1) * BLK)
        for q in range(GC // KEY):
            cols = slice(q * KEY, (q + 1) * KEY)
            window = dpad[k * BLK : k * BLK + BLK + 8, cols]
            out = pv_ref[3:4, cols] * window[0:BLK]
            for t in range(3):
                out = out + pv_ref[t : t + 1, cols] * window[3 - t : 3 - t + BLK]
            off = pl.multiple_of(inner_off + g * GC + q * KEY, KEY)
            dproj_ref[rows, pl.ds(off, KEY)] = out.astype(bf16)

    @pl.when(g == groups - 1)
    def _():
        keys = 2 * groups * GC
        sk_ref[...] = jnp.zeros_like(sk_ref)
        sh_ref[...] = jnp.zeros_like(sh_ref)
        upper = jnp.where(row <= col, 1.0, 0.0).astype(f32)
        for k in range(blocks):
            rows = slice(k * BLK, (k + 1) * BLK)
            window = padk[k * BLK : k * BLK + BLK + 8]
            u = taps_of(window, pk_ref, slice(0, 2 * KEY))
            su = sigmoid(u)
            ds = dsc[k].astype(bf16)
            db = dkb[rows, :KEY] + mm_tn(ds, kb_ref[rows, KEY:])
            dc = dkb[rows, KEY:] + mm(ds, kb_ref[rows, :KEY])
            du = jnp.concatenate([db, dc], axis=1) * (su + u * su * (1.0 - su))
            dpadk[rows] = du
            sk_ref[4:5] += jnp.sum(du, axis=0, keepdims=True)
            for t in range(4):
                sk_ref[t : t + 1] += jnp.sum(du * window[5 + t : 133 + t], axis=0, keepdims=True)
            dla = mm_hi(upper, dsrow[rows] - dscol[:, rows].T)
            z = dtr_ref[rows] + ph_ref[0:1, :]
            rate = jnp.exp(ph_ref[1:2, :])
            dt = jax.nn.softplus(z)
            sh_ref[1:2] += jnp.sum(dla * (-dt * rate), axis=0, keepdims=True)
            dz = (ddt[rows] - dla * rate) * sigmoid(z)
            sh_ref[0:1] += jnp.sum(dz, axis=0, keepdims=True)
            dproj_ref[rows, keys + 2 * KEY : keys + 3 * KEY] = dz.astype(bf16)
            dproj_ref[rows, keys + 3 * KEY :] = jnp.zeros((BLK, dproj_ref.shape[1] - keys - 3 * KEY), bf16)
        for k in range(blocks):
            rows = slice(k * BLK, (k + 1) * BLK)
            window = dpadk[k * BLK : k * BLK + BLK + 8]
            out = pk_ref[3:4] * window[0:BLK]
            for t in range(3):
                out = out + pk_ref[t : t + 1] * window[3 - t : 3 - t + BLK]
            dproj_ref[rows, keys : keys + 2 * KEY] = out.astype(bf16)


def whole_spec(shape):
    return pl.BlockSpec(shape, lambda g: (0,) * len(shape))


def state_specs(length):
    return (
        ((length, KEY), f32),
        ((KEY, length), f32),
        ((3, length, 2 * KEY), bf16),
        ((8, 2 * KEY), bf16),
        ((length, 2 * KEY), bf16),
        ((2 * KEY, length), bf16),
        ((length // BLK, BLK, BLK), f32),
    )


def proj_specs(length, groups):
    wide = groups * GC
    return [
        pl.BlockSpec((length, GC), lambda g: (0, g)),
        pl.BlockSpec((length, GC), lambda g: (0, groups + g)),
        pl.BlockSpec((length, 2 * KEY), lambda g: (0, 2 * wide // (2 * KEY))),
        pl.BlockSpec((length, KEY), lambda g: (0, 2 * wide // KEY + 2)),
        pl.BlockSpec((8, GC), lambda g: (0, g)),
        whole_spec((8, 2 * KEY)),
        whole_spec((8, KEY)),
    ]


def mixer_forward(projected, pv, pk, ph):
    length = projected.shape[0]
    wide = pv.shape[1]
    groups = wide // GC
    blocks = length // BLK
    column = pl.BlockSpec((length, GC), lambda g: (0, g))
    shared = state_specs(length)
    return pl.pallas_call(
        fwd_kernel,
        grid=(groups,),
        in_specs=proj_specs(length, groups),
        out_specs=[
            column,
            column,
            pl.BlockSpec((blocks, KEY, GC), lambda g: (0, 0, g)),
            whole_spec((length, KEY)),
        ]
        + [whole_spec(shape) for shape, _ in shared],
        out_shape=[
            jax.ShapeDtypeStruct((length, wide), f32),
            jax.ShapeDtypeStruct((length, wide), f32),
            jax.ShapeDtypeStruct((blocks, KEY, wide), bf16),
            jax.ShapeDtypeStruct((length, KEY), f32),
        ]
        + [jax.ShapeDtypeStruct(shape, dtype) for shape, dtype in shared],
        scratch_shapes=[
            pltpu.VMEM((length + 8, GC), f32),
            pltpu.VMEM((length + 8, 2 * KEY), f32),
            pltpu.VMEM((length, KEY), f32),
            pltpu.VMEM((KEY, GC), f32),
            pltpu.VMEM((length, KEY), f32),
        ],
        name="mixer_forward",
    )(projected, projected, projected, projected, pv, pk, ph)


def mixer_backward(projected, pv, pk, ph, mixed, grad_gated, states, inverse, pull, shared):
    length, total = projected.shape
    wide = pv.shape[1]
    groups = wide // GC
    blocks = length // BLK
    column = pl.BlockSpec((length, GC), lambda g: (0, g))
    return pl.pallas_call(
        bwd_kernel,
        grid=(groups,),
        in_specs=proj_specs(length, groups)
        + [
            column,
            column,
            pl.BlockSpec((blocks, KEY, GC), lambda g: (0, 0, g)),
            whole_spec((length, KEY)),
            whole_spec((length, KEY)),
        ]
        + [whole_spec(shape) for shape, _ in state_specs(length)],
        out_specs=[
            whole_spec((length, total)),
            pl.BlockSpec((8, GC), lambda g: (0, g)),
            whole_spec((8, 2 * KEY)),
            whole_spec((8, KEY)),
        ],
        out_shape=[
            jax.ShapeDtypeStruct((length, total), bf16),
            jax.ShapeDtypeStruct((8, wide), f32),
            jax.ShapeDtypeStruct((8, 2 * KEY), f32),
            jax.ShapeDtypeStruct((8, KEY), f32),
        ],
        scratch_shapes=[
            pltpu.VMEM((length + 8, GC), f32),
            pltpu.VMEM((length + 8, 2 * KEY), f32),
            pltpu.VMEM((length + 8, GC), f32),
            pltpu.VMEM((length + 8, 2 * KEY), f32),
            pltpu.VMEM((length, KEY), f32),
            pltpu.VMEM((KEY, GC), f32),
            pltpu.VMEM((blocks, BLK, BLK), f32),
            pltpu.VMEM((length, 2 * KEY), f32),
            pltpu.VMEM((length, KEY), f32),
            pltpu.VMEM((KEY, length), f32),
            pltpu.VMEM((length, KEY), f32),
        ],
        name="mixer_backward",
    )(
        projected, projected, projected, projected, pv, pk, ph,
        mixed, grad_gated, states, inverse, pull, *shared,
    )


MESH = pl.DeviceIdType.MESH
HALF = 256


def places():
    d, f = lax.axis_index("dp"), lax.axis_index("fsdp")
    z, x, y, c = d // 2, d % 2, f // 2, f % 2
    over_core = (d, y * 2 + 1 - c)
    over_x = (z * 2 + 1 - x, f)
    over_y = (d, (1 - y) * 2 + c)
    far = (((z + 2) % 4) * 2 + x, f)
    near = ((z + 1 - 2 * (z % 2)) * 2 + x, f)
    peers = ((over_core, over_x, over_y, far, near), (over_core, over_y, over_x, far, near))
    own = ((c, x, y, z // 2, z % 2), (c, y, x, z // 2, z % 2))
    return peers, own


def greet(partners):
    barrier = pltpu.get_barrier_semaphore()
    for partner in partners:
        pl.semaphore_signal(barrier, inc=1, device_id=partner, device_id_type=MESH)
    pl.semaphore_wait(barrier, len(partners))


def block_order(half, i):
    z, x, y, c = i // 8, i // 4 % 2, i // 2 % 2, i % 2
    first, second = (x, y) if half == 0 else (y, x)
    return c, first * 8 + second * 4 + z


def scatter_kernel(
    n, rb, lhs_ref, rhs_ref, extra_ref, head_ref, out_ref, sums_ref,
    parts, r0, r1, r2, r3, r4, sums, sums_in, send, recv, sums_sem,
):
    peers, own = places()
    held = (r0, r1, r2, r3, r4)
    greet(peers[0])

    def sums_copy(stage):
        return pltpu.make_async_remote_copy(
            src_ref=sums.at[stage],
            dst_ref=sums_in.at[stage],
            send_sem=sums_sem.at[0, stage],
            recv_sem=sums_sem.at[1, stage],
            device_id=peers[0][stage],
            device_id_type=MESH,
        )

    sums[0] = head_ref[...]
    sums_copy(0).start()

    def copy(stage, i, half):
        count = 16 >> stage
        if stage == 0:
            src = parts.at[lax.rem(i, 2), 1 - own[half][0], half]
        else:
            src = held[stage - 1].at[i, half, pl.ds((1 - own[half][stage]) * count, count)]
        return pltpu.make_async_remote_copy(
            src_ref=src,
            dst_ref=held[stage].at[i, half],
            send_sem=send.at[i, half, stage],
            recv_sem=recv.at[i, half, stage],
            device_id=peers[half][stage],
            device_id_type=MESH,
        )

    def tick(t, carry):
        @pl.when(t < n)
        def _():
            slot = lax.rem(t, 2)

            @pl.when(t >= 2)
            def _():
                for half in range(2):
                    copy(0, t - 2, half).wait_send()

            for half in range(2):
                cols = pl.ds(pl.multiple_of(t * 2 * HALF + half * HALF, HALF), HALF)
                right = rhs_ref[:, cols]
                for z in range(4):
                    rows = slice(z * 8 * rb, (z + 1) * 8 * rb)
                    res = lax.dot_general(
                        lhs_ref[rows], right, (((1,), (0,)), ((), ())), preferred_element_type=f32
                    )
                    for b in range(8):
                        c, at = block_order(half, z * 8 + b)
                        parts[slot, c, half, at] = res[b * rb : (b + 1) * rb].astype(bf16)

            @pl.when(t == n - 1)
            def _():
                for i in range(32):
                    c, at = block_order(1, i)
                    rows = slice(i * rb, (i + 1) * rb)
                    parts[slot, c, 1, at, :, :KEY] = (
                        parts[slot, c, 1, at, :, :KEY].astype(f32) + extra_ref[rows]
                    ).astype(bf16)

            for half in range(2):
                copy(0, t, half).start()

        for stage in range(5):
            i = t - stage - 1

            @pl.when(i == 0)
            def _(stage=stage):
                sums_copy(stage).wait()
                if stage < 4:
                    sums[stage + 1] = sums[stage] + sums_in[stage]
                    sums_copy(stage + 1).start()
                else:
                    sums_ref[...] = sums[stage] + sums_in[stage]

            @pl.when((i >= 0) & (i < n))
            def _(stage=stage, i=i):
                count = 16 >> stage
                for half in range(2):
                    done = copy(stage, i, half)
                    if stage == 0:
                        done.wait_recv()
                        mine = parts[lax.rem(i, 2), own[half][0], half]
                    else:
                        done.wait()
                        mine = held[stage - 1][i, half, pl.ds(own[half][stage] * count, count)]
                    if stage < 4:
                        held[stage][i, half] = (
                            held[stage][i, half].astype(f32) + mine.astype(f32)
                        ).astype(bf16)
                        copy(stage + 1, i, half).start()
                    else:
                        cols = pl.ds(pl.multiple_of(i * 2 * HALF + half * HALF, HALF), HALF)
                        out_ref[:, cols] = held[stage][i, half, 0].astype(f32) + mine[0].astype(f32)

        return carry

    lax.fori_loop(0, n + 5, tick, 0)
    for i in (n - 2, n - 1):
        for half in range(2):
            copy(0, i, half).wait_send()


def scatter_product(lhs, rhs, extra, heads):
    rows, depth = lhs.shape
    columns = rhs.shape[1]
    n, rb = columns // (2 * HALF), rows // 32
    vmem = pl.BlockSpec(memory_space=pltpu.VMEM)
    return pl.pallas_call(
        partial(scatter_kernel, n, rb),
        out_shape=(jax.ShapeDtypeStruct((rb, columns), f32), jax.ShapeDtypeStruct(heads.shape, f32)),
        in_specs=[vmem] * 4,
        out_specs=(vmem, vmem),
        scratch_shapes=[pltpu.VMEM((2, 2, 2, 16, rb, HALF), bf16)]
        + [pltpu.VMEM((n, 2, 16 >> stage, rb, HALF), bf16) for stage in range(5)]
        + [pltpu.VMEM((5,) + heads.shape, f32)] * 2
        + [pltpu.SemaphoreType.DMA((n, 2, 5))] * 2
        + [pltpu.SemaphoreType.DMA((2, 5))],
        compiler_params=pltpu.CompilerParams(
            collective_id=1, has_side_effects=True, vmem_limit_bytes=60 << 20
        ),
        name="scatter_product",
    )(lhs, rhs, extra, heads)


def gather_kernel(
    n, gain_at, hidden_ref, w_ref, w_out, proj_out, normed_ref, flipped_ref,
    held, w_stage, proj_stage, send, recv, out_sem,
):
    rb = w_ref.shape[0]
    peers, own = places()
    greet(peers[0])
    base = [own[h][0] * 16 + own[h][1] * 8 + own[h][2] * 4 + own[h][3] * 2 + own[h][4] for h in range(2)]
    count = (1, 2, 4, 8, 16)
    source = lambda i: lax.rem(i + n - 1, n)

    def columns(i, half):
        return pl.ds(pl.multiple_of(source(i) * 2 * HALF + half * HALF, HALF), HALF)

    def copy(stage, i, half):
        start = base[half] // count[stage] * count[stage]
        block = held.at[i, half, pl.ds(start, count[stage])]
        return pltpu.make_async_remote_copy(
            src_ref=block,
            dst_ref=block,
            send_sem=send.at[i, half, stage],
            recv_sem=recv.at[i, half, stage],
            device_id=peers[half][4 - stage],
            device_id_type=MESH,
        )

    def stores(i):
        slot = lax.rem(i, 2)
        cols = pl.ds(pl.multiple_of(source(i) * 2 * HALF, 2 * HALF), 2 * HALF)
        return (
            pltpu.make_async_copy(w_stage.at[slot], w_out.at[:, cols], out_sem.at[0, slot]),
            pltpu.make_async_copy(proj_stage.at[slot], proj_out.at[:, cols], out_sem.at[1, slot]),
        )

    def land(i, carry):
        for half in range(2):
            held[i, half, base[half]] = w_ref[:, columns(i, half)]
        return carry

    lax.fori_loop(0, n, land, 0)

    def tick(t, carry):
        @pl.when(t < n)
        def _():
            for half in range(2):
                copy(0, t, half).start()

        for stage in range(5):
            i = t - stage - 1

            @pl.when((i >= 0) & (i < n))
            def _(stage=stage, i=i):
                for half in range(2):
                    copy(stage, i, half).wait()
                    if stage < 4:
                        copy(stage + 1, i, half).start()
                if stage == 4:
                    slot = lax.rem(i, 2)

                    @pl.when(i >= 2)
                    def _():
                        for store in stores(i - 2):
                            store.wait()

                    for half in range(2):
                        for b in range(32):
                            c, at = block_order(half, b)
                            w_stage[slot, b * rb : (b + 1) * rb, half * HALF : (half + 1) * HALF] = held[
                                i, half, c * 16 + at
                            ]

                    @pl.when(i == 0)
                    def _():
                        tile = w_stage[slot, :, HALF : HALF + KEY].astype(f32)
                        gain = tile.T[gain_at : gain_at + 1]
                        for k in range(0, hidden_ref.shape[0], KEY):
                            wide = hidden_ref[k : k + KEY].astype(f32)
                            mean = jnp.mean(wide * wide, axis=1, keepdims=True)
                            normed = (wide * lax.rsqrt(mean + epsilon) * gain).astype(bf16)
                            normed_ref[k : k + KEY] = normed
                            flipped_ref[:, k : k + KEY] = normed.T

                    for half in range(2):
                        cols = slice(half * HALF, (half + 1) * HALF)
                        proj_stage[slot, :, cols] = lax.dot_general(
                            normed_ref[...],
                            w_stage[slot, :, cols],
                            (((1,), (0,)), ((), ())),
                            preferred_element_type=f32,
                        )
                    for store in stores(i):
                        store.start()

        return carry

    lax.fori_loop(0, n + 5, tick, 0)
    for i in (n - 2, n - 1):
        for store in stores(i):
            store.wait()


def gather_product(hidden, shard, gain_at):
    length, width = hidden.shape
    rb, columns = shard.shape
    n = columns // (2 * HALF)
    vmem = pl.BlockSpec(memory_space=pltpu.VMEM)
    anywhere = pl.BlockSpec(memory_space=pl.ANY)
    return pl.pallas_call(
        partial(gather_kernel, n, gain_at),
        out_shape=(
            jax.ShapeDtypeStruct((width, columns), bf16),
            jax.ShapeDtypeStruct((length, columns), f32),
            jax.ShapeDtypeStruct((length, width), bf16),
            jax.ShapeDtypeStruct((width, length), bf16),
        ),
        in_specs=[vmem, vmem],
        out_specs=(anywhere, anywhere, vmem, vmem),
        scratch_shapes=[
            pltpu.VMEM((n, 2, 32, rb, HALF), bf16),
            pltpu.VMEM((2, width, 2 * HALF), bf16),
            pltpu.VMEM((2, length, 2 * HALF), f32),
            pltpu.SemaphoreType.DMA((n, 2, 5)),
            pltpu.SemaphoreType.DMA((n, 2, 5)),
            pltpu.SemaphoreType.DMA((2, 2)),
        ],
        compiler_params=pltpu.CompilerParams(
            collective_id=2, has_side_effects=True, vmem_limit_bytes=60 << 20
        ),
        name="gather_product",
    )(hidden, shard)


def pre_norm_inverse(rows):
    return lax.rsqrt(jnp.mean(rows * rows, axis=1, keepdims=True) + epsilon)


AXES = ("dp", "fsdp")
HEAD_LANES = KEY


def gather_rows(shard):
    return lax.all_gather(shard, AXES, axis=0, tiled=True)


def scatter_rows(whole):
    return lax.psum_scatter(whole, AXES, scatter_dimension=0, tiled=True)


def pack_columns(parts, rows, width):
    flat = jnp.concatenate([part.reshape(-1) for part in parts])
    return jnp.pad(flat, (0, rows * width - flat.shape[0])).reshape(rows, width)


def shards(
    kernels, hidden, cotangent, lengths, norm_gain, in_proj, dt_proj, conv_weight, conv_bias,
    dt_bias, a_log, skip_gain, gate_gain, out_proj,
):
    length, width = hidden.shape
    assert lengths.shape[0] == 1
    rows_in, columns = in_proj.shape
    heads = dt_bias.shape[0]
    parts = width // rows_in
    taps, conv_part = conv_weight.shape
    gate_part = gate_gain.shape[0]
    wide = gate_part * parts
    small_count = taps * conv_part + conv_part + gate_part
    small_width = -(-small_count // rows_in)
    total = columns + 2 * KEY
    gain_at = columns + heads
    small_at = gain_at + 1

    small = pack_columns((conv_weight, conv_bias, gate_gain), rows_in, small_width)
    fill = jnp.zeros((rows_in, total - small_at - small_width), bf16)
    packed = jnp.concatenate([in_proj, dt_proj, norm_gain[:, None], small, fill], axis=1)
    w_out = gather_rows(out_proj)
    rows_wide = hidden.astype(f32)
    inverse_one = pre_norm_inverse(rows_wide)
    if kernels:
        w_in, projected, normed, flipped = gather_product(hidden, packed, heads)
        gain_one = w_in[:, gain_at].astype(f32)
    else:
        w_in = gather_rows(packed)
        gain_one = w_in[:, gain_at].astype(f32)
        normed = (rows_wide * inverse_one * gain_one[None, :]).astype(bf16)
        projected = mm(normed, w_in)
    small_all = w_in[:, small_at : small_at + small_width].astype(f32).reshape(parts, -1)
    ends = [taps * conv_part, small_count - gate_part, small_count]
    conv_taps = jnp.transpose(small_all[:, : ends[0]].reshape(parts, taps, conv_part), (1, 0, 2))
    conv_taps = conv_taps.reshape(taps, parts * conv_part)
    conv_shift = small_all[:, ends[0] : ends[1]].reshape(1, -1)
    gain_two = small_all[:, ends[1] : ends[2]].reshape(1, -1)
    live = (jnp.arange(length) < lengths[0]).astype(f32)[:, None]

    skip_wide = jnp.repeat(skip_gain.astype(f32), HD)[None]
    pv = jnp.concatenate(
        [conv_taps[:, :wide], conv_shift[:, :wide], gain_two, skip_wide, jnp.zeros((1, wide), f32)], axis=0
    )
    pk = jnp.concatenate([conv_taps[:, wide:], conv_shift[:, wide:], jnp.zeros((3, 2 * KEY), f32)], axis=0)
    ph = jnp.pad(jnp.stack([dt_bias, a_log]).astype(f32), ((0, 6), (0, KEY - heads)))
    mixed, product, states, inverse_two, *shared = mixer_forward(projected, pv, pk, ph)
    inv = inverse_two[:, :1]
    gated = (product * inv * gain_two).astype(bf16)
    output = (rows_wide + live * mm(gated, w_out)).astype(bf16)

    cot_wide = cotangent.astype(f32)
    upstream = (cot_wide * live).astype(bf16)
    grad_gated = mm_nt(upstream, w_out)
    pull = jnp.sum(grad_gated * gain_two * product, axis=1, keepdims=True)
    pull = jnp.broadcast_to(inv * inv * inv * pull / wide, inverse_two.shape)
    grad_proj, sums_v, sums_k, sums_h = mixer_backward(
        projected, pv, pk, ph, mixed, grad_gated, states, inverse_two, pull, shared
    )
    skip_grad = jnp.pad(jnp.sum(sums_v[6].reshape(heads, HD), axis=1), (0, KEY - heads))[None]
    head_grads = jnp.concatenate([sums_h[:2], skip_grad, jnp.zeros((5, KEY), f32)], axis=0)

    grad_normed = mm_nt(grad_proj, w_in)
    scaled = grad_normed * gain_one[None, :]
    dots = jnp.sum(scaled * rows_wide, axis=1, keepdims=True) / width
    grad_rows = inverse_one * scaled - rows_wide * (inverse_one * inverse_one * inverse_one * dots)
    input_grad = cot_wide + grad_rows
    grad_gain_one = jnp.sum(grad_normed * rows_wide * inverse_one, axis=0)

    conv_grad = jnp.concatenate([sums_v[:5], sums_k[:5]], axis=1)
    small_grad = jnp.concatenate(
        [
            jnp.transpose(conv_grad[:taps].reshape(taps, parts, conv_part), (1, 0, 2)).reshape(parts, -1),
            conv_grad[taps].reshape(parts, conv_part),
            sums_v[5].reshape(parts, gate_part),
            jnp.zeros((parts, rows_in * small_width - small_count), f32),
        ],
        axis=1,
    ).reshape(width, small_width)
    extra = jnp.concatenate(
        [
            jnp.zeros((width, heads), f32),
            grad_gain_one[:, None],
            small_grad,
            jnp.zeros((width, KEY - heads - 1 - small_width), f32),
        ],
        axis=1,
    )

    grad_out = scatter_rows(mm_tn(gated, upstream).astype(bf16)).astype(f32)
    if kernels:
        grad_in, head_sums = scatter_product(flipped, grad_proj, extra, head_grads)
    else:
        head_sums = lax.psum(head_grads, AXES)
        grad_in = mm_tn(normed, grad_proj)
        grad_in = grad_in + jnp.pad(extra, ((0, 0), (columns, total - columns - KEY)))
        grad_in = scatter_rows(grad_in.astype(bf16)).astype(f32)
    small_sum = grad_in[:, small_at : small_at + small_width].reshape(-1)
    return (
        output,
        input_grad,
        grad_in[:, gain_at],
        grad_in[:, :columns],
        grad_in[:, columns:gain_at],
        small_sum[: ends[0]].reshape(taps, conv_part),
        small_sum[ends[0] : ends[1]],
        head_sums[0, :heads],
        head_sums[1, :heads],
        head_sums[2, :heads],
        small_sum[ends[1] : ends[2]],
        grad_out,
    )


def solution(mesh):
    rows = P(AXES, None)
    vector = P(AXES)
    last = P(None, AXES)
    return jax.shard_map(
        partial(shards, mesh.shape["dp"] == 8 and mesh.shape["fsdp"] == 4),
        mesh=mesh,
        in_specs=(rows, rows, vector, vector, rows, rows, last, vector, P(), P(), P(), vector, rows),
        out_specs=(rows, rows, vector, rows, rows, last, vector, P(), P(), P(), vector, rows),
        check_vma=False,
    )
```

```python
from functools import partial

import jax
import jax.numpy as jnp
from jax import lax
from jax.experimental import pallas as pl
from jax.experimental.pallas import tpu as pltpu
from jax.sharding import PartitionSpec as P

f32 = jnp.float32
bf16 = jnp.bfloat16
epsilon = 1e-05
highest = lax.Precision.HIGHEST
BLK = 128
GH = 4
HD = 64
GC = GH * HD
KEY = 128
NEG = -1e30


def sigmoid(v):
    return 0.5 * jnp.tanh(0.5 * v) + 0.5


def mm(a, b):
    return lax.dot_general(a, b, (((1,), (0,)), ((), ())), preferred_element_type=f32)


def mm_nt(a, b):
    return lax.dot_general(a, b, (((1,), (1,)), ((), ())), preferred_element_type=f32)


def mm_tn(a, b):
    return lax.dot_general(a, b, (((0,), (0,)), ((), ())), preferred_element_type=f32)


def mm_hi(a, b, dims=((1,), (0,))):
    return lax.dot_general(a, b, (dims, ((), ())), preferred_element_type=f32, precision=highest)


def split(v):
    hi = v.astype(bf16)
    lo = (v - hi.astype(f32)).astype(bf16)
    return jnp.concatenate([hi, lo], axis=1)


def iota(shape, dim):
    return lax.broadcasted_iota(jnp.int32, shape, dim)


def expander(g):
    rows = iota((2 * KEY, GC), 0)
    cols = iota((2 * KEY, GC), 1)
    return jnp.where(lax.rem(rows, KEY) == cols // HD + g * GH, 1.0, 0.0).astype(bf16)


def reducer(g):
    rows = iota((GC, KEY), 0)
    cols = iota((GC, KEY), 1)
    return jnp.where(rows // HD + g * GH == cols, 1.0, 0.0).astype(bf16)


def taps_of(window, par):
    out = par[4:5] + par[3:4] * window[8:136]
    for k in range(3):
        out = out + par[k : k + 1] * window[5 + k : 133 + k]
    return out


def group_rows(st_ref, g, half, rows):
    tile = st_ref[pl.ds(pl.multiple_of(g // 2 * 8, 8), 8), rows]
    return jnp.where(half == 0, tile[:GH], tile[GH:])


def forward_shared(
    rawk_ref, dtr_ref, pv_ref, key_at, ph_ref, s_ref, st_ref, hl_ref, ehl_ref, kb_ref, kt_ref, sc_ref, padk
):
    blocks = rawk_ref.shape[0] // BLK
    dt = jax.nn.softplus(dtr_ref[...] + ph_ref[0:1, :])
    la = -dt * jnp.exp(ph_ref[1:2, :])
    tri = jnp.where(iota((BLK, BLK), 0) >= iota((BLK, BLK), 1), 1.0, 0.0).astype(f32)
    hl_ref[0] = split(dt)
    ehl_ref[...] = jnp.zeros_like(ehl_ref)
    padk[0:8] = jnp.zeros((8, 2 * KEY), f32)
    padk[8:] = rawk_ref[...]
    par = pv_ref[:, key_at : key_at + 2 * KEY]
    for k in range(blocks):
        rows = slice(k * BLK, (k + 1) * BLK)
        s = mm_hi(tri, la[rows])
        s_ref[rows] = s
        st_ref[:, rows] = s.T
        hl_ref[1, rows] = split(jnp.exp(s))
        hl_ref[2, rows] = split(jnp.exp(s[BLK - 1 :] - s))
        ehl_ref[k : k + 1] = split(jnp.exp(s[BLK - 1 :]))
        u = taps_of(padk[k * BLK : k * BLK + BLK + 8], par)
        v = u * sigmoid(u)
        kb_ref[rows] = v.astype(bf16)
        kt_ref[:, rows] = v.T.astype(bf16)
        sc_ref[k] = mm_hi(v[:, KEY:], v[:, :KEY], ((1,), (1,)))


def forward_group(
    g, gate_ref, rawv_ref, pv_ref, s_ref, st_ref, hl_ref, ehl_ref, kb_ref, kt_ref, sc_ref,
    y_ref, p_ref, hst_ref, pad, sg, hcar, ssq,
):
    blocks = gate_ref.shape[0] // BLK
    pad[8:] = rawv_ref[...]
    sg[...] = pltpu.roll(s_ref[...], lax.rem(KEY - g * GH, KEY), 1)
    ex = expander(g)
    bias = jnp.where(iota((BLK, BLK), 0) >= iota((BLK, BLK), 1), 0.0, NEG).astype(f32)
    low = iota((BLK, KEY), 1) < HD
    eend = mm(ehl_ref[...], ex)
    parg = pv_ref[:, pl.ds(pl.multiple_of(g * GC, GC), GC)]
    half = lax.rem(g, 8 // GH)
    hcar[...] = jnp.zeros_like(hcar)
    for k in range(blocks):
        rows = slice(k * BLK, (k + 1) * BLK)
        dtx = mm(hl_ref[0, rows], ex)
        exx = mm(hl_ref[1, rows], ex)
        txx = mm(hl_ref[2, rows], ex)
        hb = hcar[...].astype(bf16)
        hst_ref[k] = hb
        outer = mm(kb_ref[rows, KEY:], hb)
        across = group_rows(st_ref, g, half, rows)
        xts = []
        for q in range(GC // KEY):
            cols = slice(q * KEY, (q + 1) * KEY)
            par = parg[:, cols]
            u = taps_of(pad[k * BLK : k * BLK + BLK + 8, cols], par)
            v = u * sigmoid(u)
            x = v * dtx[:, cols]
            xts.append((x * txx[:, cols]).astype(bf16))
            xb = x.astype(bf16)
            zero = jnp.zeros_like(xb)
            x2 = jnp.concatenate([jnp.where(low, xb, zero), jnp.where(low, zero, xb)], axis=0)
            ms = []
            for side in range(2):
                j = 2 * q + side
                spread = sg[rows, j : j + 1] - across[j : j + 1]
                ms.append((jnp.exp(spread + bias) * sc_ref[k]).astype(bf16))
            y = mm(jnp.concatenate(ms, axis=1), x2)
            y = y + outer[:, cols] * exx[:, cols] + par[6:7] * v
            y_ref[rows, cols] = y
            gate = gate_ref[rows, cols]
            p = y * (gate * sigmoid(gate))
            p_ref[rows, pl.ds(pl.multiple_of(g * GC + q * KEY, KEY), KEY)] = p
            ssq[rows] += p * p
        if k + 1 < blocks:
            hcar[...] = eend[k : k + 1] * hcar[...] + mm(kt_ref[:KEY, rows], jnp.concatenate(xts, axis=1))


def fwd_kernel(
    gate_ref, rawv_ref, rawk_ref, dtr_ref, pv_ref, ph_ref,
    y_ref, p_ref, hst_ref, r_ref, s_ref, st_ref, hl_ref, ehl_ref, kb_ref, kt_ref, sc_ref,
    pad, padk, sg, hcar, ssq,
):
    g = pl.program_id(0)
    wide = p_ref.shape[1]
    shared = (s_ref, st_ref, hl_ref, ehl_ref, kb_ref, kt_ref, sc_ref)

    @pl.when(g == 0)
    def _():
        forward_shared(rawk_ref, dtr_ref, pv_ref, wide, ph_ref, *shared, padk)
        pad[0:8] = jnp.zeros((8, GC), f32)
        ssq[...] = jnp.zeros_like(ssq)

    forward_group(g, gate_ref, rawv_ref, pv_ref, *shared, y_ref, p_ref, hst_ref, pad, sg, hcar, ssq)

    @pl.when(g == pl.num_programs(0) - 1)
    def _():
        mean = jnp.sum(ssq[...], axis=1, keepdims=True) / wide
        r_ref[...] = jnp.broadcast_to(lax.rsqrt(mean + epsilon), r_ref.shape)


def backward_start(length, pad, dpad, dsc, dkb, dsrow, dscol, ddt):
    pad[0:8] = jnp.zeros((8, GC), f32)
    dpad[length:] = jnp.zeros((8, GC), f32)
    for ref in (dsc, dkb, dsrow, dscol, ddt):
        ref[...] = jnp.zeros_like(ref)


def backward_group(
    g, gate_ref, rawv_ref, y_ref, gg_ref, hst_ref, r_ref, c_ref, pv_ref, shared,
    dgate_ref, draw_ref, sv_ref, pad, dpad, sg, dhcar, dsc, dkb, dsrow, dscol, ddt,
):
    s_ref, st_ref, hl_ref, ehl_ref, kb_ref, kt_ref, sc_ref = shared
    blocks = gate_ref.shape[0] // BLK
    pad[8:] = rawv_ref[...]
    sg[...] = pltpu.roll(s_ref[...], lax.rem(KEY - g * GH, KEY), 1)
    ex = expander(g)
    red = reducer(g)
    row = iota((BLK, BLK), 0)
    col = iota((BLK, BLK), 1)
    bias = jnp.where(row >= col, 0.0, NEG).astype(f32)
    strict = row > col
    low = iota((BLK, KEY), 1) < HD
    eend = mm(ehl_ref[...], ex)
    parg = pv_ref[:, pl.ds(pl.multiple_of(g * GC, GC), GC)]
    half = lax.rem(g, 8 // GH)
    tile_at = pl.ds(pl.multiple_of(g // 2 * 8, 8), 8)
    mine = (iota((8, BLK), 0) < GH) == (half == 0)
    dhcar[...] = jnp.zeros_like(dhcar)
    sv_ref[...] = jnp.zeros_like(sv_ref)
    for k in range(blocks - 1, -1, -1):
        rows = slice(k * BLK, (k + 1) * BLK)
        dtx = mm(hl_ref[0, rows], ex)
        exx = mm(hl_ref[1, rows], ex)
        txx = mm(hl_ref[2, rows], ex)
        hb = hst_ref[k]
        dhb = dhcar[...].astype(bf16)
        ch = mm(kb_ref[rows, KEY:], hb)
        qq = mm(kb_ref[rows, :KEY], dhb)
        across = group_rows(st_ref, g, half, rows)
        dyes, xts, zs, oys, ddts, ecols = [], [], [], [], [], []
        dsrow_k = jnp.zeros((BLK, KEY), f32)
        for q in range(GC // KEY):
            cols = slice(q * KEY, (q + 1) * KEY)
            par = parg[:, cols]
            window = pad[k * BLK : k * BLK + BLK + 8, cols]
            u = taps_of(window, par)
            su = sigmoid(u)
            v = u * su
            x = v * dtx[:, cols]
            xb = x.astype(bf16)
            gate = gate_ref[rows, cols]
            y = y_ref[rows, cols]
            sgt = sigmoid(gate)
            silu_g = gate * sgt
            p = y * silu_g
            dgn = gg_ref[rows, cols] * r_ref[rows]
            sv_ref[5:6, cols] += jnp.sum(dgn * p, axis=0, keepdims=True)
            dp = dgn * par[5:6] - p * c_ref[rows]
            dgate_ref[rows, cols] = (dp * y * (sgt + silu_g * (1.0 - sgt))).astype(bf16)
            dy = dp * silu_g
            sv_ref[6:7, cols] += jnp.sum(dy * v, axis=0, keepdims=True)
            dyb = dy.astype(bf16)
            dye = dy * exx[:, cols]
            dyes.append(dye.astype(bf16))
            oys.append((dye * ch[:, cols]).astype(bf16))
            xt = x * txx[:, cols]
            xts.append(xt.astype(bf16))
            zs.append((xt * qq[:, cols]).astype(bf16))
            zero = jnp.zeros_like(dyb)
            dy2 = jnp.concatenate([jnp.where(low, dyb, zero), jnp.where(low, zero, dyb)], axis=0)
            dm2 = mm_nt(dy2, xb)
            ms = []
            for side in range(2):
                j = 2 * q + side
                spread = sg[rows, j : j + 1] - across[j : j + 1]
                decay = jnp.exp(spread + bias)
                m = decay * sc_ref[k]
                ms.append(m.astype(bf16))
                dm = dm2[side * BLK : (side + 1) * BLK]
                dsc[k] += decay * dm
                e = jnp.where(strict, m * dm, 0.0)
                dsrow_k = jnp.where(col == g * GH + j, jnp.sum(e, axis=1, keepdims=True), dsrow_k)
                ecols.append(jnp.sum(e, axis=0, keepdims=True))
            dx = mm_tn(jnp.concatenate(ms, axis=0), dy2) + qq[:, cols] * txx[:, cols]
            dv = dx * dtx[:, cols] + par[6:7] * dy
            ddts.append((dx * v).astype(bf16))
            du = dv * (su + v * (1.0 - su))
            dpad[rows, cols] = du
            sv_ref[4:5, cols] += jnp.sum(du, axis=0, keepdims=True)
            for t in range(4):
                sv_ref[t : t + 1, cols] += jnp.sum(du * window[5 + t : 133 + t], axis=0, keepdims=True)
        dscol[tile_at, rows] += jnp.where(mine, jnp.concatenate(ecols + ecols, axis=0), 0.0)
        dye = jnp.concatenate(dyes, axis=1)
        xt = jnp.concatenate(xts, axis=1)
        zsum = mm(jnp.concatenate(zs, axis=1), red)
        ddt[rows] += mm(jnp.concatenate(ddts, axis=1), red)
        hterm = eend[k : k + 1] * jnp.sum(dhcar[...] * hb.astype(f32), axis=0, keepdims=True)
        end = jnp.sum(zsum, axis=0, keepdims=True) + mm_hi(hterm, red.astype(f32))
        add = dsrow_k + mm(jnp.concatenate(oys, axis=1), red) - zsum
        dsrow[rows] += add + jnp.where(row == BLK - 1, end, 0.0)
        dkb[rows, KEY:] += mm_nt(dye, hb)
        dkb[rows, :KEY] += mm_nt(xt, dhb)
        if k:
            dhcar[...] = eend[k : k + 1] * dhcar[...] + mm(kt_ref[KEY:, rows], dye)

    for k in range(blocks):
        rows = slice(k * BLK, (k + 1) * BLK)
        for q in range(GC // KEY):
            cols = slice(q * KEY, (q + 1) * KEY)
            par = parg[:, cols]
            window = dpad[k * BLK : k * BLK + BLK + 8, cols]
            out = par[3:4] * window[0:BLK]
            for t in range(3):
                out = out + par[t : t + 1] * window[3 - t : 3 - t + BLK]
            draw_ref[rows, cols] = out.astype(bf16)


def backward_shared(
    rawk_ref, dtr_ref, pv_ref, key_at, ph_ref, kb_ref, dkeys_ref, ddt_ref, sk_ref, sh_ref,
    padk, dpadk, dsc, dkb, dsrow, dscol, ddt,
):
    length = rawk_ref.shape[0]
    blocks = length // BLK
    row = iota((BLK, BLK), 0)
    col = iota((BLK, BLK), 1)
    padk[0:8] = jnp.zeros((8, 2 * KEY), f32)
    padk[8:] = rawk_ref[...]
    dpadk[length:] = jnp.zeros((8, 2 * KEY), f32)
    sk_ref[...] = jnp.zeros_like(sk_ref)
    sh_ref[...] = jnp.zeros_like(sh_ref)
    upper = jnp.where(row <= col, 1.0, 0.0).astype(f32)
    par = pv_ref[:, key_at : key_at + 2 * KEY]
    for k in range(blocks):
        rows = slice(k * BLK, (k + 1) * BLK)
        window = padk[k * BLK : k * BLK + BLK + 8]
        u = taps_of(window, par)
        su = sigmoid(u)
        ds = dsc[k].astype(bf16)
        db = dkb[rows, :KEY] + mm_tn(ds, kb_ref[rows, KEY:])
        dc = dkb[rows, KEY:] + mm(ds, kb_ref[rows, :KEY])
        du = jnp.concatenate([db, dc], axis=1) * (su + u * su * (1.0 - su))
        dpadk[rows] = du
        sk_ref[4:5] += jnp.sum(du, axis=0, keepdims=True)
        for t in range(4):
            sk_ref[t : t + 1] += jnp.sum(du * window[5 + t : 133 + t], axis=0, keepdims=True)
        dla = mm_hi(upper, dsrow[rows] - dscol[:, rows].T)
        z = dtr_ref[rows] + ph_ref[0:1, :]
        rate = jnp.exp(ph_ref[1:2, :])
        dt = jax.nn.softplus(z)
        sh_ref[1:2] += jnp.sum(dla * (-dt * rate), axis=0, keepdims=True)
        dz = (ddt[rows] - dla * rate) * sigmoid(z)
        sh_ref[0:1] += jnp.sum(dz, axis=0, keepdims=True)
        ddt_ref[rows] = dz.astype(bf16)
    for k in range(blocks):
        rows = slice(k * BLK, (k + 1) * BLK)
        window = dpadk[k * BLK : k * BLK + BLK + 8]
        out = par[3:4] * window[0:BLK]
        for t in range(3):
            out = out + par[t : t + 1] * window[3 - t : 3 - t + BLK]
        dkeys_ref[rows] = out.astype(bf16)


def bwd_kernel(
    gate_ref, rawv_ref, rawk_ref, dtr_ref, pv_ref, ph_ref,
    y_ref, gg_ref, hst_ref, r_ref, c_ref, s_ref, st_ref, hl_ref, ehl_ref, kb_ref, kt_ref, sc_ref,
    dproj_ref, sv_ref, sk_ref, sh_ref,
    pad, padk, dpad, dpadk, sg, dhcar, dsc, dkb, dsrow, dscol, ddt,
):
    g = pl.program_id(0)
    length, total = dproj_ref.shape
    wide = GC * pl.num_programs(0)
    shared = (s_ref, st_ref, hl_ref, ehl_ref, kb_ref, kt_ref, sc_ref)

    @pl.when(g == 0)
    def _():
        backward_start(length, pad, dpad, dsc, dkb, dsrow, dscol, ddt)

    gate_at = pl.ds(pl.multiple_of(g * GC, GC), GC)
    draw_at = pl.ds(pl.multiple_of(wide + g * GC, GC), GC)
    backward_group(
        g, gate_ref, rawv_ref, y_ref, gg_ref, hst_ref, r_ref, c_ref, pv_ref, shared,
        dproj_ref.at[:, gate_at], dproj_ref.at[:, draw_at], sv_ref,
        pad, dpad, sg, dhcar, dsc, dkb, dsrow, dscol, ddt,
    )

    @pl.when(g == pl.num_programs(0) - 1)
    def _():
        keys = 2 * wide
        dproj_ref[:, keys + 3 * KEY :] = jnp.zeros((length, total - keys - 3 * KEY), bf16)
        backward_shared(
            rawk_ref, dtr_ref, pv_ref, wide, ph_ref, kb_ref,
            dproj_ref.at[:, keys : keys + 2 * KEY], dproj_ref.at[:, keys + 2 * KEY : keys + 3 * KEY],
            sk_ref, sh_ref, padk, dpadk, dsc, dkb, dsrow, dscol, ddt,
        )


def whole_spec(shape):
    return pl.BlockSpec(shape, lambda g: (0,) * len(shape))


def state_specs(length):
    return (
        ((length, KEY), f32),
        ((KEY, length), f32),
        ((3, length, 2 * KEY), bf16),
        ((8, 2 * KEY), bf16),
        ((length, 2 * KEY), bf16),
        ((2 * KEY, length), bf16),
        ((length // BLK, BLK, BLK), f32),
    )


def proj_specs(length, groups):
    wide = groups * GC
    return [
        pl.BlockSpec((length, GC), lambda g: (0, g)),
        pl.BlockSpec((length, GC), lambda g: (0, groups + g)),
        pl.BlockSpec((length, 2 * KEY), lambda g: (0, 2 * wide // (2 * KEY))),
        pl.BlockSpec((length, KEY), lambda g: (0, 2 * wide // KEY + 2)),
        whole_spec((8, wide + 2 * KEY)),
        whole_spec((8, KEY)),
    ]


def mixer_forward(projected, pv, ph):
    length = projected.shape[0]
    wide = pv.shape[1] - 2 * KEY
    groups = wide // GC
    blocks = length // BLK
    column = pl.BlockSpec((length, GC), lambda g: (0, g))
    shared = state_specs(length)
    return pl.pallas_call(
        fwd_kernel,
        grid=(groups,),
        in_specs=proj_specs(length, groups),
        out_specs=[
            column,
            whole_spec((length, wide)),
            pl.BlockSpec((blocks, KEY, GC), lambda g: (0, 0, g)),
            whole_spec((length, KEY)),
        ]
        + [whole_spec(shape) for shape, _ in shared],
        out_shape=[
            jax.ShapeDtypeStruct((length, wide), f32),
            jax.ShapeDtypeStruct((length, wide), f32),
            jax.ShapeDtypeStruct((blocks, KEY, wide), bf16),
            jax.ShapeDtypeStruct((length, KEY), f32),
        ]
        + [jax.ShapeDtypeStruct(shape, dtype) for shape, dtype in shared],
        scratch_shapes=[
            pltpu.VMEM((length + 8, GC), f32),
            pltpu.VMEM((length + 8, 2 * KEY), f32),
            pltpu.VMEM((length, KEY), f32),
            pltpu.VMEM((KEY, GC), f32),
            pltpu.VMEM((length, KEY), f32),
        ],
        name="mixer_forward",
    )(projected, projected, projected, projected, pv, ph)


def backward_scratch(length):
    return [
        pltpu.VMEM((length + 8, GC), f32),
        pltpu.VMEM((length + 8, 2 * KEY), f32),
        pltpu.VMEM((length + 8, GC), f32),
        pltpu.VMEM((length + 8, 2 * KEY), f32),
        pltpu.VMEM((length, KEY), f32),
        pltpu.VMEM((KEY, GC), f32),
        pltpu.VMEM((length // BLK, BLK, BLK), f32),
        pltpu.VMEM((length, 2 * KEY), f32),
        pltpu.VMEM((length, KEY), f32),
        pltpu.VMEM((KEY, length), f32),
        pltpu.VMEM((length, KEY), f32),
    ]


def mixer_backward(projected, pv, ph, mixed, grad_gated, states, inverse, pull, shared):
    length, total = projected.shape
    wide = pv.shape[1] - 2 * KEY
    groups = wide // GC
    blocks = length // BLK
    column = pl.BlockSpec((length, GC), lambda g: (0, g))
    return pl.pallas_call(
        bwd_kernel,
        grid=(groups,),
        in_specs=proj_specs(length, groups)
        + [
            column,
            column,
            pl.BlockSpec((blocks, KEY, GC), lambda g: (0, 0, g)),
            whole_spec((length, KEY)),
            whole_spec((length, KEY)),
        ]
        + [whole_spec(shape) for shape, _ in state_specs(length)],
        out_specs=[
            whole_spec((length, total)),
            pl.BlockSpec((8, GC), lambda g: (0, g)),
            whole_spec((8, 2 * KEY)),
            whole_spec((8, KEY)),
        ],
        out_shape=[
            jax.ShapeDtypeStruct((length, total), bf16),
            jax.ShapeDtypeStruct((8, wide), f32),
            jax.ShapeDtypeStruct((8, 2 * KEY), f32),
            jax.ShapeDtypeStruct((8, KEY), f32),
        ],
        scratch_shapes=backward_scratch(length),
        name="mixer_backward",
    )(projected, projected, projected, projected, pv, ph, mixed, grad_gated, states, inverse, pull, *shared)


MESH = pl.DeviceIdType.MESH
HALF = 256


def places():
    d, f = lax.axis_index("dp"), lax.axis_index("fsdp")
    z, x, y, c = d // 2, d % 2, f // 2, f % 2
    over_core = (d, y * 2 + 1 - c)
    over_x = (z * 2 + 1 - x, f)
    over_y = (d, (1 - y) * 2 + c)
    near = ((z + 1 - 2 * (z % 2)) * 2 + x, f)
    far = (((z + 2) % 4) * 2 + x, f)
    peers = ((over_core, over_x, over_y, near, far), (over_core, over_y, over_x, near, far))
    own = ((c, x, y, z % 2, z // 2), (c, y, x, z % 2, z // 2))
    return peers, own


def greet(partners):
    barrier = pltpu.get_barrier_semaphore()
    for partner in partners:
        pl.semaphore_signal(barrier, inc=1, device_id=partner, device_id_type=MESH)
    pl.semaphore_wait(barrier, len(partners))


def block_order(half, i):
    z, x, y, c = i // 8, i // 4 % 2, i // 2 % 2, i % 2
    first, second = (x, y) if half == 0 else (y, x)
    return c, first * 8 + second * 4 + z % 2 * 2 + z // 2


def spread_lanes(tiles, width, lane, count):
    out = [jnp.zeros(tiles[0].shape, f32) for _ in range(count)]
    for i, tile in enumerate(tiles):
        at, shift = divmod(i * width, KEY)
        turned = pltpu.roll(tile, shift, 1) if shift else tile
        end = shift + width
        out[at] = out[at] + jnp.where((lane >= shift) & (lane < end), turned, 0.0)
        if end > KEY:
            out[at + 1] = out[at + 1] + jnp.where(lane < end - KEY, turned, 0.0)
    return out


def forward_kernel(
    n_in, n_out, hidden_ref, cot_ref, live_ref, w_ref, wo_ref, tile_ref, skip_ref, ph_ref,
    w_out, proj_out, mixed_out, states_out, flipped_gated_out, gg_out,
    out_ref, flipped_ref, pv_ref, gain, r_ref, c_ref, s_ref, st_ref, hl_ref, ehl_ref, kb_ref, kt_ref, sc_ref,
    held, tiles, w_stage, wo_stage, proj_stage, mixed_stage, states_stage, flip_stage, normed, gated, big,
    pad, padk, sg, hcar, ssq, dots,
    send, recv, tile_sem, out_sem,
):
    rb = w_ref.shape[0]
    length, width = hidden_ref.shape
    wide = big.shape[1]
    n = n_in + n_out
    peers, own = places()
    greet(peers[0])
    base = [sum(bit * (16 >> k) for k, bit in enumerate(own[h])) for h in range(2)]
    count = (1, 2, 4, 8, 16)

    def columns(i, half):
        group = (i - 1) * HALF + half * wide
        return pl.ds(pl.multiple_of(jnp.where(i == 0, 2 * wide + half * HALF, group), HALF), HALF)

    def copy(stage, i, half):
        start = base[half] // count[stage] * count[stage]
        block = held.at[i, half, pl.ds(start, count[stage])]
        return pltpu.make_async_remote_copy(
            src_ref=block,
            dst_ref=block,
            send_sem=send.at[i, half, stage],
            recv_sem=recv.at[i, half, stage],
            device_id=peers[half][4 - stage],
            device_id_type=MESH,
        )

    def tile_copy(stage):
        block = tiles.at[pl.ds(base[0] // count[stage] * count[stage], count[stage])]
        return pltpu.make_async_remote_copy(
            src_ref=block,
            dst_ref=block,
            send_sem=tile_sem.at[0, stage],
            recv_sem=tile_sem.at[1, stage],
            device_id=peers[0][4 - stage],
            device_id_type=MESH,
        )

    def weight_stores(i):
        slot = lax.rem(i, 2)
        copies = []
        for half in range(2):
            cols = slice(half * HALF, (half + 1) * HALF)
            copies.append(
                pltpu.make_async_copy(
                    w_stage.at[slot, :, cols], w_out.at[:, columns(i, half)], out_sem.at[half, slot]
                )
            )
            copies.append(
                pltpu.make_async_copy(
                    proj_stage.at[slot, :, cols], proj_out.at[:, columns(i, half)], out_sem.at[2 + half, slot]
                )
            )
        return copies

    def group_stores(i):
        slot = lax.rem(i, 2)
        cols = pl.ds(pl.multiple_of((i - 1) * HALF, HALF), HALF)
        return (
            pltpu.make_async_copy(mixed_stage.at[slot], mixed_out.at[:, cols], out_sem.at[4, slot]),
            pltpu.make_async_copy(states_stage.at[slot], states_out.at[:, :, cols], out_sem.at[5, slot]),
        )

    def flip_store(k):
        return pltpu.make_async_copy(
            flip_stage.at[k % 2], flipped_gated_out.at[k * HALF : (k + 1) * HALF], out_sem.at[6, k % 2]
        )

    tiles[base[0]] = tile_ref[...]
    tile_copy(0).start()

    def land(i, carry):
        for half in range(2):
            held[i, half, base[half]] = w_ref[:, columns(i, half)]
        return carry

    lax.fori_loop(0, n_in, land, 0)
    for j in range(n_out):
        for half in range(2):
            held[n_in + j, half, base[half]] = wo_ref[half * rb : (half + 1) * rb, j * HALF : (j + 1) * HALF]

    def keys_chunk(slot):
        lane = iota((8, KEY), 1)
        row = iota((8, KEY), 0)
        order = [tiles[c * 16 + at] for c, at in (block_order(0, i) for i in range(32))]
        conv = spread_lanes(order, (wide + 2 * KEY) // 32, lane, wide // KEY + 2)
        gate = spread_lanes(order, wide // 32, lane, wide // KEY)
        pre = spread_lanes(order, width // 32, lane, width // KEY)
        for k, tile in enumerate(conv):
            cols = slice(k * KEY, (k + 1) * KEY)
            if k < wide // KEY:
                tile = jnp.where(row == 5, gate[k], jnp.where(row == 6, skip_ref[:, cols], tile))
            pv_ref[:, cols] = tile
        for k, tile in enumerate(pre):
            gain[:, k * KEY : (k + 1) * KEY] = tile
        for k in range(0, length, KEY):
            values = hidden_ref[k : k + KEY].astype(f32)
            mean = jnp.mean(values * values, axis=1, keepdims=True)
            rows = (values * lax.rsqrt(mean + epsilon) * gain[6:7]).astype(bf16)
            normed[k : k + KEY] = rows
            flipped_ref[:, k : k + KEY] = rows.T
        project(slot)
        forward_shared(
            proj_stage.at[slot, :, 0:HALF], proj_stage.at[slot, :, HALF : HALF + KEY], pv_ref, wide, ph_ref,
            s_ref, st_ref, hl_ref, ehl_ref, kb_ref, kt_ref, sc_ref, padk,
        )
        pad[0:8] = jnp.zeros((8, GC), f32)
        ssq[...] = jnp.zeros_like(ssq)
        dots[...] = jnp.zeros_like(dots)

    def project(slot):
        for half in range(2):
            cols = slice(half * HALF, (half + 1) * HALF)
            proj_stage[slot, :, cols] = mm(normed[...], w_stage[slot, :, cols])

    def group_chunk(slot, g):
        project(slot)
        forward_group(
            g, proj_stage.at[slot, :, 0:HALF], proj_stage.at[slot, :, HALF : 2 * HALF], pv_ref,
            s_ref, st_ref, hl_ref, ehl_ref, kb_ref, kt_ref, sc_ref,
            mixed_stage.at[slot], big, states_stage.at[slot], pad, sg, hcar, ssq,
        )

    def finish_groups():
        mean = jnp.sum(ssq[...], axis=1, keepdims=True) / wide
        r_ref[...] = jnp.broadcast_to(lax.rsqrt(mean + epsilon), r_ref.shape)
        for k in range(wide // HALF):
            if k >= 2:
                flip_store(k - 2).wait()
            for q in range(HALF // KEY):
                cols = slice(k * HALF + q * KEY, k * HALF + (q + 1) * KEY)
                part = (big[:, cols] * r_ref[...] * pv_ref[5:6, cols]).astype(bf16)
                gated[:, cols] = part
                flip_stage[k % 2, q * KEY : (q + 1) * KEY] = part.T
            flip_store(k).start()
        for k in range(wide // HALF - 2, wide // HALF):
            flip_store(k).wait()

    def out_chunk(i):
        j = i - n_in
        for b in range(32):
            for half in range(2):
                c, at = block_order(half, b)
                wo_stage[(2 * b + half) * rb : (2 * b + half + 1) * rb] = held[i, half, c * 16 + at]
        cols = pl.ds(pl.multiple_of(j * HALF, HALF), HALF)
        branch = mm(gated[...], wo_stage[...])
        live = jnp.concatenate([live_ref[...]] * (HALF // KEY), axis=1)
        out_ref[:, cols] = (hidden_ref[:, cols].astype(f32) + live * branch).astype(bf16)
        upstream = (cot_ref[:, cols].astype(f32) * live).astype(bf16)
        dots[...] += upstream.astype(f32) * branch
        for q in range(0, wide, 512):
            more = mm_nt(upstream, wo_stage[q : q + 512])

            @pl.when(j == 0)
            def _():
                big[:, q : q + 512] = more

            @pl.when(j > 0)
            def _():
                big[:, q : q + 512] += more

    def consume(i):
        slot = lax.rem(i, 2)

        @pl.when(i < n_in)
        def _():
            @pl.when(i >= 2)
            def _():
                for store in weight_stores(i - 2):
                    store.wait()

            for half in range(2):
                for b in range(32):
                    c, at = block_order(half, b)
                    w_stage[slot, b * rb : (b + 1) * rb, half * HALF : (half + 1) * HALF] = held[i, half, c * 16 + at]

            @pl.when(i == 0)
            def _():
                keys_chunk(slot)

            @pl.when(i > 0)
            def _():
                @pl.when(i >= 3)
                def _():
                    for store in group_stores(i - 2):
                        store.wait()

                group_chunk(slot, i - 1)
                for store in group_stores(i):
                    store.start()

            for store in weight_stores(i):
                store.start()

            @pl.when(i == n_in - 1)
            def _():
                finish_groups()

        @pl.when(i >= n_in)
        def _():
            out_chunk(i)

    def tick(t, carry):
        @pl.when(t < n)
        def _():
            for half in range(2):
                copy(0, t, half).start()

        for stage in range(5):
            i = t - stage - 1

            @pl.when(i == 0)
            def _(stage=stage):
                tile_copy(stage).wait()
                if stage < 4:
                    tile_copy(stage + 1).start()

            @pl.when((i >= 0) & (i < n))
            def _(stage=stage, i=i):
                for half in range(2):
                    copy(stage, i, half).wait()
                    if stage < 4:
                        copy(stage + 1, i, half).start()
                if stage == 4:
                    consume(i)

        return carry

    lax.fori_loop(0, n + 5, tick, 0)
    whole = pltpu.make_async_copy(big, gg_out, out_sem.at[6, 0])
    whole.start()
    pull = jnp.sum(dots[...], axis=1, keepdims=True) / wide
    c_ref[...] = r_ref[...] * r_ref[...] * pull
    for i in (n_in - 2, n_in - 1):
        for store in weight_stores(i) + list(group_stores(i)):
            store.wait()
    whole.wait()


def gather_forward(hidden, cotangent, live, shard, out_shard, tile, skip_rows, ph):
    length, width = hidden.shape
    rb, columns = shard.shape
    wide = out_shard.shape[0] * 32
    n_in, n_out = columns // (2 * HALF), width // HALF
    blocks = length // BLK
    vmem = pl.BlockSpec(memory_space=pltpu.VMEM)
    anywhere = pl.BlockSpec(memory_space=pl.ANY)
    struct = jax.ShapeDtypeStruct
    shared = [struct(shape, dtype) for shape, dtype in state_specs(length)]
    return pl.pallas_call(
        partial(forward_kernel, n_in, n_out),
        out_shape=[
            struct((width, columns), bf16),
            struct((length, columns), f32),
            struct((length, wide), f32),
            struct((blocks, KEY, wide), bf16),
            struct((wide, length), bf16),
            struct((length, wide), f32),
            struct((length, width), bf16),
            struct((width, length), bf16),
            struct((8, wide + 2 * KEY), f32),
            struct((8, width), f32),
            struct((length, KEY), f32),
            struct((length, KEY), f32),
        ]
        + shared,
        in_specs=[vmem] * 8,
        out_specs=[anywhere] * 6 + [vmem] * (6 + len(shared)),
        scratch_shapes=[
            pltpu.VMEM((n_in + n_out, 2, 32, rb, HALF), bf16),
            pltpu.VMEM((32, 8, KEY), f32),
            pltpu.VMEM((2, width, 2 * HALF), bf16),
            pltpu.VMEM((wide, HALF), bf16),
            pltpu.VMEM((2, length, 2 * HALF), f32),
            pltpu.VMEM((2, length, HALF), f32),
            pltpu.VMEM((2, blocks, KEY, HALF), bf16),
            pltpu.VMEM((2, HALF, length), bf16),
            pltpu.VMEM((length, width), bf16),
            pltpu.VMEM((length, wide), bf16),
            pltpu.VMEM((length, wide), f32),
            pltpu.VMEM((length + 8, GC), f32),
            pltpu.VMEM((length + 8, 2 * KEY), f32),
            pltpu.VMEM((length, KEY), f32),
            pltpu.VMEM((KEY, GC), f32),
            pltpu.VMEM((length, KEY), f32),
            pltpu.VMEM((length, HALF), f32),
            pltpu.SemaphoreType.DMA((n_in + n_out, 2, 5)),
            pltpu.SemaphoreType.DMA((n_in + n_out, 2, 5)),
            pltpu.SemaphoreType.DMA((2, 5)),
            pltpu.SemaphoreType.DMA((7, 2)),
        ],
        compiler_params=pltpu.CompilerParams(
            collective_id=2, has_side_effects=True, vmem_limit_bytes=63 << 20
        ),
        name="gather_forward",
    )(hidden, cotangent, live, shard, out_shard, tile, skip_rows, ph)


def scatter_kernel(
    n, rb, lhs_ref, rhs_ref, tile_ref, head_ref, out_ref, tile_out, sums_ref,
    parts, r0, r1, r2, r3, r4, tiles, t0, t1, t2, t3, t4, sums, sums_in, send, recv, tile_sem, sums_sem,
):
    peers, own = places()
    held = (r0, r1, r2, r3, r4)
    tile_held = (t0, t1, t2, t3, t4)
    greet(peers[0])

    def sums_copy(stage):
        return pltpu.make_async_remote_copy(
            src_ref=sums.at[stage],
            dst_ref=sums_in.at[stage],
            send_sem=sums_sem.at[0, stage],
            recv_sem=sums_sem.at[1, stage],
            device_id=peers[0][stage],
            device_id_type=MESH,
        )

    def tile_copy(stage):
        count = 16 >> stage
        source = (tiles,) + tile_held
        return pltpu.make_async_remote_copy(
            src_ref=source[stage].at[pl.ds((1 - own[0][stage]) * count, count)],
            dst_ref=tile_held[stage],
            send_sem=tile_sem.at[0, stage],
            recv_sem=tile_sem.at[1, stage],
            device_id=peers[0][stage],
            device_id_type=MESH,
        )

    sums[0] = head_ref[...]
    sums_copy(0).start()
    for i in range(32):
        c, at = block_order(0, i)
        tiles[c * 16 + at] = tile_ref[i]
    tile_copy(0).start()

    def copy(stage, i, half):
        count = 16 >> stage
        if stage == 0:
            src = parts.at[lax.rem(i, 2), 1 - own[half][0], half]
        else:
            src = held[stage - 1].at[i, half, pl.ds((1 - own[half][stage]) * count, count)]
        return pltpu.make_async_remote_copy(
            src_ref=src,
            dst_ref=held[stage].at[i, half],
            send_sem=send.at[i, half, stage],
            recv_sem=recv.at[i, half, stage],
            device_id=peers[half][stage],
            device_id_type=MESH,
        )

    def tick(t, carry):
        @pl.when(t < n)
        def _():
            slot = lax.rem(t, 2)

            @pl.when(t >= 2)
            def _():
                for half in range(2):
                    copy(0, t - 2, half).wait_send()

            for half in range(2):
                cols = pl.ds(pl.multiple_of(t * 2 * HALF + half * HALF, HALF), HALF)
                right = rhs_ref[:, cols]
                for z in range(4):
                    res = mm(lhs_ref[z * 8 * rb : (z + 1) * 8 * rb], right)
                    for b in range(8):
                        c, at = block_order(half, z * 8 + b)
                        parts[slot, c, half, at] = res[b * rb : (b + 1) * rb].astype(bf16)
            for half in range(2):
                copy(0, t, half).start()

        for stage in range(5):
            i = t - stage - 1

            @pl.when(i == 0)
            def _(stage=stage):
                count = 16 >> stage
                sums_copy(stage).wait()
                tile_copy(stage).wait()
                total = tile_held[stage][...] + ((tiles,) + tile_held)[stage][pl.ds(own[0][stage] * count, count)]
                if stage < 4:
                    sums[stage + 1] = sums[stage] + sums_in[stage]
                    sums_copy(stage + 1).start()
                    tile_held[stage][...] = total
                    tile_copy(stage + 1).start()
                else:
                    sums_ref[...] = sums[stage] + sums_in[stage]
                    tile_out[...] = total[0]

            @pl.when((i >= 0) & (i < n))
            def _(stage=stage, i=i):
                count = 16 >> stage
                for half in range(2):
                    done = copy(stage, i, half)
                    if stage == 0:
                        done.wait_recv()
                        mine = parts[lax.rem(i, 2), own[half][0], half]
                    else:
                        done.wait()
                        mine = held[stage - 1][i, half, pl.ds(own[half][stage] * count, count)]
                    if stage < 4:
                        held[stage][i, half] = (
                            held[stage][i, half].astype(f32) + mine.astype(f32)
                        ).astype(bf16)
                        copy(stage + 1, i, half).start()
                    else:
                        cols = pl.ds(pl.multiple_of(i * 2 * HALF + half * HALF, HALF), HALF)
                        out_ref[:, cols] = held[stage][i, half, 0].astype(f32) + mine[0].astype(f32)

        return carry

    lax.fori_loop(0, n + 5, tick, 0)
    for i in (n - 2, n - 1):
        for half in range(2):
            copy(0, i, half).wait_send()


def scatter_product(lhs, rhs, tiles, heads):
    rows, depth = lhs.shape
    columns = rhs.shape[1]
    n, rb = columns // (2 * HALF), rows // 32
    vmem = pl.BlockSpec(memory_space=pltpu.VMEM)
    return pl.pallas_call(
        partial(scatter_kernel, n, rb),
        out_shape=(
            jax.ShapeDtypeStruct((rb, columns), f32),
            jax.ShapeDtypeStruct(tiles.shape[1:], f32),
            jax.ShapeDtypeStruct(heads.shape, f32),
        ),
        in_specs=[vmem] * 4,
        out_specs=(vmem, vmem, vmem),
        scratch_shapes=[pltpu.VMEM((2, 2, 2, 16, rb, HALF), bf16)]
        + [pltpu.VMEM((n, 2, 16 >> stage, rb, HALF), bf16) for stage in range(5)]
        + [pltpu.VMEM(((32 >> stage),) + tiles.shape[1:], f32) for stage in range(6)]
        + [pltpu.VMEM((5,) + heads.shape, f32)] * 2
        + [pltpu.SemaphoreType.DMA((n, 2, 5))] * 2
        + [pltpu.SemaphoreType.DMA((2, 5))] * 2,
        compiler_params=pltpu.CompilerParams(
            collective_id=1, has_side_effects=True, vmem_limit_bytes=60 << 20
        ),
        name="scatter_product",
    )(lhs, rhs, tiles, heads)


def pre_norm_inverse(rows):
    return lax.rsqrt(jnp.mean(rows * rows, axis=1, keepdims=True) + epsilon)


AXES = ("dp", "fsdp")


def gather_rows(shard):
    return lax.all_gather(shard, AXES, axis=0, tiled=True)


def scatter_rows(whole):
    return lax.psum_scatter(whole, AXES, scatter_dimension=0, tiled=True)


def vector_tile(conv_weight, conv_bias, gate_gain, norm_gain):
    rows = [conv_weight, conv_bias[None], gate_gain[None], norm_gain[None]]
    rows = [jnp.pad(row.astype(f32), ((0, 0), (0, KEY - row.shape[1]))) for row in rows]
    return jnp.concatenate(rows + [jnp.zeros((1, KEY), f32)], axis=0)


def vector_tiles(conv, gate, pre, parts):
    rows = []
    for whole in (conv, gate, pre):
        part = whole.shape[1] // parts
        split_up = jnp.transpose(whole.reshape(-1, parts, part), (1, 0, 2))
        rows.append(jnp.pad(split_up, ((0, 0), (0, 0), (0, KEY - part))))
    return jnp.concatenate(rows + [jnp.zeros((parts, 1, KEY), f32)], axis=1)


def shards(
    kernels, hidden, cotangent, lengths, norm_gain, in_proj, dt_proj, conv_weight, conv_bias,
    dt_bias, a_log, skip_gain, gate_gain, out_proj,
):
    length, width = hidden.shape
    assert lengths.shape[0] == 1
    rows_in, columns = in_proj.shape
    heads = dt_bias.shape[0]
    parts = width // rows_in
    taps, conv_part = conv_weight.shape
    gate_part = gate_gain.shape[0]
    wide = gate_part * parts
    total = columns + 2 * KEY

    fill = jnp.zeros((rows_in, total - columns - heads), bf16)
    packed = jnp.concatenate([in_proj, dt_proj, fill], axis=1)
    tile = vector_tile(conv_weight, conv_bias, gate_gain, norm_gain)
    ph = jnp.pad(jnp.stack([dt_bias, a_log]).astype(f32), ((0, 6), (0, KEY - heads)))
    skip_wide = jnp.repeat(skip_gain.astype(f32), HD)[None]
    live = (jnp.arange(length) < lengths[0]).astype(f32)[:, None]
    rows_wide = hidden.astype(f32)
    cot_wide = cotangent.astype(f32)
    upstream = (cot_wide * live).astype(bf16)
    inverse_one = pre_norm_inverse(rows_wide)
    if kernels:
        skip_rows = jnp.broadcast_to(skip_wide, (8, wide))
        (
            w_in, projected, mixed, states, gated_flipped, grad_gated, output, flipped, pv, gains, inverse_two, pull,
            *shared,
        ) = gather_forward(
            hidden, cotangent, jnp.broadcast_to(live, (length, KEY)), packed, out_proj, tile, skip_rows, ph
        )
        gain_one = gains[6]
        grad_out = mm(gated_flipped, upstream)
    else:
        w_in, w_out = gather_rows(packed), gather_rows(out_proj)
        tiles = gather_rows(tile[None])
        whole = lambda rows, part: jnp.transpose(tiles[:, rows, :part], (1, 0, 2)).reshape(-1, parts * part)
        conv_all = whole(slice(0, 5), conv_part)
        gain_two = whole(slice(5, 6), gate_part)
        gain_one = whole(slice(6, 7), rows_in)[0]
        rest = jnp.concatenate([gain_two, skip_wide, jnp.zeros((1, wide), f32)], axis=0)
        pv = jnp.concatenate([conv_all, jnp.pad(rest, ((0, 0), (0, 2 * KEY)))], axis=0)
        normed = (rows_wide * inverse_one * gain_one[None, :]).astype(bf16)
        projected = mm(normed, w_in)
        mixed, product, states, inverse_two, *shared = mixer_forward(projected, pv, ph)
        inv = inverse_two[:, :1]
        gated = (product * inv * gain_two).astype(bf16)
        output = (rows_wide + live * mm(gated, w_out)).astype(bf16)
        grad_gated = mm_nt(upstream, w_out)
        pull = jnp.sum(grad_gated * gain_two * product, axis=1, keepdims=True)
        pull = jnp.broadcast_to(inv * inv * inv * pull / wide, inverse_two.shape)
        grad_out = mm_tn(gated, upstream)
    grad_proj, sums_v, sums_k, sums_h = mixer_backward(
        projected, pv, ph, mixed, grad_gated, states, inverse_two, pull, shared
    )
    skip_grad = jnp.pad(jnp.sum(sums_v[6].reshape(heads, HD), axis=1), (0, KEY - heads))[None]
    head_grads = jnp.concatenate([sums_h[:2], skip_grad, jnp.zeros((5, KEY), f32)], axis=0)

    grad_normed = mm_nt(grad_proj, w_in)
    scaled = grad_normed * gain_one[None, :]
    row_sums = jnp.sum(scaled * rows_wide, axis=1, keepdims=True) / width
    grad_rows = inverse_one * scaled - rows_wide * (inverse_one * inverse_one * inverse_one * row_sums)
    input_grad = cot_wide + grad_rows
    grad_gain_one = jnp.sum(grad_normed * rows_wide * inverse_one, axis=0, keepdims=True)

    conv_grad = jnp.concatenate([sums_v[:5], sums_k[:5]], axis=1)
    small = vector_tiles(conv_grad, sums_v[5:6], grad_gain_one, parts)
    grad_out = scatter_rows(grad_out.astype(bf16)).astype(f32)
    if kernels:
        grad_in, small_sum, head_sums = scatter_product(flipped, grad_proj, small, head_grads)
    else:
        head_sums = lax.psum(head_grads, AXES)
        grad_in = scatter_rows(mm_tn(normed, grad_proj).astype(bf16)).astype(f32)
        small_sum = scatter_rows(small)[0]
    return (
        output,
        input_grad,
        small_sum[6, :rows_in],
        grad_in[:, :columns],
        grad_in[:, columns : columns + heads],
        small_sum[:taps, :conv_part],
        small_sum[taps, :conv_part],
        head_sums[0, :heads],
        head_sums[1, :heads],
        head_sums[2, :heads],
        small_sum[5, :gate_part],
        grad_out,
    )


def solution(mesh):
    rows = P(AXES, None)
    vector = P(AXES)
    last = P(None, AXES)
    return jax.shard_map(
        partial(shards, mesh.shape["dp"] == 8 and mesh.shape["fsdp"] == 4),
        mesh=mesh,
        in_specs=(rows, rows, vector, vector, rows, rows, last, vector, P(), P(), P(), vector, rows),
        out_specs=(rows, rows, vector, rows, rows, last, vector, P(), P(), P(), vector, rows),
        check_vma=False,
    )
```

```python
from functools import partial

import jax
import jax.numpy as jnp
from jax import lax
from jax.experimental import pallas as pl
from jax.experimental.pallas import tpu as pltpu
from jax.sharding import PartitionSpec as P

f32 = jnp.float32
bf16 = jnp.bfloat16
epsilon = 1e-05
highest = lax.Precision.HIGHEST
BLK = 128
GH = 4
HD = 64
GC = GH * HD
KEY = 128
NEG = -1e30


def sigmoid(v):
    return 0.5 * jnp.tanh(0.5 * v) + 0.5


def mm(a, b):
    return lax.dot_general(a, b, (((1,), (0,)), ((), ())), preferred_element_type=f32)


def mm_nt(a, b):
    return lax.dot_general(a, b, (((1,), (1,)), ((), ())), preferred_element_type=f32)


def mm_tn(a, b):
    return lax.dot_general(a, b, (((0,), (0,)), ((), ())), preferred_element_type=f32)


def mm_hi(a, b, dims=((1,), (0,))):
    return lax.dot_general(a, b, (dims, ((), ())), preferred_element_type=f32, precision=highest)


def split(v):
    hi = v.astype(bf16)
    lo = (v - hi.astype(f32)).astype(bf16)
    return jnp.concatenate([hi, lo], axis=1)


def iota(shape, dim):
    return lax.broadcasted_iota(jnp.int32, shape, dim)


def expander(g):
    rows = iota((2 * KEY, GC), 0)
    cols = iota((2 * KEY, GC), 1)
    return jnp.where(lax.rem(rows, KEY) == cols // HD + g * GH, 1.0, 0.0).astype(bf16)


def reducer(g):
    rows = iota((GC, KEY), 0)
    cols = iota((GC, KEY), 1)
    return jnp.where(rows // HD + g * GH == cols, 1.0, 0.0).astype(bf16)


def taps_of(window, par):
    out = par[4:5] + par[3:4] * window[8:136]
    for k in range(3):
        out = out + par[k : k + 1] * window[5 + k : 133 + k]
    return out


def group_rows(st_ref, g, half, rows):
    tile = st_ref[pl.ds(pl.multiple_of(g // 2 * 8, 8), 8), rows]
    return jnp.where(half == 0, tile[:GH], tile[GH:])


def forward_shared(
    rawk_ref, dtr_ref, pv_ref, key_at, ph_ref, s_ref, st_ref, hl_ref, ehl_ref, kb_ref, kt_ref, sc_ref, padk
):
    blocks = rawk_ref.shape[0] // BLK
    dt = jax.nn.softplus(dtr_ref[...] + ph_ref[0:1, :])
    la = -dt * jnp.exp(ph_ref[1:2, :])
    tri = jnp.where(iota((BLK, BLK), 0) >= iota((BLK, BLK), 1), 1.0, 0.0).astype(f32)
    hl_ref[0] = split(dt)
    ehl_ref[...] = jnp.zeros_like(ehl_ref)
    padk[0:8] = jnp.zeros((8, 2 * KEY), f32)
    padk[8:] = rawk_ref[...]
    par = pv_ref[:, key_at : key_at + 2 * KEY]
    for k in range(blocks):
        rows = slice(k * BLK, (k + 1) * BLK)
        s = mm_hi(tri, la[rows])
        s_ref[rows] = s
        st_ref[:, rows] = s.T
        hl_ref[1, rows] = split(jnp.exp(s))
        hl_ref[2, rows] = split(jnp.exp(s[BLK - 1 :] - s))
        ehl_ref[k : k + 1] = split(jnp.exp(s[BLK - 1 :]))
        u = taps_of(padk[k * BLK : k * BLK + BLK + 8], par)
        v = u * sigmoid(u)
        kb_ref[rows] = v.astype(bf16)
        kt_ref[:, rows] = v.T.astype(bf16)
        sc_ref[k] = mm_hi(v[:, KEY:], v[:, :KEY], ((1,), (1,)))


def forward_group(
    g, gate_ref, rawv_ref, pv_ref, s_ref, st_ref, hl_ref, ehl_ref, kb_ref, kt_ref, sc_ref,
    y_ref, p_ref, hst_ref, pad, sg, hcar, ssq,
):
    blocks = gate_ref.shape[0] // BLK
    pad[8:] = rawv_ref[...]
    sg[...] = pltpu.roll(s_ref[...], lax.rem(KEY - g * GH, KEY), 1)
    ex = expander(g)
    bias = jnp.where(iota((BLK, BLK), 0) >= iota((BLK, BLK), 1), 0.0, NEG).astype(f32)
    low = iota((BLK, KEY), 1) < HD
    eend = mm(ehl_ref[...], ex)
    parg = pv_ref[:, pl.ds(pl.multiple_of(g * GC, GC), GC)]
    half = lax.rem(g, 8 // GH)
    hcar[...] = jnp.zeros_like(hcar)
    for k in range(blocks):
        rows = slice(k * BLK, (k + 1) * BLK)
        dtx = mm(hl_ref[0, rows], ex)
        exx = mm(hl_ref[1, rows], ex)
        txx = mm(hl_ref[2, rows], ex)
        hb = hcar[...].astype(bf16)
        hst_ref[k] = hb
        outer = mm(kb_ref[rows, KEY:], hb)
        across = group_rows(st_ref, g, half, rows)
        xts = []
        for q in range(GC // KEY):
            cols = slice(q * KEY, (q + 1) * KEY)
            par = parg[:, cols]
            u = taps_of(pad[k * BLK : k * BLK + BLK + 8, cols], par)
            v = u * sigmoid(u)
            x = v * dtx[:, cols]
            xts.append((x * txx[:, cols]).astype(bf16))
            xb = x.astype(bf16)
            zero = jnp.zeros_like(xb)
            x2 = jnp.concatenate([jnp.where(low, xb, zero), jnp.where(low, zero, xb)], axis=0)
            ms = []
            for side in range(2):
                j = 2 * q + side
                spread = sg[rows, j : j + 1] - across[j : j + 1]
                ms.append((jnp.exp(spread + bias) * sc_ref[k]).astype(bf16))
            y = mm(jnp.concatenate(ms, axis=1), x2)
            y = y + outer[:, cols] * exx[:, cols] + par[6:7] * v
            y_ref[rows, cols] = y
            gate = gate_ref[rows, cols]
            p = y * (gate * sigmoid(gate))
            p_ref[rows, pl.ds(pl.multiple_of(g * GC + q * KEY, KEY), KEY)] = p
            ssq[rows] += p * p
        if k + 1 < blocks:
            hcar[...] = eend[k : k + 1] * hcar[...] + mm(kt_ref[:KEY, rows], jnp.concatenate(xts, axis=1))


def fwd_kernel(
    gate_ref, rawv_ref, rawk_ref, dtr_ref, pv_ref, ph_ref,
    y_ref, p_ref, hst_ref, r_ref, s_ref, st_ref, hl_ref, ehl_ref, kb_ref, kt_ref, sc_ref,
    pad, padk, sg, hcar, ssq,
):
    g = pl.program_id(0)
    wide = p_ref.shape[1]
    shared = (s_ref, st_ref, hl_ref, ehl_ref, kb_ref, kt_ref, sc_ref)

    @pl.when(g == 0)
    def _():
        forward_shared(rawk_ref, dtr_ref, pv_ref, wide, ph_ref, *shared, padk)
        pad[0:8] = jnp.zeros((8, GC), f32)
        ssq[...] = jnp.zeros_like(ssq)

    forward_group(g, gate_ref, rawv_ref, pv_ref, *shared, y_ref, p_ref, hst_ref, pad, sg, hcar, ssq)

    @pl.when(g == pl.num_programs(0) - 1)
    def _():
        mean = jnp.sum(ssq[...], axis=1, keepdims=True) / wide
        r_ref[...] = jnp.broadcast_to(lax.rsqrt(mean + epsilon), r_ref.shape)


def backward_start(length, pad, dpad, dsc, dkb, dsrow, dscol, ddt):
    pad[0:8] = jnp.zeros((8, GC), f32)
    dpad[length:] = jnp.zeros((8, GC), f32)
    for ref in (dsc, dkb, dsrow, dscol, ddt):
        ref[...] = jnp.zeros_like(ref)


def backward_group(
    g, gate_ref, rawv_ref, y_ref, gg_ref, hst_ref, r_ref, c_ref, pv_ref, shared,
    dgate_ref, draw_ref, sv_ref, pad, dpad, sg, dhcar, dsc, dkb, dsrow, dscol, ddt,
):
    s_ref, st_ref, hl_ref, ehl_ref, kb_ref, kt_ref, sc_ref = shared
    blocks = gate_ref.shape[0] // BLK
    pad[8:] = rawv_ref[...]
    sg[...] = pltpu.roll(s_ref[...], lax.rem(KEY - g * GH, KEY), 1)
    ex = expander(g)
    red = reducer(g)
    row = iota((BLK, BLK), 0)
    col = iota((BLK, BLK), 1)
    bias = jnp.where(row >= col, 0.0, NEG).astype(f32)
    strict = row > col
    low = iota((BLK, KEY), 1) < HD
    eend = mm(ehl_ref[...], ex)
    parg = pv_ref[:, pl.ds(pl.multiple_of(g * GC, GC), GC)]
    half = lax.rem(g, 8 // GH)
    tile_at = pl.ds(pl.multiple_of(g // 2 * 8, 8), 8)
    mine = (iota((8, BLK), 0) < GH) == (half == 0)
    dhcar[...] = jnp.zeros_like(dhcar)
    sv_ref[...] = jnp.zeros_like(sv_ref)
    for k in range(blocks - 1, -1, -1):
        rows = slice(k * BLK, (k + 1) * BLK)
        dtx = mm(hl_ref[0, rows], ex)
        exx = mm(hl_ref[1, rows], ex)
        txx = mm(hl_ref[2, rows], ex)
        hb = hst_ref[k]
        dhb = dhcar[...].astype(bf16)
        ch = mm(kb_ref[rows, KEY:], hb)
        qq = mm(kb_ref[rows, :KEY], dhb)
        across = group_rows(st_ref, g, half, rows)
        dyes, xts, zs, oys, ddts, ecols = [], [], [], [], [], []
        dsrow_k = jnp.zeros((BLK, KEY), f32)
        for q in range(GC // KEY):
            cols = slice(q * KEY, (q + 1) * KEY)
            par = parg[:, cols]
            window = pad[k * BLK : k * BLK + BLK + 8, cols]
            u = taps_of(window, par)
            su = sigmoid(u)
            v = u * su
            x = v * dtx[:, cols]
            xb = x.astype(bf16)
            gate = gate_ref[rows, cols]
            y = y_ref[rows, cols]
            sgt = sigmoid(gate)
            silu_g = gate * sgt
            p = y * silu_g
            dgn = gg_ref[rows, cols] * r_ref[rows]
            sv_ref[5:6, cols] += jnp.sum(dgn * p, axis=0, keepdims=True)
            dp = dgn * par[5:6] - p * c_ref[rows]
            dgate_ref[rows, cols] = (dp * y * (sgt + silu_g * (1.0 - sgt))).astype(bf16)
            dy = dp * silu_g
            sv_ref[6:7, cols] += jnp.sum(dy * v, axis=0, keepdims=True)
            dyb = dy.astype(bf16)
            dye = dy * exx[:, cols]
            dyes.append(dye.astype(bf16))
            oys.append((dye * ch[:, cols]).astype(bf16))
            xt = x * txx[:, cols]
            xts.append(xt.astype(bf16))
            zs.append((xt * qq[:, cols]).astype(bf16))
            zero = jnp.zeros_like(dyb)
            dy2 = jnp.concatenate([jnp.where(low, dyb, zero), jnp.where(low, zero, dyb)], axis=0)
            dm2 = mm_nt(dy2, xb)
            ms = []
            for side in range(2):
                j = 2 * q + side
                spread = sg[rows, j : j + 1] - across[j : j + 1]
                decay = jnp.exp(spread + bias)
                m = decay * sc_ref[k]
                ms.append(m.astype(bf16))
                dm = dm2[side * BLK : (side + 1) * BLK]
                dsc[k] += decay * dm
                e = jnp.where(strict, m * dm, 0.0)
                dsrow_k = jnp.where(col == g * GH + j, jnp.sum(e, axis=1, keepdims=True), dsrow_k)
                ecols.append(jnp.sum(e, axis=0, keepdims=True))
            dx = mm_tn(jnp.concatenate(ms, axis=0), dy2) + qq[:, cols] * txx[:, cols]
            dv = dx * dtx[:, cols] + par[6:7] * dy
            ddts.append((dx * v).astype(bf16))
            du = dv * (su + v * (1.0 - su))
            dpad[rows, cols] = du
            sv_ref[4:5, cols] += jnp.sum(du, axis=0, keepdims=True)
            for t in range(4):
                sv_ref[t : t + 1, cols] += jnp.sum(du * window[5 + t : 133 + t], axis=0, keepdims=True)
        dscol[tile_at, rows] += jnp.where(mine, jnp.concatenate(ecols + ecols, axis=0), 0.0)
        dye = jnp.concatenate(dyes, axis=1)
        xt = jnp.concatenate(xts, axis=1)
        zsum = mm(jnp.concatenate(zs, axis=1), red)
        ddt[rows] += mm(jnp.concatenate(ddts, axis=1), red)
        hterm = eend[k : k + 1] * jnp.sum(dhcar[...] * hb.astype(f32), axis=0, keepdims=True)
        end = jnp.sum(zsum, axis=0, keepdims=True) + mm_hi(hterm, red.astype(f32))
        add = dsrow_k + mm(jnp.concatenate(oys, axis=1), red) - zsum
        dsrow[rows] += add + jnp.where(row == BLK - 1, end, 0.0)
        dkb[rows, KEY:] += mm_nt(dye, hb)
        dkb[rows, :KEY] += mm_nt(xt, dhb)
        if k:
            dhcar[...] = eend[k : k + 1] * dhcar[...] + mm(kt_ref[KEY:, rows], dye)

    for k in range(blocks):
        rows = slice(k * BLK, (k + 1) * BLK)
        for q in range(GC // KEY):
            cols = slice(q * KEY, (q + 1) * KEY)
            par = parg[:, cols]
            window = dpad[k * BLK : k * BLK + BLK + 8, cols]
            out = par[3:4] * window[0:BLK]
            for t in range(3):
                out = out + par[t : t + 1] * window[3 - t : 3 - t + BLK]
            draw_ref[rows, cols] = out.astype(bf16)


def backward_shared(
    rawk_ref, dtr_ref, pv_ref, key_at, ph_ref, kb_ref, dkeys_ref, ddt_ref, sk_ref, sh_ref,
    padk, dpadk, dsc, dkb, dsrow, dscol, ddt,
):
    length = rawk_ref.shape[0]
    blocks = length // BLK
    row = iota((BLK, BLK), 0)
    col = iota((BLK, BLK), 1)
    padk[0:8] = jnp.zeros((8, 2 * KEY), f32)
    padk[8:] = rawk_ref[...]
    dpadk[length:] = jnp.zeros((8, 2 * KEY), f32)
    sk_ref[...] = jnp.zeros_like(sk_ref)
    sh_ref[...] = jnp.zeros_like(sh_ref)
    upper = jnp.where(row <= col, 1.0, 0.0).astype(f32)
    par = pv_ref[:, key_at : key_at + 2 * KEY]
    for k in range(blocks):
        rows = slice(k * BLK, (k + 1) * BLK)
        window = padk[k * BLK : k * BLK + BLK + 8]
        u = taps_of(window, par)
        su = sigmoid(u)
        ds = dsc[k].astype(bf16)
        db = dkb[rows, :KEY] + mm_tn(ds, kb_ref[rows, KEY:])
        dc = dkb[rows, KEY:] + mm(ds, kb_ref[rows, :KEY])
        du = jnp.concatenate([db, dc], axis=1) * (su + u * su * (1.0 - su))
        dpadk[rows] = du
        sk_ref[4:5] += jnp.sum(du, axis=0, keepdims=True)
        for t in range(4):
            sk_ref[t : t + 1] += jnp.sum(du * window[5 + t : 133 + t], axis=0, keepdims=True)
        dla = mm_hi(upper, dsrow[rows] - dscol[:, rows].T)
        z = dtr_ref[rows] + ph_ref[0:1, :]
        rate = jnp.exp(ph_ref[1:2, :])
        dt = jax.nn.softplus(z)
        sh_ref[1:2] += jnp.sum(dla * (-dt * rate), axis=0, keepdims=True)
        dz = (ddt[rows] - dla * rate) * sigmoid(z)
        sh_ref[0:1] += jnp.sum(dz, axis=0, keepdims=True)
        ddt_ref[rows] = dz.astype(bf16)
    for k in range(blocks):
        rows = slice(k * BLK, (k + 1) * BLK)
        window = dpadk[k * BLK : k * BLK + BLK + 8]
        out = par[3:4] * window[0:BLK]
        for t in range(3):
            out = out + par[t : t + 1] * window[3 - t : 3 - t + BLK]
        dkeys_ref[rows] = out.astype(bf16)


def bwd_kernel(
    gate_ref, rawv_ref, rawk_ref, dtr_ref, pv_ref, ph_ref,
    y_ref, gg_ref, hst_ref, r_ref, c_ref, s_ref, st_ref, hl_ref, ehl_ref, kb_ref, kt_ref, sc_ref,
    dproj_ref, sv_ref, sk_ref, sh_ref,
    pad, padk, dpad, dpadk, sg, dhcar, dsc, dkb, dsrow, dscol, ddt,
):
    g = pl.program_id(0)
    length, total = dproj_ref.shape
    wide = GC * pl.num_programs(0)
    shared = (s_ref, st_ref, hl_ref, ehl_ref, kb_ref, kt_ref, sc_ref)

    @pl.when(g == 0)
    def _():
        backward_start(length, pad, dpad, dsc, dkb, dsrow, dscol, ddt)

    gate_at = pl.ds(pl.multiple_of(g * GC, GC), GC)
    draw_at = pl.ds(pl.multiple_of(wide + g * GC, GC), GC)
    backward_group(
        g, gate_ref, rawv_ref, y_ref, gg_ref, hst_ref, r_ref, c_ref, pv_ref, shared,
        dproj_ref.at[:, gate_at], dproj_ref.at[:, draw_at], sv_ref,
        pad, dpad, sg, dhcar, dsc, dkb, dsrow, dscol, ddt,
    )

    @pl.when(g == pl.num_programs(0) - 1)
    def _():
        keys = 2 * wide
        dproj_ref[:, keys + 3 * KEY :] = jnp.zeros((length, total - keys - 3 * KEY), bf16)
        backward_shared(
            rawk_ref, dtr_ref, pv_ref, wide, ph_ref, kb_ref,
            dproj_ref.at[:, keys : keys + 2 * KEY], dproj_ref.at[:, keys + 2 * KEY : keys + 3 * KEY],
            sk_ref, sh_ref, padk, dpadk, dsc, dkb, dsrow, dscol, ddt,
        )


def whole_spec(shape):
    return pl.BlockSpec(shape, lambda g: (0,) * len(shape))


def state_specs(length):
    return (
        ((length, KEY), f32),
        ((KEY, length), f32),
        ((3, length, 2 * KEY), bf16),
        ((8, 2 * KEY), bf16),
        ((length, 2 * KEY), bf16),
        ((2 * KEY, length), bf16),
        ((length // BLK, BLK, BLK), f32),
    )


def proj_specs(length, groups):
    wide = groups * GC
    return [
        pl.BlockSpec((length, GC), lambda g: (0, g)),
        pl.BlockSpec((length, GC), lambda g: (0, groups + g)),
        pl.BlockSpec((length, 2 * KEY), lambda g: (0, 2 * wide // (2 * KEY))),
        pl.BlockSpec((length, KEY), lambda g: (0, 2 * wide // KEY + 2)),
        whole_spec((8, wide + 2 * KEY)),
        whole_spec((8, KEY)),
    ]


def mixer_forward(projected, pv, ph):
    length = projected.shape[0]
    wide = pv.shape[1] - 2 * KEY
    groups = wide // GC
    blocks = length // BLK
    column = pl.BlockSpec((length, GC), lambda g: (0, g))
    shared = state_specs(length)
    return pl.pallas_call(
        fwd_kernel,
        grid=(groups,),
        in_specs=proj_specs(length, groups),
        out_specs=[
            column,
            whole_spec((length, wide)),
            pl.BlockSpec((blocks, KEY, GC), lambda g: (0, 0, g)),
            whole_spec((length, KEY)),
        ]
        + [whole_spec(shape) for shape, _ in shared],
        out_shape=[
            jax.ShapeDtypeStruct((length, wide), f32),
            jax.ShapeDtypeStruct((length, wide), f32),
            jax.ShapeDtypeStruct((blocks, KEY, wide), bf16),
            jax.ShapeDtypeStruct((length, KEY), f32),
        ]
        + [jax.ShapeDtypeStruct(shape, dtype) for shape, dtype in shared],
        scratch_shapes=[
            pltpu.VMEM((length + 8, GC), f32),
            pltpu.VMEM((length + 8, 2 * KEY), f32),
            pltpu.VMEM((length, KEY), f32),
            pltpu.VMEM((KEY, GC), f32),
            pltpu.VMEM((length, KEY), f32),
        ],
        name="mixer_forward",
    )(projected, projected, projected, projected, pv, ph)


def backward_scratch(length):
    return [
        pltpu.VMEM((length + 8, GC), f32),
        pltpu.VMEM((length + 8, 2 * KEY), f32),
        pltpu.VMEM((length + 8, GC), f32),
        pltpu.VMEM((length + 8, 2 * KEY), f32),
        pltpu.VMEM((length, KEY), f32),
        pltpu.VMEM((KEY, GC), f32),
        pltpu.VMEM((length // BLK, BLK, BLK), f32),
        pltpu.VMEM((length, 2 * KEY), f32),
        pltpu.VMEM((length, KEY), f32),
        pltpu.VMEM((KEY, length), f32),
        pltpu.VMEM((length, KEY), f32),
    ]


def mixer_backward(projected, pv, ph, mixed, grad_gated, states, inverse, pull, shared):
    length, total = projected.shape
    wide = pv.shape[1] - 2 * KEY
    groups = wide // GC
    blocks = length // BLK
    column = pl.BlockSpec((length, GC), lambda g: (0, g))
    return pl.pallas_call(
        bwd_kernel,
        grid=(groups,),
        in_specs=proj_specs(length, groups)
        + [
            column,
            column,
            pl.BlockSpec((blocks, KEY, GC), lambda g: (0, 0, g)),
            whole_spec((length, KEY)),
            whole_spec((length, KEY)),
        ]
        + [whole_spec(shape) for shape, _ in state_specs(length)],
        out_specs=[
            whole_spec((length, total)),
            pl.BlockSpec((8, GC), lambda g: (0, g)),
            whole_spec((8, 2 * KEY)),
            whole_spec((8, KEY)),
        ],
        out_shape=[
            jax.ShapeDtypeStruct((length, total), bf16),
            jax.ShapeDtypeStruct((8, wide), f32),
            jax.ShapeDtypeStruct((8, 2 * KEY), f32),
            jax.ShapeDtypeStruct((8, KEY), f32),
        ],
        scratch_shapes=backward_scratch(length),
        name="mixer_backward",
    )(projected, projected, projected, projected, pv, ph, mixed, grad_gated, states, inverse, pull, *shared)


MESH = pl.DeviceIdType.MESH
HALF = 256


def places():
    d, f = lax.axis_index("dp"), lax.axis_index("fsdp")
    z, x, y, c = d // 2, d % 2, f // 2, f % 2
    over_core = (d, y * 2 + 1 - c)
    over_x = (z * 2 + 1 - x, f)
    over_y = (d, (1 - y) * 2 + c)
    near = ((z + 1 - 2 * (z % 2)) * 2 + x, f)
    far = (((z + 2) % 4) * 2 + x, f)
    peers = ((over_core, over_x, over_y, near, far), (over_core, over_y, over_x, near, far))
    own = ((c, x, y, z % 2, z // 2), (c, y, x, z % 2, z // 2))
    return peers, own


def greet(partners):
    barrier = pltpu.get_barrier_semaphore()
    for partner in partners:
        pl.semaphore_signal(barrier, inc=1, device_id=partner, device_id_type=MESH)
    pl.semaphore_wait(barrier, len(partners))


def block_order(half, i):
    z, x, y, c = i // 8, i // 4 % 2, i // 2 % 2, i % 2
    first, second = (x, y) if half == 0 else (y, x)
    return c, first * 8 + second * 4 + z % 2 * 2 + z // 2


def spread_lanes(tiles, width, lane, count):
    out = [jnp.zeros(tiles[0].shape, f32) for _ in range(count)]
    for i, tile in enumerate(tiles):
        at, shift = divmod(i * width, KEY)
        turned = pltpu.roll(tile, shift, 1) if shift else tile
        end = shift + width
        out[at] = out[at] + jnp.where((lane >= shift) & (lane < end), turned, 0.0)
        if end > KEY:
            out[at + 1] = out[at + 1] + jnp.where(lane < end - KEY, turned, 0.0)
    return out


def forward_kernel(
    n_in, n_out, hidden_ref, cot_ref, live_ref, w_ref, wo_ref, tile_ref, skip_ref, ph_ref,
    w_out, proj_out, mixed_out, states_out, flipped_gated_out, gg_out,
    out_ref, flipped_ref, pv_ref, gain, r_ref, c_ref, s_ref, st_ref, hl_ref, ehl_ref, kb_ref, kt_ref, sc_ref,
    held, tiles, w_stage, wo_stage, proj_stage, mixed_stage, states_stage, flip_stage, normed, gated, big,
    pad, padk, sg, hcar, ssq, dots,
    send, recv, tile_sem, out_sem,
):
    rb = w_ref.shape[0]
    length, width = hidden_ref.shape
    wide = big.shape[1]
    n = n_in + n_out
    peers, own = places()
    greet(peers[0])
    base = [sum(bit * (16 >> k) for k, bit in enumerate(own[h])) for h in range(2)]
    count = (1, 2, 4, 8, 16)

    def columns(i, half):
        group = (i - 1) * HALF + half * wide
        return pl.ds(pl.multiple_of(jnp.where(i == 0, 2 * wide + half * HALF, group), HALF), HALF)

    def copy(stage, i, half):
        start = base[half] // count[stage] * count[stage]
        block = held.at[i, half, pl.ds(start, count[stage])]
        return pltpu.make_async_remote_copy(
            src_ref=block,
            dst_ref=block,
            send_sem=send.at[i, half, stage],
            recv_sem=recv.at[i, half, stage],
            device_id=peers[half][4 - stage],
            device_id_type=MESH,
        )

    def tile_copy(stage):
        block = tiles.at[pl.ds(base[0] // count[stage] * count[stage], count[stage])]
        return pltpu.make_async_remote_copy(
            src_ref=block,
            dst_ref=block,
            send_sem=tile_sem.at[0, stage],
            recv_sem=tile_sem.at[1, stage],
            device_id=peers[0][4 - stage],
            device_id_type=MESH,
        )

    def weight_stores(i):
        slot = lax.rem(i, 2)
        copies = []
        for half in range(2):
            cols = slice(half * HALF, (half + 1) * HALF)
            copies.append(
                pltpu.make_async_copy(
                    w_stage.at[slot, :, cols], w_out.at[:, columns(i, half)], out_sem.at[half, slot]
                )
            )
            copies.append(
                pltpu.make_async_copy(
                    proj_stage.at[slot, :, cols], proj_out.at[:, columns(i, half)], out_sem.at[2 + half, slot]
                )
            )
        return copies

    def group_stores(i):
        slot = lax.rem(i, 2)
        cols = pl.ds(pl.multiple_of((i - 1) * HALF, HALF), HALF)
        return (
            pltpu.make_async_copy(mixed_stage.at[slot], mixed_out.at[:, cols], out_sem.at[4, slot]),
            pltpu.make_async_copy(states_stage.at[slot], states_out.at[:, :, cols], out_sem.at[5, slot]),
        )

    def flip_store(k):
        return pltpu.make_async_copy(
            flip_stage.at[k % 2], flipped_gated_out.at[k * HALF : (k + 1) * HALF], out_sem.at[6, k % 2]
        )

    tiles[base[0]] = tile_ref[...]
    tile_copy(0).start()

    def land(i, carry):
        for half in range(2):
            held[i, half, base[half]] = w_ref[:, columns(i, half)]
        return carry

    lax.fori_loop(0, n_in, land, 0)
    for j in range(n_out):
        for half in range(2):
            held[n_in + j, half, base[half]] = wo_ref[half * rb : (half + 1) * rb, j * HALF : (j + 1) * HALF]

    def keys_chunk(slot):
        lane = iota((8, KEY), 1)
        row = iota((8, KEY), 0)
        order = [tiles[c * 16 + at] for c, at in (block_order(0, i) for i in range(32))]
        conv = spread_lanes(order, (wide + 2 * KEY) // 32, lane, wide // KEY + 2)
        gate = spread_lanes(order, wide // 32, lane, wide // KEY)
        pre = spread_lanes(order, width // 32, lane, width // KEY)
        for k, tile in enumerate(conv):
            cols = slice(k * KEY, (k + 1) * KEY)
            if k < wide // KEY:
                tile = jnp.where(row == 5, gate[k], jnp.where(row == 6, skip_ref[:, cols], tile))
            pv_ref[:, cols] = tile
        for k, tile in enumerate(pre):
            gain[:, k * KEY : (k + 1) * KEY] = tile
        for k in range(0, length, KEY):
            values = hidden_ref[k : k + KEY].astype(f32)
            mean = jnp.mean(values * values, axis=1, keepdims=True)
            rows = (values * lax.rsqrt(mean + epsilon) * gain[6:7]).astype(bf16)
            normed[k : k + KEY] = rows
            flipped_ref[:, k : k + KEY] = rows.T
        project(slot)
        forward_shared(
            proj_stage.at[slot, :, 0:HALF], proj_stage.at[slot, :, HALF : HALF + KEY], pv_ref, wide, ph_ref,
            s_ref, st_ref, hl_ref, ehl_ref, kb_ref, kt_ref, sc_ref, padk,
        )
        pad[0:8] = jnp.zeros((8, GC), f32)
        ssq[...] = jnp.zeros_like(ssq)
        dots[...] = jnp.zeros_like(dots)

    def project(slot):
        for half in range(2):
            cols = slice(half * HALF, (half + 1) * HALF)
            proj_stage[slot, :, cols] = mm(normed[...], w_stage[slot, :, cols])

    def group_chunk(slot, g):
        project(slot)
        forward_group(
            g, proj_stage.at[slot, :, 0:HALF], proj_stage.at[slot, :, HALF : 2 * HALF], pv_ref,
            s_ref, st_ref, hl_ref, ehl_ref, kb_ref, kt_ref, sc_ref,
            mixed_stage.at[slot], big, states_stage.at[slot], pad, sg, hcar, ssq,
        )

    def finish_groups():
        mean = jnp.sum(ssq[...], axis=1, keepdims=True) / wide
        r_ref[...] = jnp.broadcast_to(lax.rsqrt(mean + epsilon), r_ref.shape)
        for k in range(wide // HALF):
            if k >= 2:
                flip_store(k - 2).wait()
            for q in range(HALF // KEY):
                cols = slice(k * HALF + q * KEY, k * HALF + (q + 1) * KEY)
                part = (big[:, cols] * r_ref[...] * pv_ref[5:6, cols]).astype(bf16)
                gated[:, cols] = part
                flip_stage[k % 2, q * KEY : (q + 1) * KEY] = part.T
            flip_store(k).start()
        for k in range(wide // HALF - 2, wide // HALF):
            flip_store(k).wait()

    def out_chunk(i):
        j = i - n_in
        for b in range(32):
            for half in range(2):
                c, at = block_order(half, b)
                wo_stage[(2 * b + half) * rb : (2 * b + half + 1) * rb] = held[i, half, c * 16 + at]
        cols = pl.ds(pl.multiple_of(j * HALF, HALF), HALF)
        branch = mm(gated[...], wo_stage[...])
        live = jnp.concatenate([live_ref[...]] * (HALF // KEY), axis=1)
        out_ref[:, cols] = (hidden_ref[:, cols].astype(f32) + live * branch).astype(bf16)
        upstream = (cot_ref[:, cols].astype(f32) * live).astype(bf16)
        dots[...] += upstream.astype(f32) * branch
        for q in range(0, wide, 512):
            more = mm_nt(upstream, wo_stage[q : q + 512])

            @pl.when(j == 0)
            def _():
                big[:, q : q + 512] = more

            @pl.when(j > 0)
            def _():
                big[:, q : q + 512] += more

    def consume(i):
        slot = lax.rem(i, 2)

        @pl.when(i < n_in)
        def _():
            @pl.when(i >= 2)
            def _():
                for store in weight_stores(i - 2):
                    store.wait()

            for half in range(2):
                for b in range(32):
                    c, at = block_order(half, b)
                    w_stage[slot, b * rb : (b + 1) * rb, half * HALF : (half + 1) * HALF] = held[i, half, c * 16 + at]

            @pl.when(i == 0)
            def _():
                keys_chunk(slot)

            @pl.when(i > 0)
            def _():
                @pl.when(i >= 3)
                def _():
                    for store in group_stores(i - 2):
                        store.wait()

                group_chunk(slot, i - 1)
                for store in group_stores(i):
                    store.start()

            for store in weight_stores(i):
                store.start()

            @pl.when(i == n_in - 1)
            def _():
                finish_groups()

        @pl.when(i >= n_in)
        def _():
            out_chunk(i)

    def tick(t, carry):
        @pl.when(t < n)
        def _():
            for half in range(2):
                copy(0, t, half).start()

        for stage in range(5):
            i = t - stage - 1

            @pl.when(i == 0)
            def _(stage=stage):
                tile_copy(stage).wait()
                if stage < 4:
                    tile_copy(stage + 1).start()

            @pl.when((i >= 0) & (i < n))
            def _(stage=stage, i=i):
                for half in range(2):
                    copy(stage, i, half).wait()
                    if stage < 4:
                        copy(stage + 1, i, half).start()
                if stage == 4:
                    consume(i)

        return carry

    lax.fori_loop(0, n + 5, tick, 0)
    whole = pltpu.make_async_copy(big, gg_out, out_sem.at[6, 0])
    whole.start()
    pull = jnp.sum(dots[...], axis=1, keepdims=True) / wide
    c_ref[...] = r_ref[...] * r_ref[...] * pull
    for i in (n_in - 2, n_in - 1):
        for store in weight_stores(i) + list(group_stores(i)):
            store.wait()
    whole.wait()


def gather_forward(hidden, cotangent, live, shard, out_shard, tile, skip_rows, ph):
    length, width = hidden.shape
    rb, columns = shard.shape
    wide = out_shard.shape[0] * 32
    n_in, n_out = columns // (2 * HALF), width // HALF
    blocks = length // BLK
    vmem = pl.BlockSpec(memory_space=pltpu.VMEM)
    anywhere = pl.BlockSpec(memory_space=pl.ANY)
    struct = jax.ShapeDtypeStruct
    shared = [struct(shape, dtype) for shape, dtype in state_specs(length)]
    return pl.pallas_call(
        partial(forward_kernel, n_in, n_out),
        out_shape=[
            struct((width, columns), bf16),
            struct((length, columns), f32),
            struct((length, wide), f32),
            struct((blocks, KEY, wide), bf16),
            struct((wide, length), bf16),
            struct((length, wide), f32),
            struct((length, width), bf16),
            struct((width, length), bf16),
            struct((8, wide + 2 * KEY), f32),
            struct((8, width), f32),
            struct((length, KEY), f32),
            struct((length, KEY), f32),
        ]
        + shared,
        in_specs=[vmem] * 8,
        out_specs=[anywhere] * 6 + [vmem] * (6 + len(shared)),
        scratch_shapes=[
            pltpu.VMEM((n_in + n_out, 2, 32, rb, HALF), bf16),
            pltpu.VMEM((32, 8, KEY), f32),
            pltpu.VMEM((2, width, 2 * HALF), bf16),
            pltpu.VMEM((wide, HALF), bf16),
            pltpu.VMEM((2, length, 2 * HALF), f32),
            pltpu.VMEM((2, length, HALF), f32),
            pltpu.VMEM((2, blocks, KEY, HALF), bf16),
            pltpu.VMEM((2, HALF, length), bf16),
            pltpu.VMEM((length, width), bf16),
            pltpu.VMEM((length, wide), bf16),
            pltpu.VMEM((length, wide), f32),
            pltpu.VMEM((length + 8, GC), f32),
            pltpu.VMEM((length + 8, 2 * KEY), f32),
            pltpu.VMEM((length, KEY), f32),
            pltpu.VMEM((KEY, GC), f32),
            pltpu.VMEM((length, KEY), f32),
            pltpu.VMEM((length, HALF), f32),
            pltpu.SemaphoreType.DMA((n_in + n_out, 2, 5)),
            pltpu.SemaphoreType.DMA((n_in + n_out, 2, 5)),
            pltpu.SemaphoreType.DMA((2, 5)),
            pltpu.SemaphoreType.DMA((7, 2)),
        ],
        compiler_params=pltpu.CompilerParams(
            collective_id=2, has_side_effects=True, vmem_limit_bytes=63 << 20
        ),
        name="gather_forward",
    )(hidden, cotangent, live, shard, out_shard, tile, skip_rows, ph)


EARLY = 6


def gather_lanes(row_tiles, width, lane, i):
    at, shift = divmod(i * width, KEY)
    if shift == 0:
        return row_tiles[at]
    first = pltpu.roll(row_tiles[at], KEY - shift, 1)
    if shift + width <= KEY:
        return first
    return jnp.where(lane < KEY - shift, first, pltpu.roll(row_tiles[at + 1], KEY - shift, 1))


def backward_kernel(
    n_in, n_out, hidden_ref, cot_ref, live_ref, flipped_ref, gated_ref, pv_ref, gain_ref, ph_ref, r_ref, c_ref,
    s_ref, st_ref, hl_ref, ehl_ref, kb_ref, kt_ref, sc_ref,
    proj_in, mixed_in, gg_in, states_in, w_in,
    rows_out, in_ref, dt_ref, out_ref, tile_out, sums_ref,
    parts, r0, r1, r2, r3, r4, tiles, t0, t1, t2, t3, t4, sums, sums_in,
    stage_in, states_stage, w_stage, keys_stage, dchunk, rows_grad, sv, sv_all, sk, sh, skip_sum, gain_sum,
    pad, padk, dpad, dpadk, sg, dhcar, dsc, dkb, dsrow, dscol, ddt,
    send, recv, tile_sem, sums_sem, in_sem, out_sem,
):
    length, width = hidden_ref.shape
    wide = mixed_in.shape[1]
    rb = in_ref.shape[0]
    n = n_in + n_out
    groups = n_in - 1
    keys_tick = n - 2
    shared = (s_ref, st_ref, hl_ref, ehl_ref, kb_ref, kt_ref, sc_ref)
    peers, own = places()
    held = (r0, r1, r2, r3, r4)
    tile_source = (tiles, t0, t1, t2, t3, t4)
    greet(peers[0])

    def is_out(t):
        return ((t < 3 * n_out - 3) & (lax.rem(t, 3) == 0)) | (t == n - 1)

    def out_index(t):
        return jnp.where(t == n - 1, n_out - 1, t // 3)

    def group_index(t):
        return jnp.where(t < 3 * n_out - 3, t // 3 * 2 + lax.rem(t, 3) - 1, t - n_out + 1)

    def loads(g):
        slot = lax.rem(g, 2)
        near = pl.ds(pl.multiple_of(g * HALF, HALF), HALF)
        far = pl.ds(pl.multiple_of(wide + g * HALF, HALF), HALF)
        pairs = (
            (proj_in.at[:, near], stage_in.at[slot, 0]),
            (proj_in.at[:, far], stage_in.at[slot, 1]),
            (mixed_in.at[:, near], stage_in.at[slot, 2]),
            (gg_in.at[:, near], stage_in.at[slot, 3]),
            (states_in.at[:, :, near], states_stage.at[slot]),
        )
        return [pltpu.make_async_copy(a, b, in_sem.at[k, slot]) for k, (a, b) in enumerate(pairs)]

    def weight_loads(g):
        slot = lax.rem(g, 2)
        first = jnp.where(g == groups, 2 * wide, g * HALF)
        second = jnp.where(g == groups, 2 * wide + HALF, wide + g * HALF)
        return [
            pltpu.make_async_copy(
                w_in.at[:, pl.ds(pl.multiple_of(at, HALF), HALF)],
                w_stage.at[slot, :, half * HALF : (half + 1) * HALF],
                in_sem.at[5 + half, slot],
            )
            for half, at in enumerate((first, second))
        ]

    keys_load = pltpu.make_async_copy(proj_in.at[:, 2 * wide : 2 * wide + 3 * KEY], keys_stage, in_sem.at[7, 0])
    for load in loads(0) + weight_loads(0) + [keys_load]:
        load.start()
    rows_store = pltpu.make_async_copy(rows_grad, rows_out, out_sem.at[0])

    def sums_copy(stage):
        return pltpu.make_async_remote_copy(
            src_ref=sums.at[stage],
            dst_ref=sums_in.at[stage],
            send_sem=sums_sem.at[0, stage],
            recv_sem=sums_sem.at[1, stage],
            device_id=peers[0][stage],
            device_id_type=MESH,
        )

    def tile_copy(stage):
        count = 16 >> stage
        return pltpu.make_async_remote_copy(
            src_ref=tile_source[stage].at[pl.ds((1 - own[0][stage]) * count, count)],
            dst_ref=tile_source[stage + 1],
            send_sem=tile_sem.at[0, stage],
            recv_sem=tile_sem.at[1, stage],
            device_id=peers[0][stage],
            device_id_type=MESH,
        )

    def place(stage, i):
        return lax.rem(i, EARLY) if stage == 0 else i

    def copy(stage, i, half):
        count = 16 >> stage
        if stage == 0:
            src = parts.at[lax.rem(i, 2), 1 - own[half][0], half]
        else:
            src = held[stage - 1].at[place(stage - 1, i), half, pl.ds((1 - own[half][stage]) * count, count)]
        return pltpu.make_async_remote_copy(
            src_ref=src,
            dst_ref=held[stage].at[place(stage, i), half],
            send_sem=send.at[i, half, stage],
            recv_sem=recv.at[i, half, stage],
            device_id=peers[half][stage],
            device_id_type=MESH,
        )

    backward_start(length, pad, dpad, dsc, dkb, dsrow, dscol, ddt)
    skip_sum[...] = jnp.zeros_like(skip_sum)
    rows_grad[...] = jnp.zeros_like(rows_grad)

    def out_chunk(slot, j):
        cols = pl.ds(pl.multiple_of(j * HALF, HALF), HALF)
        live = jnp.concatenate([live_ref[...]] * (HALF // KEY), axis=1)
        upstream = (cot_ref[:, cols].astype(f32) * live).astype(bf16)
        for z in range(4):
            res = mm(gated_ref[z * 16 * rb : (z + 1) * 16 * rb], upstream)
            for b in range(8):
                for half in range(2):
                    c, at = block_order(half, z * 8 + b)
                    at_row = (2 * b + half) * rb
                    parts[slot, c, half, at] = res[at_row : at_row + rb].astype(bf16)

    def weight_chunk(slot, g):
        for load in weight_loads(g):
            load.wait()
        at = lax.rem(g, 2)
        for half in range(2):
            right = dchunk[:, half * HALF : (half + 1) * HALF]
            for z in range(4):
                res = mm(flipped_ref[z * 8 * rb : (z + 1) * 8 * rb], right)
                for b in range(8):
                    c, where = block_order(half, z * 8 + b)
                    parts[slot, c, half, where] = res[b * rb : (b + 1) * rb].astype(bf16)
        for k in range(0, width, 512):
            rows_grad[:, k : k + 512] += mm_nt(dchunk[...], w_stage[at, k : k + 512])

    def group_chunk(slot, g):
        for load in weight_loads(g + 1):
            load.start()

        @pl.when(g + 1 < groups)
        def _():
            for load in loads(g + 1):
                load.start()

        for load in loads(g):
            load.wait()
        at = lax.rem(g, 2)
        backward_group(
            g, stage_in.at[at, 0], stage_in.at[at, 1], stage_in.at[at, 2], stage_in.at[at, 3], states_stage.at[at],
            r_ref, c_ref, pv_ref, shared, dchunk.at[:, 0:HALF], dchunk.at[:, HALF : 2 * HALF], sv,
            pad, dpad, sg, dhcar, dsc, dkb, dsrow, dscol, ddt,
        )
        sv_all[:, pl.ds(pl.multiple_of(g * HALF, HALF), HALF)] = sv[...]
        skip_sum[...] += mm_hi(sv[...], reducer(g).astype(f32))
        weight_chunk(slot, g)

    def keys_chunk(slot):
        keys_load.wait()
        dchunk[:, 3 * KEY :] = jnp.zeros((length, KEY), bf16)
        backward_shared(
            keys_stage.at[:, 0:HALF], keys_stage.at[:, HALF : HALF + KEY], pv_ref, wide, ph_ref, kb_ref,
            dchunk.at[:, 0:HALF], dchunk.at[:, HALF : HALF + KEY], sk, sh,
            padk, dpadk, dsc, dkb, dsrow, dscol, ddt,
        )
        weight_chunk(slot, groups)
        for half in range(2):
            copy(0, keys_tick, half).start()
        gain = gain_ref[6:7]
        gain_sum[...] = jnp.zeros_like(gain_sum)
        for k in range(0, length, KEY):
            values = hidden_ref[k : k + KEY].astype(f32)
            inverse = lax.rsqrt(jnp.mean(values * values, axis=1, keepdims=True) + epsilon)
            grads = rows_grad[k : k + KEY]
            gain_sum[0:1] += jnp.sum(grads * values * inverse, axis=0, keepdims=True)
            scaled = grads * gain
            pull = jnp.sum(scaled * values, axis=1, keepdims=True) / width
            back = inverse * scaled - values * (inverse * inverse * inverse * pull)
            rows_grad[k : k + KEY] = cot_ref[k : k + KEY].astype(f32) + back
        rows_store.start()
        row = iota((8, KEY), 0)
        lane = iota((8, KEY), 1)
        conv = [sv_all[:, k * KEY : (k + 1) * KEY] for k in range(wide // KEY)]
        gate = conv
        conv = conv + [sk[:, 0:KEY], sk[:, KEY : 2 * KEY]]
        pre = [jnp.broadcast_to(gain_sum[0:1, k * KEY : (k + 1) * KEY], (8, KEY)) for k in range(width // KEY)]
        for i in range(32):
            c, at = block_order(0, i)
            tile = gather_lanes(conv, (wide + 2 * KEY) // 32, lane, i)
            tile = jnp.where(row == 5, gather_lanes(gate, wide // 32, lane, i), tile)
            tiles[c * 16 + at] = jnp.where(row == 6, gather_lanes(pre, width // 32, lane, i), tile)
        tile_copy(0).start()
        sums[0] = jnp.where(row == 2, skip_sum[6:7], sh[...])
        sums_copy(0).start()

    def write_out(i, half, value):
        @pl.when(is_out(i))
        def _():
            cols = pl.ds(pl.multiple_of(out_index(i) * HALF, HALF), HALF)
            out_ref[half * rb : (half + 1) * rb, cols] = value

        @pl.when(jnp.logical_not(is_out(i)) & (i != keys_tick))
        def _():
            cols = pl.ds(pl.multiple_of(half * wide + group_index(i) * HALF, HALF), HALF)
            in_ref[:, cols] = value

        @pl.when(i == keys_tick)
        def _():
            if half == 0:
                in_ref[:, 2 * wide : 2 * wide + HALF] = value
            else:
                dt_ref[...] = value[:, :KEY]

    def tick(t, carry):
        @pl.when(t < n)
        def _():
            slot = lax.rem(t, 2)

            @pl.when(t >= 2)
            def _():
                for half in range(2):
                    copy(0, t - 2, half).wait_send()

            @pl.when(is_out(t))
            def _():
                out_chunk(slot, out_index(t))

            @pl.when(jnp.logical_not(is_out(t)) & (t != keys_tick))
            def _():
                group_chunk(slot, group_index(t))

            @pl.when(t == keys_tick)
            def _():
                keys_chunk(slot)

            @pl.when(t != keys_tick)
            def _():
                for half in range(2):
                    copy(0, t, half).start()

        for stage in range(5):
            i = t - stage - 1
            count = 16 >> stage

            @pl.when(i == keys_tick)
            def _(stage=stage, count=count):
                sums_copy(stage).wait()
                tile_copy(stage).wait()
                total = tile_source[stage + 1][...] + tile_source[stage][pl.ds(own[0][stage] * count, count)]
                if stage < 4:
                    sums[stage + 1] = sums[stage] + sums_in[stage]
                    sums_copy(stage + 1).start()
                    tile_source[stage + 1][...] = total
                    tile_copy(stage + 1).start()
                else:
                    sums_ref[...] = sums[stage] + sums_in[stage]
                    tile_out[...] = total[0]

            @pl.when((i >= 0) & (i < n))
            def _(stage=stage, i=i, count=count):
                for half in range(2):
                    done = copy(stage, i, half)
                    if stage == 0:
                        done.wait_recv()
                        mine = parts[lax.rem(i, 2), own[half][0], half]
                    else:
                        done.wait()
                        mine = held[stage - 1][place(stage - 1, i), half, pl.ds(own[half][stage] * count, count)]
                    if stage < 4:
                        at = place(stage, i)
                        held[stage][at, half] = (
                            held[stage][at, half].astype(f32) + mine.astype(f32)
                        ).astype(bf16)
                        copy(stage + 1, i, half).start()
                    else:
                        write_out(i, half, held[stage][i, half, 0].astype(f32) + mine[0].astype(f32))

        return carry

    lax.fori_loop(0, n + 5, tick, 0)
    for i in (n - 2, n - 1):
        for half in range(2):
            copy(0, i, half).wait_send()
    rows_store.wait()


def backward_scatter(
    hidden, cotangent, live, flipped, gated_flipped, pv, gains, ph, inverse, pull, shared,
    projected, mixed, grad_gated, states, w_in, rb,
):
    length, width = hidden.shape
    columns = projected.shape[1]
    wide = mixed.shape[1]
    n_in, n_out = columns // (2 * HALF), width // HALF
    n = n_in + n_out
    blocks = length // BLK
    vmem = pl.BlockSpec(memory_space=pltpu.VMEM)
    anywhere = pl.BlockSpec(memory_space=pl.ANY)
    struct = jax.ShapeDtypeStruct
    return pl.pallas_call(
        partial(backward_kernel, n_in, n_out),
        out_shape=[
            struct((length, width), f32),
            struct((rb, columns - 2 * KEY), f32),
            struct((rb, KEY), f32),
            struct((2 * rb, width), f32),
            struct((8, KEY), f32),
            struct((8, KEY), f32),
        ],
        in_specs=[vmem] * 17 + [anywhere] * 5,
        out_specs=[anywhere] + [vmem] * 5,
        scratch_shapes=[pltpu.VMEM((2, 2, 2, 16, rb, HALF), bf16)]
        + [pltpu.VMEM((n if stage else EARLY, 2, 16 >> stage, rb, HALF), bf16) for stage in range(5)]
        + [pltpu.VMEM((32 >> stage, 8, KEY), f32) for stage in range(6)]
        + [pltpu.VMEM((5, 8, KEY), f32)] * 2
        + [
            pltpu.VMEM((2, 4, length, HALF), f32),
            pltpu.VMEM((2, blocks, KEY, HALF), bf16),
            pltpu.VMEM((2, width, 2 * HALF), bf16),
            pltpu.VMEM((length, 3 * KEY), f32),
            pltpu.VMEM((length, 2 * HALF), bf16),
            pltpu.VMEM((length, width), f32),
            pltpu.VMEM((8, HALF), f32),
            pltpu.VMEM((8, wide), f32),
            pltpu.VMEM((8, HALF), f32),
            pltpu.VMEM((8, KEY), f32),
            pltpu.VMEM((8, KEY), f32),
            pltpu.VMEM((8, width), f32),
        ]
        + backward_scratch(length)
        + [pltpu.SemaphoreType.DMA((n, 2, 5))] * 2
        + [pltpu.SemaphoreType.DMA((2, 5))] * 2
        + [pltpu.SemaphoreType.DMA((8, 2)), pltpu.SemaphoreType.DMA((1,))],
        compiler_params=pltpu.CompilerParams(
            collective_id=1, has_side_effects=True, vmem_limit_bytes=67043328
        ),
        name="backward_scatter",
    )(
        hidden, cotangent, live, flipped, gated_flipped, pv, gains, ph, inverse, pull, *shared,
        projected, mixed, grad_gated, states, w_in,
    )


def pre_norm_inverse(rows):
    return lax.rsqrt(jnp.mean(rows * rows, axis=1, keepdims=True) + epsilon)


AXES = ("dp", "fsdp")


def gather_rows(shard):
    return lax.all_gather(shard, AXES, axis=0, tiled=True)


def scatter_rows(whole):
    return lax.psum_scatter(whole, AXES, scatter_dimension=0, tiled=True)


def vector_tile(conv_weight, conv_bias, gate_gain, norm_gain):
    rows = [conv_weight, conv_bias[None], gate_gain[None], norm_gain[None]]
    rows = [jnp.pad(row.astype(f32), ((0, 0), (0, KEY - row.shape[1]))) for row in rows]
    return jnp.concatenate(rows + [jnp.zeros((1, KEY), f32)], axis=0)


def vector_tiles(conv, gate, pre, parts):
    rows = []
    for whole in (conv, gate, pre):
        part = whole.shape[1] // parts
        split_up = jnp.transpose(whole.reshape(-1, parts, part), (1, 0, 2))
        rows.append(jnp.pad(split_up, ((0, 0), (0, 0), (0, KEY - part))))
    return jnp.concatenate(rows + [jnp.zeros((parts, 1, KEY), f32)], axis=1)


def shards(
    kernels, hidden, cotangent, lengths, norm_gain, in_proj, dt_proj, conv_weight, conv_bias,
    dt_bias, a_log, skip_gain, gate_gain, out_proj,
):
    length, width = hidden.shape
    assert lengths.shape[0] == 1
    rows_in, columns = in_proj.shape
    heads = dt_bias.shape[0]
    parts = width // rows_in
    taps, conv_part = conv_weight.shape
    gate_part = gate_gain.shape[0]
    wide = gate_part * parts
    total = columns + 2 * KEY

    fill = jnp.zeros((rows_in, total - columns - heads), bf16)
    packed = jnp.concatenate([in_proj, dt_proj, fill], axis=1)
    tile = vector_tile(conv_weight, conv_bias, gate_gain, norm_gain)
    ph = jnp.pad(jnp.stack([dt_bias, a_log]).astype(f32), ((0, 6), (0, KEY - heads)))
    skip_wide = jnp.repeat(skip_gain.astype(f32), HD)[None]
    live = (jnp.arange(length) < lengths[0]).astype(f32)[:, None]
    if kernels:
        skip_rows = jnp.broadcast_to(skip_wide, (8, wide))
        (
            w_in, projected, mixed, states, gated_flipped, grad_gated, output, flipped, pv, gains, inverse_two, pull,
            *shared,
        ) = gather_forward(
            hidden, cotangent, jnp.broadcast_to(live, (length, KEY)), packed, out_proj, tile, skip_rows, ph
        )
        input_grad, grad_in, grad_dt, grad_out, small_sum, head_sums = backward_scatter(
            hidden, cotangent, jnp.broadcast_to(live, (length, KEY)), flipped, gated_flipped, pv, gains, ph,
            inverse_two, pull, shared, projected, mixed, grad_gated, states, w_in, rows_in,
        )
    else:
        rows_wide = hidden.astype(f32)
        cot_wide = cotangent.astype(f32)
        upstream = (cot_wide * live).astype(bf16)
        inverse_one = pre_norm_inverse(rows_wide)
        w_in, w_out = gather_rows(packed), gather_rows(out_proj)
        tiles = gather_rows(tile[None])
        whole = lambda rows, part: jnp.transpose(tiles[:, rows, :part], (1, 0, 2)).reshape(-1, parts * part)
        conv_all = whole(slice(0, 5), conv_part)
        gain_two = whole(slice(5, 6), gate_part)
        gain_one = whole(slice(6, 7), rows_in)[0]
        rest = jnp.concatenate([gain_two, skip_wide, jnp.zeros((1, wide), f32)], axis=0)
        pv = jnp.concatenate([conv_all, jnp.pad(rest, ((0, 0), (0, 2 * KEY)))], axis=0)
        normed = (rows_wide * inverse_one * gain_one[None, :]).astype(bf16)
        projected = mm(normed, w_in)
        mixed, product, states, inverse_two, *shared = mixer_forward(projected, pv, ph)
        inv = inverse_two[:, :1]
        gated = (product * inv * gain_two).astype(bf16)
        output = (rows_wide + live * mm(gated, w_out)).astype(bf16)
        grad_gated = mm_nt(upstream, w_out)
        pull = jnp.sum(grad_gated * gain_two * product, axis=1, keepdims=True)
        pull = jnp.broadcast_to(inv * inv * inv * pull / wide, inverse_two.shape)
        grad_out = mm_tn(gated, upstream)
        grad_proj, sums_v, sums_k, sums_h = mixer_backward(
            projected, pv, ph, mixed, grad_gated, states, inverse_two, pull, shared
        )
        skip_grad = jnp.pad(jnp.sum(sums_v[6].reshape(heads, HD), axis=1), (0, KEY - heads))[None]
        head_grads = jnp.concatenate([sums_h[:2], skip_grad, jnp.zeros((5, KEY), f32)], axis=0)

        grad_normed = mm_nt(grad_proj, w_in)
        scaled = grad_normed * gain_one[None, :]
        row_sums = jnp.sum(scaled * rows_wide, axis=1, keepdims=True) / width
        grad_rows = inverse_one * scaled - rows_wide * (inverse_one * inverse_one * inverse_one * row_sums)
        input_grad = cot_wide + grad_rows
        grad_gain_one = jnp.sum(grad_normed * rows_wide * inverse_one, axis=0, keepdims=True)

        conv_grad = jnp.concatenate([sums_v[:5], sums_k[:5]], axis=1)
        small = vector_tiles(conv_grad, sums_v[5:6], grad_gain_one, parts)
        grad_out = scatter_rows(grad_out.astype(bf16)).astype(f32)
        head_sums = lax.psum(head_grads, AXES)
        grad_all = scatter_rows(mm_tn(normed, grad_proj).astype(bf16)).astype(f32)
        grad_in, grad_dt = grad_all[:, :columns], grad_all[:, columns:]
        small_sum = scatter_rows(small)[0]
    return (
        output,
        input_grad,
        small_sum[6, :rows_in],
        grad_in,
        grad_dt[:, :heads],
        small_sum[:taps, :conv_part],
        small_sum[taps, :conv_part],
        head_sums[0, :heads],
        head_sums[1, :heads],
        head_sums[2, :heads],
        small_sum[5, :gate_part],
        grad_out,
    )


def solution(mesh):
    rows = P(AXES, None)
    vector = P(AXES)
    last = P(None, AXES)
    return jax.shard_map(
        partial(shards, mesh.shape["dp"] == 8 and mesh.shape["fsdp"] == 4),
        mesh=mesh,
        in_specs=(rows, rows, vector, vector, rows, rows, last, vector, P(), P(), P(), vector, rows),
        out_specs=(rows, rows, vector, rows, rows, last, vector, P(), P(), P(), vector, rows),
        check_vma=False,
    )
```

```python
from functools import partial

import jax
import jax.numpy as jnp
from jax import lax
from jax.experimental import pallas as pl
from jax.experimental.pallas import tpu as pltpu
from jax.sharding import PartitionSpec as P

f32 = jnp.float32
bf16 = jnp.bfloat16
epsilon = 1e-05
highest = lax.Precision.HIGHEST
BLK = 128
GH = 4
HD = 64
GC = GH * HD
KEY = 128
NEG = -1e30


def sigmoid(v):
    return 0.5 * jnp.tanh(0.5 * v) + 0.5


def mm(a, b):
    return lax.dot_general(a, b, (((1,), (0,)), ((), ())), preferred_element_type=f32)


def mm_nt(a, b):
    return lax.dot_general(a, b, (((1,), (1,)), ((), ())), preferred_element_type=f32)


def mm_tn(a, b):
    return lax.dot_general(a, b, (((0,), (0,)), ((), ())), preferred_element_type=f32)


def mm_hi(a, b, dims=((1,), (0,))):
    return lax.dot_general(a, b, (dims, ((), ())), preferred_element_type=f32, precision=highest)


def split(v):
    hi = v.astype(bf16)
    lo = (v - hi.astype(f32)).astype(bf16)
    return jnp.concatenate([hi, lo], axis=1)


def iota(shape, dim):
    return lax.broadcasted_iota(jnp.int32, shape, dim)


def expander(g):
    rows = iota((2 * KEY, GC), 0)
    cols = iota((2 * KEY, GC), 1)
    return jnp.where(lax.rem(rows, KEY) == cols // HD + g * GH, 1.0, 0.0).astype(bf16)


def reducer(g):
    rows = iota((GC, KEY), 0)
    cols = iota((GC, KEY), 1)
    return jnp.where(rows // HD + g * GH == cols, 1.0, 0.0).astype(bf16)


def taps_of(window, par):
    out = par[4:5] + par[3:4] * window[8:136]
    for k in range(3):
        out = out + par[k : k + 1] * window[5 + k : 133 + k]
    return out


def group_rows(st_ref, g, half, rows):
    tile = st_ref[pl.ds(pl.multiple_of(g // 2 * 8, 8), 8), rows]
    return jnp.where(half == 0, tile[:GH], tile[GH:])


def forward_shared(
    rawk_ref, dtr_ref, pv_ref, key_at, ph_ref, s_ref, st_ref, hl_ref, ehl_ref, kb_ref, kt_ref, sc_ref, padk
):
    blocks = rawk_ref.shape[0] // BLK
    dt = jax.nn.softplus(dtr_ref[...] + ph_ref[0:1, :])
    la = -dt * jnp.exp(ph_ref[1:2, :])
    tri = jnp.where(iota((BLK, BLK), 0) >= iota((BLK, BLK), 1), 1.0, 0.0).astype(f32)
    hl_ref[0] = split(dt)
    ehl_ref[...] = jnp.zeros_like(ehl_ref)
    padk[0:8] = jnp.zeros((8, 2 * KEY), f32)
    padk[8:] = rawk_ref[...]
    par = pv_ref[:, key_at : key_at + 2 * KEY]
    for k in range(blocks):
        rows = slice(k * BLK, (k + 1) * BLK)
        s = mm_hi(tri, la[rows])
        s_ref[rows] = s
        st_ref[:, rows] = s.T
        hl_ref[1, rows] = split(jnp.exp(s))
        hl_ref[2, rows] = split(jnp.exp(s[BLK - 1 :] - s))
        ehl_ref[k : k + 1] = split(jnp.exp(s[BLK - 1 :]))
        u = taps_of(padk[k * BLK : k * BLK + BLK + 8], par)
        v = u * sigmoid(u)
        kb_ref[rows] = v.astype(bf16)
        kt_ref[:, rows] = v.T.astype(bf16)
        sc_ref[k] = mm_hi(v[:, KEY:], v[:, :KEY], ((1,), (1,)))


def forward_group(
    g, gate_ref, rawv_ref, pv_ref, s_ref, st_ref, hl_ref, ehl_ref, kb_ref, kt_ref, sc_ref,
    y_ref, p_ref, hst_ref, pad, sg, hcar, ssq,
):
    blocks = gate_ref.shape[0] // BLK
    pad[8:] = rawv_ref[...]
    sg[...] = pltpu.roll(s_ref[...], lax.rem(KEY - g * GH, KEY), 1)
    ex = expander(g)
    bias = jnp.where(iota((BLK, BLK), 0) >= iota((BLK, BLK), 1), 0.0, NEG).astype(f32)
    low = iota((BLK, KEY), 1) < HD
    eend = mm(ehl_ref[...], ex)
    parg = pv_ref[:, pl.ds(pl.multiple_of(g * GC, GC), GC)]
    half = lax.rem(g, 8 // GH)
    hcar[...] = jnp.zeros_like(hcar)
    for k in range(blocks):
        rows = slice(k * BLK, (k + 1) * BLK)
        dtx = mm(hl_ref[0, rows], ex)
        exx = mm(hl_ref[1, rows], ex)
        txx = mm(hl_ref[2, rows], ex)
        hb = hcar[...].astype(bf16)
        hst_ref[k] = hb
        outer = mm(kb_ref[rows, KEY:], hb)
        across = group_rows(st_ref, g, half, rows)
        xts = []
        for q in range(GC // KEY):
            cols = slice(q * KEY, (q + 1) * KEY)
            par = parg[:, cols]
            u = taps_of(pad[k * BLK : k * BLK + BLK + 8, cols], par)
            v = u * sigmoid(u)
            x = v * dtx[:, cols]
            xts.append((x * txx[:, cols]).astype(bf16))
            xb = x.astype(bf16)
            zero = jnp.zeros_like(xb)
            x2 = jnp.concatenate([jnp.where(low, xb, zero), jnp.where(low, zero, xb)], axis=0)
            ms = []
            for side in range(2):
                j = 2 * q + side
                spread = sg[rows, j : j + 1] - across[j : j + 1]
                ms.append((jnp.exp(spread + bias) * sc_ref[k]).astype(bf16))
            y = mm(jnp.concatenate(ms, axis=1), x2)
            y = y + outer[:, cols] * exx[:, cols] + par[6:7] * v
            y_ref[rows, cols] = y
            gate = gate_ref[rows, cols]
            p = y * (gate * sigmoid(gate))
            p_ref[rows, pl.ds(pl.multiple_of(g * GC + q * KEY, KEY), KEY)] = p
            ssq[rows] += p * p
        if k + 1 < blocks:
            hcar[...] = eend[k : k + 1] * hcar[...] + mm(kt_ref[:KEY, rows], jnp.concatenate(xts, axis=1))


def fwd_kernel(
    gate_ref, rawv_ref, rawk_ref, dtr_ref, pv_ref, ph_ref,
    y_ref, p_ref, hst_ref, r_ref, s_ref, st_ref, hl_ref, ehl_ref, kb_ref, kt_ref, sc_ref,
    pad, padk, sg, hcar, ssq,
):
    g = pl.program_id(0)
    wide = p_ref.shape[1]
    shared = (s_ref, st_ref, hl_ref, ehl_ref, kb_ref, kt_ref, sc_ref)

    @pl.when(g == 0)
    def _():
        forward_shared(rawk_ref, dtr_ref, pv_ref, wide, ph_ref, *shared, padk)
        pad[0:8] = jnp.zeros((8, GC), f32)
        ssq[...] = jnp.zeros_like(ssq)

    forward_group(g, gate_ref, rawv_ref, pv_ref, *shared, y_ref, p_ref, hst_ref, pad, sg, hcar, ssq)

    @pl.when(g == pl.num_programs(0) - 1)
    def _():
        mean = jnp.sum(ssq[...], axis=1, keepdims=True) / wide
        r_ref[...] = jnp.broadcast_to(lax.rsqrt(mean + epsilon), r_ref.shape)


def backward_start(length, pad, dpad, dsc, dkb, dsrow, dscol, ddt):
    pad[0:8] = jnp.zeros((8, GC), f32)
    dpad[length:] = jnp.zeros((8, GC), f32)
    for ref in (dsc, dkb, dsrow, dscol, ddt):
        ref[...] = jnp.zeros_like(ref)


def backward_group(
    g, gate_ref, rawv_ref, y_ref, gg_ref, hst_ref, r_ref, c_ref, pv_ref, shared,
    dgate_ref, draw_ref, sv_ref, pad, dpad, sg, dhcar, dsc, dkb, dsrow, dscol, ddt,
):
    s_ref, st_ref, hl_ref, ehl_ref, kb_ref, kt_ref, sc_ref = shared
    blocks = gate_ref.shape[0] // BLK
    pad[8:] = rawv_ref[...]
    sg[...] = pltpu.roll(s_ref[...], lax.rem(KEY - g * GH, KEY), 1)
    ex = expander(g)
    red = reducer(g)
    row = iota((BLK, BLK), 0)
    col = iota((BLK, BLK), 1)
    bias = jnp.where(row >= col, 0.0, NEG).astype(f32)
    strict = row > col
    low = iota((BLK, KEY), 1) < HD
    eend = mm(ehl_ref[...], ex)
    parg = pv_ref[:, pl.ds(pl.multiple_of(g * GC, GC), GC)]
    half = lax.rem(g, 8 // GH)
    tile_at = pl.ds(pl.multiple_of(g // 2 * 8, 8), 8)
    mine = (iota((8, BLK), 0) < GH) == (half == 0)
    dhcar[...] = jnp.zeros_like(dhcar)
    sv_ref[...] = jnp.zeros_like(sv_ref)
    for k in range(blocks - 1, -1, -1):
        rows = slice(k * BLK, (k + 1) * BLK)
        dtx = mm(hl_ref[0, rows], ex)
        exx = mm(hl_ref[1, rows], ex)
        txx = mm(hl_ref[2, rows], ex)
        hb = hst_ref[k]
        dhb = dhcar[...].astype(bf16)
        ch = mm(kb_ref[rows, KEY:], hb)
        qq = mm(kb_ref[rows, :KEY], dhb)
        across = group_rows(st_ref, g, half, rows)
        dyes, xts, zs, oys, ddts, ecols = [], [], [], [], [], []
        dsrow_k = jnp.zeros((BLK, KEY), f32)
        for q in range(GC // KEY):
            cols = slice(q * KEY, (q + 1) * KEY)
            par = parg[:, cols]
            window = pad[k * BLK : k * BLK + BLK + 8, cols]
            u = taps_of(window, par)
            su = sigmoid(u)
            v = u * su
            x = v * dtx[:, cols]
            xb = x.astype(bf16)
            gate = gate_ref[rows, cols]
            y = y_ref[rows, cols]
            sgt = sigmoid(gate)
            silu_g = gate * sgt
            p = y * silu_g
            dgn = gg_ref[rows, cols] * r_ref[rows]
            sv_ref[5:6, cols] += jnp.sum(dgn * p, axis=0, keepdims=True)
            dp = dgn * par[5:6] - p * c_ref[rows]
            dgate_ref[rows, cols] = (dp * y * (sgt + silu_g * (1.0 - sgt))).astype(bf16)
            dy = dp * silu_g
            sv_ref[6:7, cols] += jnp.sum(dy * v, axis=0, keepdims=True)
            dyb = dy.astype(bf16)
            dye = dy * exx[:, cols]
            dyes.append(dye.astype(bf16))
            oys.append((dye * ch[:, cols]).astype(bf16))
            xt = x * txx[:, cols]
            xts.append(xt.astype(bf16))
            zs.append((xt * qq[:, cols]).astype(bf16))
            zero = jnp.zeros_like(dyb)
            dy2 = jnp.concatenate([jnp.where(low, dyb, zero), jnp.where(low, zero, dyb)], axis=0)
            dm2 = mm_nt(dy2, xb)
            ms = []
            for side in range(2):
                j = 2 * q + side
                spread = sg[rows, j : j + 1] - across[j : j + 1]
                decay = jnp.exp(spread + bias)
                m = decay * sc_ref[k]
                ms.append(m.astype(bf16))
                dm = dm2[side * BLK : (side + 1) * BLK]
                dsc[k] += decay * dm
                e = jnp.where(strict, m * dm, 0.0)
                dsrow_k = jnp.where(col == g * GH + j, jnp.sum(e, axis=1, keepdims=True), dsrow_k)
                ecols.append(jnp.sum(e, axis=0, keepdims=True))
            dx = mm_tn(jnp.concatenate(ms, axis=0), dy2) + qq[:, cols] * txx[:, cols]
            dv = dx * dtx[:, cols] + par[6:7] * dy
            ddts.append((dx * v).astype(bf16))
            du = dv * (su + v * (1.0 - su))
            dpad[rows, cols] = du
            sv_ref[4:5, cols] += jnp.sum(du, axis=0, keepdims=True)
            for t in range(4):
                sv_ref[t : t + 1, cols] += jnp.sum(du * window[5 + t : 133 + t], axis=0, keepdims=True)
        dscol[tile_at, rows] += jnp.where(mine, jnp.concatenate(ecols + ecols, axis=0), 0.0)
        dye = jnp.concatenate(dyes, axis=1)
        xt = jnp.concatenate(xts, axis=1)
        zsum = mm(jnp.concatenate(zs, axis=1), red)
        ddt[rows] += mm(jnp.concatenate(ddts, axis=1), red)
        hterm = eend[k : k + 1] * jnp.sum(dhcar[...] * hb.astype(f32), axis=0, keepdims=True)
        end = jnp.sum(zsum, axis=0, keepdims=True) + mm_hi(hterm, red.astype(f32))
        add = dsrow_k + mm(jnp.concatenate(oys, axis=1), red) - zsum
        dsrow[rows] += add + jnp.where(row == BLK - 1, end, 0.0)
        dkb[rows, KEY:] += mm_nt(dye, hb)
        dkb[rows, :KEY] += mm_nt(xt, dhb)
        if k:
            dhcar[...] = eend[k : k + 1] * dhcar[...] + mm(kt_ref[KEY:, rows], dye)

    for k in range(blocks):
        rows = slice(k * BLK, (k + 1) * BLK)
        for q in range(GC // KEY):
            cols = slice(q * KEY, (q + 1) * KEY)
            par = parg[:, cols]
            window = dpad[k * BLK : k * BLK + BLK + 8, cols]
            out = par[3:4] * window[0:BLK]
            for t in range(3):
                out = out + par[t : t + 1] * window[3 - t : 3 - t + BLK]
            draw_ref[rows, cols] = out.astype(bf16)


def backward_shared(
    rawk_ref, dtr_ref, pv_ref, key_at, ph_ref, kb_ref, dkeys_ref, ddt_ref, sk_ref, sh_ref,
    padk, dpadk, dsc, dkb, dsrow, dscol, ddt,
):
    length = rawk_ref.shape[0]
    blocks = length // BLK
    row = iota((BLK, BLK), 0)
    col = iota((BLK, BLK), 1)
    padk[0:8] = jnp.zeros((8, 2 * KEY), f32)
    padk[8:] = rawk_ref[...]
    dpadk[length:] = jnp.zeros((8, 2 * KEY), f32)
    sk_ref[...] = jnp.zeros_like(sk_ref)
    sh_ref[...] = jnp.zeros_like(sh_ref)
    upper = jnp.where(row <= col, 1.0, 0.0).astype(f32)
    par = pv_ref[:, key_at : key_at + 2 * KEY]
    for k in range(blocks):
        rows = slice(k * BLK, (k + 1) * BLK)
        window = padk[k * BLK : k * BLK + BLK + 8]
        u = taps_of(window, par)
        su = sigmoid(u)
        ds = dsc[k].astype(bf16)
        db = dkb[rows, :KEY] + mm_tn(ds, kb_ref[rows, KEY:])
        dc = dkb[rows, KEY:] + mm(ds, kb_ref[rows, :KEY])
        du = jnp.concatenate([db, dc], axis=1) * (su + u * su * (1.0 - su))
        dpadk[rows] = du
        sk_ref[4:5] += jnp.sum(du, axis=0, keepdims=True)
        for t in range(4):
            sk_ref[t : t + 1] += jnp.sum(du * window[5 + t : 133 + t], axis=0, keepdims=True)
        dla = mm_hi(upper, dsrow[rows] - dscol[:, rows].T)
        z = dtr_ref[rows] + ph_ref[0:1, :]
        rate = jnp.exp(ph_ref[1:2, :])
        dt = jax.nn.softplus(z)
        sh_ref[1:2] += jnp.sum(dla * (-dt * rate), axis=0, keepdims=True)
        dz = (ddt[rows] - dla * rate) * sigmoid(z)
        sh_ref[0:1] += jnp.sum(dz, axis=0, keepdims=True)
        ddt_ref[rows] = dz.astype(bf16)
    for k in range(blocks):
        rows = slice(k * BLK, (k + 1) * BLK)
        window = dpadk[k * BLK : k * BLK + BLK + 8]
        out = par[3:4] * window[0:BLK]
        for t in range(3):
            out = out + par[t : t + 1] * window[3 - t : 3 - t + BLK]
        dkeys_ref[rows] = out.astype(bf16)


def bwd_kernel(
    gate_ref, rawv_ref, rawk_ref, dtr_ref, pv_ref, ph_ref,
    y_ref, gg_ref, hst_ref, r_ref, c_ref, s_ref, st_ref, hl_ref, ehl_ref, kb_ref, kt_ref, sc_ref,
    dproj_ref, sv_ref, sk_ref, sh_ref,
    pad, padk, dpad, dpadk, sg, dhcar, dsc, dkb, dsrow, dscol, ddt,
):
    g = pl.program_id(0)
    length, total = dproj_ref.shape
    wide = GC * pl.num_programs(0)
    shared = (s_ref, st_ref, hl_ref, ehl_ref, kb_ref, kt_ref, sc_ref)

    @pl.when(g == 0)
    def _():
        backward_start(length, pad, dpad, dsc, dkb, dsrow, dscol, ddt)

    gate_at = pl.ds(pl.multiple_of(g * GC, GC), GC)
    draw_at = pl.ds(pl.multiple_of(wide + g * GC, GC), GC)
    backward_group(
        g, gate_ref, rawv_ref, y_ref, gg_ref, hst_ref, r_ref, c_ref, pv_ref, shared,
        dproj_ref.at[:, gate_at], dproj_ref.at[:, draw_at], sv_ref,
        pad, dpad, sg, dhcar, dsc, dkb, dsrow, dscol, ddt,
    )

    @pl.when(g == pl.num_programs(0) - 1)
    def _():
        keys = 2 * wide
        dproj_ref[:, keys + 3 * KEY :] = jnp.zeros((length, total - keys - 3 * KEY), bf16)
        backward_shared(
            rawk_ref, dtr_ref, pv_ref, wide, ph_ref, kb_ref,
            dproj_ref.at[:, keys : keys + 2 * KEY], dproj_ref.at[:, keys + 2 * KEY : keys + 3 * KEY],
            sk_ref, sh_ref, padk, dpadk, dsc, dkb, dsrow, dscol, ddt,
        )


def whole_spec(shape):
    return pl.BlockSpec(shape, lambda g: (0,) * len(shape))


def state_specs(length):
    return (
        ((length, KEY), f32),
        ((KEY, length), f32),
        ((3, length, 2 * KEY), bf16),
        ((8, 2 * KEY), bf16),
        ((length, 2 * KEY), bf16),
        ((2 * KEY, length), bf16),
        ((length // BLK, BLK, BLK), f32),
    )


def proj_specs(length, groups):
    wide = groups * GC
    return [
        pl.BlockSpec((length, GC), lambda g: (0, g)),
        pl.BlockSpec((length, GC), lambda g: (0, groups + g)),
        pl.BlockSpec((length, 2 * KEY), lambda g: (0, 2 * wide // (2 * KEY))),
        pl.BlockSpec((length, KEY), lambda g: (0, 2 * wide // KEY + 2)),
        whole_spec((8, wide + 2 * KEY)),
        whole_spec((8, KEY)),
    ]


def mixer_forward(projected, pv, ph):
    length = projected.shape[0]
    wide = pv.shape[1] - 2 * KEY
    groups = wide // GC
    blocks = length // BLK
    column = pl.BlockSpec((length, GC), lambda g: (0, g))
    shared = state_specs(length)
    return pl.pallas_call(
        fwd_kernel,
        grid=(groups,),
        in_specs=proj_specs(length, groups),
        out_specs=[
            column,
            whole_spec((length, wide)),
            pl.BlockSpec((blocks, KEY, GC), lambda g: (0, 0, g)),
            whole_spec((length, KEY)),
        ]
        + [whole_spec(shape) for shape, _ in shared],
        out_shape=[
            jax.ShapeDtypeStruct((length, wide), f32),
            jax.ShapeDtypeStruct((length, wide), f32),
            jax.ShapeDtypeStruct((blocks, KEY, wide), bf16),
            jax.ShapeDtypeStruct((length, KEY), f32),
        ]
        + [jax.ShapeDtypeStruct(shape, dtype) for shape, dtype in shared],
        scratch_shapes=[
            pltpu.VMEM((length + 8, GC), f32),
            pltpu.VMEM((length + 8, 2 * KEY), f32),
            pltpu.VMEM((length, KEY), f32),
            pltpu.VMEM((KEY, GC), f32),
            pltpu.VMEM((length, KEY), f32),
        ],
        name="mixer_forward",
    )(projected, projected, projected, projected, pv, ph)


def backward_scratch(length):
    return [
        pltpu.VMEM((length + 8, GC), f32),
        pltpu.VMEM((length + 8, 2 * KEY), f32),
        pltpu.VMEM((length + 8, GC), f32),
        pltpu.VMEM((length + 8, 2 * KEY), f32),
        pltpu.VMEM((length, KEY), f32),
        pltpu.VMEM((KEY, GC), f32),
        pltpu.VMEM((length // BLK, BLK, BLK), f32),
        pltpu.VMEM((length, 2 * KEY), f32),
        pltpu.VMEM((length, KEY), f32),
        pltpu.VMEM((KEY, length), f32),
        pltpu.VMEM((length, KEY), f32),
    ]


def mixer_backward(projected, pv, ph, mixed, grad_gated, states, inverse, pull, shared):
    length, total = projected.shape
    wide = pv.shape[1] - 2 * KEY
    groups = wide // GC
    blocks = length // BLK
    column = pl.BlockSpec((length, GC), lambda g: (0, g))
    return pl.pallas_call(
        bwd_kernel,
        grid=(groups,),
        in_specs=proj_specs(length, groups)
        + [
            column,
            column,
            pl.BlockSpec((blocks, KEY, GC), lambda g: (0, 0, g)),
            whole_spec((length, KEY)),
            whole_spec((length, KEY)),
        ]
        + [whole_spec(shape) for shape, _ in state_specs(length)],
        out_specs=[
            whole_spec((length, total)),
            pl.BlockSpec((8, GC), lambda g: (0, g)),
            whole_spec((8, 2 * KEY)),
            whole_spec((8, KEY)),
        ],
        out_shape=[
            jax.ShapeDtypeStruct((length, total), bf16),
            jax.ShapeDtypeStruct((8, wide), f32),
            jax.ShapeDtypeStruct((8, 2 * KEY), f32),
            jax.ShapeDtypeStruct((8, KEY), f32),
        ],
        scratch_shapes=backward_scratch(length),
        name="mixer_backward",
    )(projected, projected, projected, projected, pv, ph, mixed, grad_gated, states, inverse, pull, *shared)


MESH = pl.DeviceIdType.MESH
HALF = 256


ORDERS = ("xylh", "yxlh", "lhxy")
GATHER_WAITS = (2, 4, 8, 13, 15)
SCATTER_WAITS = (2, 6, 10, 14, 18)


def places():
    d, f = lax.axis_index("dp"), lax.axis_index("fsdp")
    bits = {"x": d % 2, "y": f // 2, "l": d // 2 % 2, "h": d // 4, "c": f % 2}
    far = {"x": (1, 0), "y": (0, 2), "l": (2, 0), "h": (4, 0), "c": (0, 1)}
    hops = {k: tuple(w * (1 - 2 * bits[k]) if w else 0 for w in far[k]) for k in far}
    return d, f, bits, hops


def kind_of(u):
    r = lax.rem(u, 9)
    along_y = (r == 1) | (r == 3) | (r == 6) | ((r == 7) & (lax.rem(u // 9, 2) == 1))
    return jnp.where((r == 4) | (r == 8), 2, jnp.where(along_y, 1, 0))


def pick(kind, values):
    if isinstance(kind, int):
        return values[kind]
    if all(v is values[0] for v in values):
        return values[0]
    return jnp.where(kind == 0, values[0], jnp.where(kind == 1, values[1], values[2]))


def exchange(place, kind, stage):
    d, f, bits, hops = place
    axes = "ccc" if stage == 0 else [order[stage - 1] for order in ORDERS]
    side = pick(kind, [bits[a] for a in axes])
    return side, (d + pick(kind, [hops[a][0] for a in axes]), f + pick(kind, [hops[a][1] for a in axes]))


def strides(kind):
    return {a: pick(kind, [8 >> order.index(a) for order in ORDERS]) for a in "xylh"}


def position(kind, bits):
    step = strides(kind)
    return sum(bits[a] * step[a] for a in "xylh")


def all_positions(kind):
    step = strides(kind)
    out = []
    for i in range(32):
        bits = {"x": i // 4 % 2, "y": i // 2 % 2, "l": i // 8 % 2, "h": i // 16}
        out.append((i % 2, sum(step[a] for a in "xylh" if bits[a])))
    return out


def greet(partners):
    barrier = pltpu.get_barrier_semaphore()
    for partner in partners:
        pl.semaphore_signal(barrier, inc=1, device_id=partner, device_id_type=MESH)
    pl.semaphore_wait(barrier, len(partners))


def spread_lanes(tiles, width, lane, count):
    out = [jnp.zeros(tiles[0].shape, f32) for _ in range(count)]
    for i, tile in enumerate(tiles):
        at, shift = divmod(i * width, KEY)
        turned = pltpu.roll(tile, shift, 1) if shift else tile
        end = shift + width
        out[at] = out[at] + jnp.where((lane >= shift) & (lane < end), turned, 0.0)
        if end > KEY:
            out[at + 1] = out[at + 1] + jnp.where(lane < end - KEY, turned, 0.0)
    return out


def forward_kernel(
    n_in, n_out, lengths_ref, hidden_ref, cot_ref, w_ref, wd_ref, wo_ref, conv_ref, shift_ref, gate_ref, pre_ref,
    dt_ref, log_ref, skip_ref,
    w_out, proj_out, mixed_out, states_out, flipped_gated_out, gg_out,
    out_ref, flipped_ref, live_ref, ph_ref, pv_ref, gain, r_ref, c_ref, s_ref, st_ref, hl_ref, ehl_ref, kb_ref, kt_ref, sc_ref,
    held, tiles, w_stage, wo_stage, proj_stage, mixed_stage, states_stage, flip_stage, normed, gated, big,
    pad, padk, sg, hcar, ssq, dots,
    send, recv, tile_sem, out_sem,
):
    rb = w_ref.shape[0]
    length, width = hidden_ref.shape
    wide = big.shape[1]
    n = n_in + n_out
    place = places()
    greet([exchange(place, 0, stage)[1] for stage in range(5)])
    count = (1, 2, 4, 8, 16)

    def columns(i, half):
        group = (i - 1) * HALF + half * wide
        return pl.ds(pl.multiple_of(jnp.where(i == 0, 2 * wide + half * HALF, group), HALF), HALF)

    def own_at(kind):
        return place[2]["c"] * 16 + position(kind, place[2])

    def copy(stage, u):
        kind = kind_of(u)
        start = own_at(kind) // count[stage] * count[stage]
        block = held.at[u, pl.ds(start, count[stage])]
        return pltpu.make_async_remote_copy(
            src_ref=block,
            dst_ref=block,
            send_sem=send.at[u, stage],
            recv_sem=recv.at[u, stage],
            device_id=exchange(place, kind, 4 - stage)[1],
            device_id_type=MESH,
        )

    def tile_copy(stage):
        block = tiles.at[pl.ds(own_at(0) // count[stage] * count[stage], count[stage])]
        return pltpu.make_async_remote_copy(
            src_ref=block,
            dst_ref=block,
            send_sem=tile_sem.at[0, stage],
            recv_sem=tile_sem.at[1, stage],
            device_id=exchange(place, 0, 4 - stage)[1],
            device_id_type=MESH,
        )

    def weight_stores(i):
        slot = lax.rem(i, 2)
        copies = []
        for half in range(2):
            cols = slice(half * HALF, (half + 1) * HALF)
            copies.append(
                pltpu.make_async_copy(
                    w_stage.at[slot, :, cols], w_out.at[:, columns(i, half)], out_sem.at[half, slot]
                )
            )
            copies.append(
                pltpu.make_async_copy(
                    proj_stage.at[slot, :, cols], proj_out.at[:, columns(i, half)], out_sem.at[2 + half, slot]
                )
            )
        return copies

    def group_stores(i):
        slot = lax.rem(i, 2)
        cols = pl.ds(pl.multiple_of((i - 1) * HALF, HALF), HALF)
        return (
            pltpu.make_async_copy(mixed_stage.at[slot], mixed_out.at[:, cols], out_sem.at[4, slot]),
            pltpu.make_async_copy(states_stage.at[slot], states_out.at[:, :, cols], out_sem.at[5, slot]),
        )

    def flip_store(k):
        return pltpu.make_async_copy(
            flip_stage.at[k % 2], flipped_gated_out.at[k * HALF : (k + 1) * HALF], out_sem.at[6, k % 2]
        )

    tile = tiles.at[own_at(0)]
    tile[...] = jnp.zeros((8, KEY), f32)
    tile[0:4, 0 : conv_ref.shape[1]] = conv_ref[...].astype(f32)
    tile[4:5, 0 : shift_ref.shape[1]] = shift_ref[...].astype(f32)
    tile[5:6, 0 : gate_ref.shape[1]] = gate_ref[...].astype(f32)
    tile[6:7, 0 : pre_ref.shape[1]] = pre_ref[...].astype(f32)
    tile_copy(0).start()
    heads = dt_ref.shape[1]
    ph_ref[...] = jnp.zeros_like(ph_ref)
    ph_ref[0:1, 0:heads] = dt_ref[...].astype(f32)
    ph_ref[1:2, 0:heads] = log_ref[...].astype(f32)
    ph_ref[2:3, 0:heads] = skip_ref[...].astype(f32)
    live_ref[...] = jnp.where(iota((length, KEY), 0) < lengths_ref[0], 1.0, 0.0).astype(f32)

    held[0, own_at(kind_of(0))] = w_ref[:, 2 * wide : 2 * wide + HALF]
    held[1, own_at(kind_of(1))] = jnp.zeros((rb, HALF), bf16)
    held[1, own_at(kind_of(1)), :, 0:heads] = wd_ref[...]

    def land(u, carry):
        group = pl.ds(pl.multiple_of((u // 2 - 1) * HALF + lax.rem(u, 2) * wide, HALF), HALF)
        held[u, own_at(kind_of(u))] = w_ref[:, group]
        return carry

    lax.fori_loop(2, 2 * n_in, land, 0)
    for u in range(2 * n_out):
        rows = slice(u % 2 * rb, (u % 2 + 1) * rb)
        held[2 * n_in + u, own_at(kind_of(2 * n_in + u))] = wo_ref[rows, u // 2 * HALF : (u // 2 + 1) * HALF]

    def first_chunk():
        lane = iota((8, KEY), 1)
        row = iota((8, KEY), 0)
        order = [tiles[c * 16 + at] for c, at in all_positions(0)]
        conv = spread_lanes(order, (wide + 2 * KEY) // 32, lane, wide // KEY + 2)
        gate = spread_lanes(order, wide // 32, lane, wide // KEY)
        pre = spread_lanes(order, width // 32, lane, width // KEY)
        skips = split(jnp.broadcast_to(ph_ref[2:3], (8, KEY)))
        for k, tile in enumerate(conv):
            cols = slice(k * KEY, (k + 1) * KEY)
            if k < wide // KEY:
                if k % 2 == 0:
                    skip = mm(skips, expander(k // 2))
                skip_part = skip[:, k % 2 * KEY : (k % 2 + 1) * KEY]
                tile = jnp.where(row == 5, gate[k], jnp.where(row == 6, skip_part, tile))
            pv_ref[:, cols] = tile
        for k, tile in enumerate(pre):
            gain[:, k * KEY : (k + 1) * KEY] = tile
        for k in range(0, length, KEY):
            values = hidden_ref[k : k + KEY].astype(f32)
            mean = jnp.mean(values * values, axis=1, keepdims=True)
            rows = (values * lax.rsqrt(mean + epsilon) * gain[6:7]).astype(bf16)
            normed[k : k + KEY] = rows
            flipped_ref[:, k : k + KEY] = rows.T

    def keys_chunk(slot):
        forward_shared(
            proj_stage.at[slot, :, 0:HALF], proj_stage.at[slot, :, HALF : HALF + KEY], pv_ref, wide, ph_ref,
            s_ref, st_ref, hl_ref, ehl_ref, kb_ref, kt_ref, sc_ref, padk,
        )
        pad[0:8] = jnp.zeros((8, GC), f32)
        ssq[...] = jnp.zeros_like(ssq)
        dots[...] = jnp.zeros_like(dots)

    def project(slot):
        for half in range(2):
            cols = slice(half * HALF, (half + 1) * HALF)
            proj_stage[slot, :, cols] = mm(normed[...], w_stage[slot, :, cols])

    def group_chunk(slot, g):
        forward_group(
            g, proj_stage.at[slot, :, 0:HALF], proj_stage.at[slot, :, HALF : 2 * HALF], pv_ref,
            s_ref, st_ref, hl_ref, ehl_ref, kb_ref, kt_ref, sc_ref,
            mixed_stage.at[slot], big, states_stage.at[slot], pad, sg, hcar, ssq,
        )

    def finish_groups():
        mean = jnp.sum(ssq[...], axis=1, keepdims=True) / wide
        r_ref[...] = jnp.broadcast_to(lax.rsqrt(mean + epsilon), r_ref.shape)
        for k in range(wide // HALF):
            if k >= 2:
                flip_store(k - 2).wait()
            for q in range(HALF // KEY):
                cols = slice(k * HALF + q * KEY, k * HALF + (q + 1) * KEY)
                part = (big[:, cols] * r_ref[...] * pv_ref[5:6, cols]).astype(bf16)
                gated[:, cols] = part
                flip_stage[k % 2, q * KEY : (q + 1) * KEY] = part.T
            flip_store(k).start()
        for k in range(wide // HALF - 2, wide // HALF):
            flip_store(k).wait()

    def out_chunk_first(i):
        j = i - n_in
        for half in range(2):
            for b, (c, at) in enumerate(all_positions(kind_of(2 * i + half))):
                wo_stage[(2 * b + half) * rb : (2 * b + half + 1) * rb] = held[2 * i + half, c * 16 + at]
        cols = pl.ds(pl.multiple_of(j * HALF, HALF), HALF)
        branch = mm(gated[...], wo_stage[...])
        live = jnp.concatenate([live_ref[...]] * (HALF // KEY), axis=1)
        out_ref[:, cols] = (hidden_ref[:, cols].astype(f32) + live * branch).astype(bf16)
        upstream = (cot_ref[:, cols].astype(f32) * live).astype(bf16)
        dots[...] += upstream.astype(f32) * branch

    def out_chunk_second(i):
        j = i - n_in
        cols = pl.ds(pl.multiple_of(j * HALF, HALF), HALF)
        live = jnp.concatenate([live_ref[...]] * (HALF // KEY), axis=1)
        upstream = (cot_ref[:, cols].astype(f32) * live).astype(bf16)
        for q in range(0, wide, 512):
            more = mm_nt(upstream, wo_stage[q : q + 512])

            @pl.when(j == 0)
            def _():
                big[:, q : q + 512] = more

            @pl.when(j > 0)
            def _():
                big[:, q : q + 512] += more

    def consume_first(i):
        slot = lax.rem(i, 2)

        @pl.when(i < n_in)
        def _():
            @pl.when(i >= 2)
            def _():
                for store in weight_stores(i - 2):
                    store.wait()

            for half in range(2):
                for b, (c, at) in enumerate(all_positions(kind_of(2 * i + half))):
                    w_stage[slot, b * rb : (b + 1) * rb, half * HALF : (half + 1) * HALF] = held[
                        2 * i + half, c * 16 + at
                    ]

            @pl.when(i == 0)
            def _():
                first_chunk()

            project(slot)
            for store in weight_stores(i):
                store.start()

        @pl.when(i >= n_in)
        def _():
            out_chunk_first(i)

    def consume_second(i):
        slot = lax.rem(i, 2)

        @pl.when(i == 0)
        def _():
            keys_chunk(slot)

        @pl.when((i > 0) & (i < n_in))
        def _():
            @pl.when(i >= 3)
            def _():
                for store in group_stores(i - 2):
                    store.wait()

            group_chunk(slot, i - 1)
            for store in group_stores(i):
                store.start()

        @pl.when(i == n_in - 1)
        def _():
            finish_groups()

        @pl.when(i >= n_in)
        def _():
            out_chunk_second(i)

    def tick(t, carry):
        @pl.when(t < 2 * n)
        def _():
            copy(0, t).start()

        for stage in range(5):
            u = t - GATHER_WAITS[stage]

            @pl.when(u == 0)
            def _(stage=stage):
                tile_copy(stage).wait()
                if stage < 4:
                    tile_copy(stage + 1).start()

            @pl.when((u >= 0) & (u < 2 * n))
            def _(stage=stage, u=u):
                copy(stage, u).wait()
                if stage < 4:
                    copy(stage + 1, u).start()

        u = t - GATHER_WAITS[4]

        @pl.when((u >= 1) & (lax.rem(u, 2) == 1))
        def _():
            consume_first(u // 2)

        @pl.when((u >= 2) & (lax.rem(u, 2) == 0))
        def _():
            consume_second(u // 2 - 1)

        return carry

    lax.fori_loop(0, 2 * n + GATHER_WAITS[4] + 1, tick, 0)
    whole = pltpu.make_async_copy(big, gg_out, out_sem.at[6, 0])
    whole.start()
    pull = jnp.sum(dots[...], axis=1, keepdims=True) / wide
    c_ref[...] = r_ref[...] * r_ref[...] * pull
    for i in (n_in - 2, n_in - 1):
        for store in weight_stores(i) + list(group_stores(i)):
            store.wait()
    whole.wait()


def gather_forward(lengths, hidden, cotangent, shard, dt_shard, out_shard, *vectors):
    length, width = hidden.shape
    rb = shard.shape[0]
    columns = shard.shape[1] + 2 * KEY
    wide = out_shard.shape[0] * 32
    n_in, n_out = columns // (2 * HALF), width // HALF
    blocks = length // BLK
    vmem = pl.BlockSpec(memory_space=pltpu.VMEM)
    anywhere = pl.BlockSpec(memory_space=pl.ANY)
    struct = jax.ShapeDtypeStruct
    shared = [struct(shape, dtype) for shape, dtype in state_specs(length)]
    return pl.pallas_call(
        partial(forward_kernel, n_in, n_out),
        out_shape=[
            struct((width, columns), bf16),
            struct((length, columns), f32),
            struct((length, wide), f32),
            struct((blocks, KEY, wide), bf16),
            struct((wide, length), bf16),
            struct((length, wide), f32),
            struct((length, width), bf16),
            struct((width, length), bf16),
            struct((length, KEY), f32),
            struct((8, KEY), f32),
            struct((8, wide + 2 * KEY), f32),
            struct((8, width), f32),
            struct((length, KEY), f32),
            struct((length, KEY), f32),
        ]
        + shared,
        in_specs=[pl.BlockSpec(memory_space=pltpu.SMEM)] + [vmem] * (5 + len(vectors)),
        out_specs=[anywhere] * 6 + [vmem] * (8 + len(shared)),
        scratch_shapes=[
            pltpu.VMEM((2 * (n_in + n_out), 32, rb, HALF), bf16),
            pltpu.VMEM((32, 8, KEY), f32),
            pltpu.VMEM((2, width, 2 * HALF), bf16),
            pltpu.VMEM((wide, HALF), bf16),
            pltpu.VMEM((2, length, 2 * HALF), f32),
            pltpu.VMEM((2, length, HALF), f32),
            pltpu.VMEM((2, blocks, KEY, HALF), bf16),
            pltpu.VMEM((2, HALF, length), bf16),
            pltpu.VMEM((length, width), bf16),
            pltpu.VMEM((length, wide), bf16),
            pltpu.VMEM((length, wide), f32),
            pltpu.VMEM((length + 8, GC), f32),
            pltpu.VMEM((length + 8, 2 * KEY), f32),
            pltpu.VMEM((length, KEY), f32),
            pltpu.VMEM((KEY, GC), f32),
            pltpu.VMEM((length, KEY), f32),
            pltpu.VMEM((length, HALF), f32),
            pltpu.SemaphoreType.DMA((2 * (n_in + n_out), 5)),
            pltpu.SemaphoreType.DMA((2 * (n_in + n_out), 5)),
            pltpu.SemaphoreType.DMA((2, 5)),
            pltpu.SemaphoreType.DMA((7, 2)),
        ],
        compiler_params=pltpu.CompilerParams(
            collective_id=2, has_side_effects=True, vmem_limit_bytes=63 << 20
        ),
        name="gather_forward",
    )(lengths, hidden, cotangent, shard, dt_shard, out_shard, *vectors)


EARLY = 7


def gather_lanes(row_tiles, width, lane, i):
    at, shift = divmod(i * width, KEY)
    if shift == 0:
        return row_tiles[at]
    first = pltpu.roll(row_tiles[at], KEY - shift, 1)
    if shift + width <= KEY:
        return first
    return jnp.where(lane < KEY - shift, first, pltpu.roll(row_tiles[at + 1], KEY - shift, 1))


def backward_kernel(
    n_in, n_out, hidden_ref, cot_ref, live_ref, flipped_ref, gated_ref, pv_ref, gain_ref, ph_ref, r_ref, c_ref,
    s_ref, st_ref, hl_ref, ehl_ref, kb_ref, kt_ref, sc_ref,
    proj_in, mixed_in, gg_in, states_in, w_in,
    rows_out, in_ref, dt_ref, out_ref, tile_out, sums_ref,
    parts, r0, r1, r2, r3, r4, tiles, t0, t1, t2, t3, t4, sums, sums_in,
    stage_in, states_stage, w_stage, keys_stage, dchunk, rows_grad, sv, sv_all, sk, sh, skip_sum, gain_sum,
    pad, padk, dpad, dpadk, sg, dhcar, dsc, dkb, dsrow, dscol, ddt,
    send, recv, tile_sem, sums_sem, in_sem, out_sem,
):
    length, width = hidden_ref.shape
    wide = mixed_in.shape[1]
    rb = in_ref.shape[0]
    n = n_in + n_out
    groups = n_in - 1
    keys_tick = n - 2
    shared = (s_ref, st_ref, hl_ref, ehl_ref, kb_ref, kt_ref, sc_ref)
    place = places()
    held = (r0, r1, r2, r3, r4)
    tile_source = (tiles, t0, t1, t2, t3, t4)
    greet([exchange(place, 0, stage)[1] for stage in range(5)])

    def is_out(t):
        return ((t < 3 * n_out - 3) & (lax.rem(t, 3) == 0)) | (t == n - 1)

    def out_index(t):
        return jnp.where(t == n - 1, n_out - 1, t // 3)

    def group_index(t):
        return jnp.where(t < 3 * n_out - 3, t // 3 * 2 + lax.rem(t, 3) - 1, t - n_out + 1)

    def loads(g):
        slot = lax.rem(g, 2)
        near = pl.ds(pl.multiple_of(g * HALF, HALF), HALF)
        far = pl.ds(pl.multiple_of(wide + g * HALF, HALF), HALF)
        pairs = (
            (proj_in.at[:, near], stage_in.at[slot, 0]),
            (proj_in.at[:, far], stage_in.at[slot, 1]),
            (mixed_in.at[:, near], stage_in.at[slot, 2]),
            (gg_in.at[:, near], stage_in.at[slot, 3]),
            (states_in.at[:, :, near], states_stage.at[slot]),
        )
        return [pltpu.make_async_copy(a, b, in_sem.at[k, slot]) for k, (a, b) in enumerate(pairs)]

    def weight_loads(g):
        slot = lax.rem(g, 2)
        first = jnp.where(g == groups, 2 * wide, g * HALF)
        second = jnp.where(g == groups, 2 * wide + HALF, wide + g * HALF)
        return [
            pltpu.make_async_copy(
                w_in.at[:, pl.ds(pl.multiple_of(at, HALF), HALF)],
                w_stage.at[slot, :, half * HALF : (half + 1) * HALF],
                in_sem.at[5 + half, slot],
            )
            for half, at in enumerate((first, second))
        ]

    keys_load = pltpu.make_async_copy(proj_in.at[:, 2 * wide : 2 * wide + 3 * KEY], keys_stage, in_sem.at[7, 0])
    for load in loads(0) + weight_loads(0) + [keys_load]:
        load.start()
    rows_store = pltpu.make_async_copy(rows_grad, rows_out, out_sem.at[0])

    def sums_copy(stage):
        return pltpu.make_async_remote_copy(
            src_ref=sums.at[stage],
            dst_ref=sums_in.at[stage],
            send_sem=sums_sem.at[0, stage],
            recv_sem=sums_sem.at[1, stage],
            device_id=exchange(place, 0, stage)[1],
            device_id_type=MESH,
        )

    def tile_copy(stage):
        count = 16 >> stage
        return pltpu.make_async_remote_copy(
            src_ref=tile_source[stage].at[pl.ds((1 - exchange(place, 0, stage)[0]) * count, count)],
            dst_ref=tile_source[stage + 1],
            send_sem=tile_sem.at[0, stage],
            recv_sem=tile_sem.at[1, stage],
            device_id=exchange(place, 0, stage)[1],
            device_id_type=MESH,
        )

    def spot(stage, u):
        return lax.rem(u, 2 * EARLY) if stage == 0 else u

    def copy(stage, u):
        count = 16 >> stage
        side, partner = exchange(place, kind_of(u), stage)
        if stage == 0:
            src = parts.at[lax.rem(u // 2, 2), 1 - side, lax.rem(u, 2)]
        else:
            src = held[stage - 1].at[spot(stage - 1, u), pl.ds((1 - side) * count, count)]
        return pltpu.make_async_remote_copy(
            src_ref=src,
            dst_ref=held[stage].at[spot(stage, u)],
            send_sem=send.at[u, stage],
            recv_sem=recv.at[u, stage],
            device_id=partner,
            device_id_type=MESH,
        )

    backward_start(length, pad, dpad, dsc, dkb, dsrow, dscol, ddt)
    skip_sum[...] = jnp.zeros_like(skip_sum)
    rows_grad[...] = jnp.zeros_like(rows_grad)

    def out_chunk(slot, t):
        j = out_index(t)
        where = [all_positions(kind_of(2 * t + half)) for half in range(2)]
        cols = pl.ds(pl.multiple_of(j * HALF, HALF), HALF)
        live = jnp.concatenate([live_ref[...]] * (HALF // KEY), axis=1)
        upstream = (cot_ref[:, cols].astype(f32) * live).astype(bf16)
        for z in range(4):
            res = mm(gated_ref[z * 16 * rb : (z + 1) * 16 * rb], upstream)
            for b in range(8):
                for half in range(2):
                    c, at = where[half][z * 8 + b]
                    at_row = (2 * b + half) * rb
                    parts[slot, c, half, at] = res[at_row : at_row + rb].astype(bf16)

    def weight_chunk(slot, t, g):
        for load in weight_loads(g):
            load.wait()
        at = lax.rem(g, 2)
        for half in range(2):
            right = dchunk[:, half * HALF : (half + 1) * HALF]
            where = all_positions(kind_of(2 * t + half))
            for z in range(4):
                res = mm(flipped_ref[z * 8 * rb : (z + 1) * 8 * rb], right)
                for b in range(8):
                    c, to = where[z * 8 + b]
                    parts[slot, c, half, to] = res[b * rb : (b + 1) * rb].astype(bf16)
        for k in range(0, width, 512):
            rows_grad[:, k : k + 512] += mm_nt(dchunk[...], w_stage[at, k : k + 512])

    def group_chunk(t):
        g = group_index(t)

        for load in weight_loads(g + 1):
            load.start()

        @pl.when(g + 1 < groups)
        def _():
            for load in loads(g + 1):
                load.start()

        for load in loads(g):
            load.wait()
        at = lax.rem(g, 2)
        backward_group(
            g, stage_in.at[at, 0], stage_in.at[at, 1], stage_in.at[at, 2], stage_in.at[at, 3], states_stage.at[at],
            r_ref, c_ref, pv_ref, shared, dchunk.at[:, 0:HALF], dchunk.at[:, HALF : 2 * HALF], sv,
            pad, dpad, sg, dhcar, dsc, dkb, dsrow, dscol, ddt,
        )

    def group_chunk_end(slot, t):
        g = group_index(t)
        sv_all[:, pl.ds(pl.multiple_of(g * HALF, HALF), HALF)] = sv[...]
        skip_sum[...] += mm_hi(sv[...], reducer(g).astype(f32))
        weight_chunk(slot, t, g)

    def keys_chunk():
        keys_load.wait()
        dchunk[:, 3 * KEY :] = jnp.zeros((length, KEY), bf16)
        backward_shared(
            keys_stage.at[:, 0:HALF], keys_stage.at[:, HALF : HALF + KEY], pv_ref, wide, ph_ref, kb_ref,
            dchunk.at[:, 0:HALF], dchunk.at[:, HALF : HALF + KEY], sk, sh,
            padk, dpadk, dsc, dkb, dsrow, dscol, ddt,
        )

    def keys_chunk_end(slot):
        weight_chunk(slot, keys_tick, groups)
        for half in range(2):
            copy(0, 2 * keys_tick + half).start()
        gain = gain_ref[6:7]
        gain_sum[...] = jnp.zeros_like(gain_sum)
        for k in range(0, length, KEY):
            values = hidden_ref[k : k + KEY].astype(f32)
            inverse = lax.rsqrt(jnp.mean(values * values, axis=1, keepdims=True) + epsilon)
            grads = rows_grad[k : k + KEY]
            gain_sum[0:1] += jnp.sum(grads * values * inverse, axis=0, keepdims=True)
            scaled = grads * gain
            pull = jnp.sum(scaled * values, axis=1, keepdims=True) / width
            back = inverse * scaled - values * (inverse * inverse * inverse * pull)
            rows_grad[k : k + KEY] = cot_ref[k : k + KEY].astype(f32) + back
        rows_store.start()
        row = iota((8, KEY), 0)
        lane = iota((8, KEY), 1)
        conv = [sv_all[:, k * KEY : (k + 1) * KEY] for k in range(wide // KEY)]
        gate = conv
        conv = conv + [sk[:, 0:KEY], sk[:, KEY : 2 * KEY]]
        pre = [jnp.broadcast_to(gain_sum[0:1, k * KEY : (k + 1) * KEY], (8, KEY)) for k in range(width // KEY)]
        for i, (c, at) in enumerate(all_positions(0)):
            tile = gather_lanes(conv, (wide + 2 * KEY) // 32, lane, i)
            tile = jnp.where(row == 5, gather_lanes(gate, wide // 32, lane, i), tile)
            tiles[c * 16 + at] = jnp.where(row == 6, gather_lanes(pre, width // 32, lane, i), tile)
        tile_copy(0).start()
        sums[0] = jnp.where(row == 2, skip_sum[6:7], sh[...])
        sums_copy(0).start()

    def write_out(u, value):
        i, half = u // 2, lax.rem(u, 2)

        @pl.when(is_out(i))
        def _():
            cols = pl.ds(pl.multiple_of(out_index(i) * HALF, HALF), HALF)
            out_ref[pl.ds(pl.multiple_of(half * rb, 16), rb), cols] = value

        @pl.when(jnp.logical_not(is_out(i)) & (i != keys_tick))
        def _():
            cols = pl.ds(pl.multiple_of(half * wide + group_index(i) * HALF, HALF), HALF)
            in_ref[:, cols] = value

        @pl.when(u == 2 * keys_tick)
        def _():
            in_ref[:, 2 * wide : 2 * wide + HALF] = value

        @pl.when(u == 2 * keys_tick + 1)
        def _():
            dt_ref[...] = value[:, :KEY]

    def first_step(t):
        @pl.when(jnp.logical_not(is_out(t)) & (t != keys_tick))
        def _():
            group_chunk(t)

        @pl.when(t == keys_tick)
        def _():
            keys_chunk()

    def second_step(t):
        slot = lax.rem(t, 2)

        @pl.when(t >= 2)
        def _():
            for half in range(2):
                copy(0, 2 * (t - 2) + half).wait_send()

        @pl.when(is_out(t))
        def _():
            out_chunk(slot, t)

        @pl.when(jnp.logical_not(is_out(t)) & (t != keys_tick))
        def _():
            group_chunk_end(slot, t)

        @pl.when(t == keys_tick)
        def _():
            keys_chunk_end(slot)

        @pl.when(t != keys_tick)
        def _():
            for half in range(2):
                copy(0, 2 * t + half).start()

    def tick(step, carry):
        t = step // 2

        @pl.when((t < n) & (lax.rem(step, 2) == 0))
        def _():
            first_step(t)

        @pl.when((t < n) & (lax.rem(step, 2) == 1))
        def _():
            second_step(t)

        for stage in range(5):
            u = step - SCATTER_WAITS[stage]
            count = 16 >> stage

            @pl.when(u == 2 * keys_tick)
            def _(stage=stage, count=count):
                sums_copy(stage).wait()
                tile_copy(stage).wait()
                total = tile_source[stage + 1][...] + tile_source[stage][
                    pl.ds(exchange(place, 0, stage)[0] * count, count)
                ]
                if stage < 4:
                    sums[stage + 1] = sums[stage] + sums_in[stage]
                    sums_copy(stage + 1).start()
                    tile_source[stage + 1][...] = total
                    tile_copy(stage + 1).start()
                else:
                    sums_ref[...] = sums[stage] + sums_in[stage]
                    tile_out[...] = total[0]

            @pl.when((u >= 0) & (u < 2 * n))
            def _(stage=stage, u=u, count=count):
                done = copy(stage, u)
                side, _ = exchange(place, kind_of(u), stage)
                if stage == 0:
                    done.wait_recv()
                    mine = parts[lax.rem(u // 2, 2), side, lax.rem(u, 2)]
                else:
                    done.wait()
                    mine = held[stage - 1][spot(stage - 1, u), pl.ds(side * count, count)]
                if stage < 4:
                    at = spot(stage, u)
                    held[stage][at] = (held[stage][at].astype(f32) + mine.astype(f32)).astype(bf16)
                    copy(stage + 1, u).start()
                else:
                    write_out(u, held[stage][u, 0].astype(f32) + mine[0].astype(f32))

        return carry

    lax.fori_loop(0, 2 * n + SCATTER_WAITS[4], tick, 0)
    for u in range(2 * n - 4, 2 * n):
        copy(0, u).wait_send()
    rows_store.wait()


def backward_scatter(
    hidden, cotangent, live, flipped, gated_flipped, pv, gains, ph, inverse, pull, shared,
    projected, mixed, grad_gated, states, w_in, rb,
):
    length, width = hidden.shape
    columns = projected.shape[1]
    wide = mixed.shape[1]
    n_in, n_out = columns // (2 * HALF), width // HALF
    n = n_in + n_out
    blocks = length // BLK
    vmem = pl.BlockSpec(memory_space=pltpu.VMEM)
    anywhere = pl.BlockSpec(memory_space=pl.ANY)
    struct = jax.ShapeDtypeStruct
    return pl.pallas_call(
        partial(backward_kernel, n_in, n_out),
        out_shape=[
            struct((length, width), f32),
            struct((rb, columns - 2 * KEY), f32),
            struct((rb, KEY), f32),
            struct((2 * rb, width), f32),
            struct((8, KEY), f32),
            struct((8, KEY), f32),
        ],
        in_specs=[vmem] * 17 + [anywhere] * 5,
        out_specs=[anywhere] + [vmem] * 5,
        scratch_shapes=[pltpu.VMEM((2, 2, 2, 16, rb, HALF), bf16)]
        + [pltpu.VMEM((2 * (n if stage else EARLY), 16 >> stage, rb, HALF), bf16) for stage in range(5)]
        + [pltpu.VMEM((32 >> stage, 8, KEY), f32) for stage in range(6)]
        + [pltpu.VMEM((5, 8, KEY), f32)] * 2
        + [
            pltpu.VMEM((2, 4, length, HALF), f32),
            pltpu.VMEM((2, blocks, KEY, HALF), bf16),
            pltpu.VMEM((2, width, 2 * HALF), bf16),
            pltpu.VMEM((length, 3 * KEY), f32),
            pltpu.VMEM((length, 2 * HALF), bf16),
            pltpu.VMEM((length, width), f32),
            pltpu.VMEM((8, HALF), f32),
            pltpu.VMEM((8, wide), f32),
            pltpu.VMEM((8, HALF), f32),
            pltpu.VMEM((8, KEY), f32),
            pltpu.VMEM((8, KEY), f32),
            pltpu.VMEM((8, width), f32),
        ]
        + backward_scratch(length)
        + [pltpu.SemaphoreType.DMA((2 * n, 5))] * 2
        + [pltpu.SemaphoreType.DMA((2, 5))] * 2
        + [pltpu.SemaphoreType.DMA((8, 2)), pltpu.SemaphoreType.DMA((1,))],
        compiler_params=pltpu.CompilerParams(
            collective_id=1, has_side_effects=True, vmem_limit_bytes=67043328
        ),
        name="backward_scatter",
    )(
        hidden, cotangent, live, flipped, gated_flipped, pv, gains, ph, inverse, pull, *shared,
        projected, mixed, grad_gated, states, w_in,
    )


def finish_kernel(tile_ref, sums_ref, dt_in, *refs):
    big_in, refs = refs[:4], refs[4:]
    big_out, (pre_ref, dt_ref, conv_ref, shift_ref, bias_ref, log_ref, skip_ref, gate_ref) = refs[:4], refs[4:12]
    stages, (sem,) = refs[12:16], refs[16:]
    reads = [pltpu.make_async_copy(a, s, sem.at[0, k]) for k, (a, s) in enumerate(zip(big_in, stages))]
    writes = [pltpu.make_async_copy(s, b, sem.at[1, k]) for k, (s, b) in enumerate(zip(stages, big_out))]
    for read in reads:
        read.start()
    pre_ref[...] = tile_ref[6:7, 0 : pre_ref.shape[1]]
    dt_ref[...] = dt_in[:, 0 : dt_ref.shape[1]]
    conv_ref[...] = tile_ref[0:4, 0 : conv_ref.shape[1]]
    shift_ref[...] = tile_ref[4:5, 0 : shift_ref.shape[1]]
    gate_ref[...] = tile_ref[5:6, 0 : gate_ref.shape[1]]
    for k, ref in enumerate((bias_ref, log_ref, skip_ref)):
        ref[...] = sums_ref[k : k + 1, 0 : ref.shape[1]]
    for read, write in zip(reads, writes):
        read.wait()
        write.start()
    for write in writes:
        write.wait()


def finish(tile, sums, grad_dt, arrays, small_shapes):
    vmem = pl.BlockSpec(memory_space=pltpu.VMEM)
    anywhere = pl.BlockSpec(memory_space=pl.ANY)
    return pl.pallas_call(
        finish_kernel,
        out_shape=[jax.ShapeDtypeStruct(a.shape, a.dtype) for a in arrays]
        + [jax.ShapeDtypeStruct(shape, f32) for shape in small_shapes],
        in_specs=[vmem] * 3 + [anywhere] * 4,
        out_specs=[anywhere] * 4 + [vmem] * 8,
        scratch_shapes=[pltpu.VMEM(a.shape, a.dtype) for a in arrays] + [pltpu.SemaphoreType.DMA((2, 4))],
        name="finish",
    )(tile, sums, grad_dt, *arrays)


def pre_norm_inverse(rows):
    return lax.rsqrt(jnp.mean(rows * rows, axis=1, keepdims=True) + epsilon)


AXES = ("dp", "fsdp")


def gather_rows(shard):
    return lax.all_gather(shard, AXES, axis=0, tiled=True)


def scatter_rows(whole):
    return lax.psum_scatter(whole, AXES, scatter_dimension=0, tiled=True)


def vector_tile(conv_weight, conv_bias, gate_gain, norm_gain):
    rows = [conv_weight, conv_bias[None], gate_gain[None], norm_gain[None]]
    rows = [jnp.pad(row.astype(f32), ((0, 0), (0, KEY - row.shape[1]))) for row in rows]
    return jnp.concatenate(rows + [jnp.zeros((1, KEY), f32)], axis=0)


def vector_tiles(conv, gate, pre, parts):
    rows = []
    for whole in (conv, gate, pre):
        part = whole.shape[1] // parts
        split_up = jnp.transpose(whole.reshape(-1, parts, part), (1, 0, 2))
        rows.append(jnp.pad(split_up, ((0, 0), (0, 0), (0, KEY - part))))
    return jnp.concatenate(rows + [jnp.zeros((parts, 1, KEY), f32)], axis=1)


def shards(
    kernels, hidden, cotangent, lengths, norm_gain, in_proj, dt_proj, conv_weight, conv_bias,
    dt_bias, a_log, skip_gain, gate_gain, out_proj,
):
    length, width = hidden.shape
    assert lengths.shape[0] == 1
    rows_in, columns = in_proj.shape
    heads = dt_bias.shape[0]
    parts = width // rows_in
    taps, conv_part = conv_weight.shape
    gate_part = gate_gain.shape[0]
    wide = gate_part * parts
    total = columns + 2 * KEY

    if kernels:
        rows = lambda *vectors: [v.reshape(1, -1) for v in vectors]
        (
            w_in, projected, mixed, states, gated_flipped, grad_gated, output, flipped, live, ph, pv, gains, inverse_two,
            pull, *shared,
        ) = gather_forward(
            lengths, hidden, cotangent, in_proj, dt_proj, out_proj, conv_weight,
            *rows(conv_bias, gate_gain, norm_gain, dt_bias, a_log, skip_gain),
        )
        input_grad, grad_in, grad_dt, grad_out, small_sum, head_sums = backward_scatter(
            hidden, cotangent, live, flipped, gated_flipped, pv, gains, ph,
            inverse_two, pull, shared, projected, mixed, grad_gated, states, w_in, rows_in,
        )
        output, input_grad, grad_in, grad_out, *small = finish(
            small_sum, head_sums, grad_dt, (output, input_grad, grad_in, grad_out),
            ((1, rows_in), (rows_in, heads), (taps, conv_part), (1, conv_part))
            + ((1, heads),) * 3 + ((1, gate_part),),
        )
        pre, dt, conv, shift, bias, log, skip, gate = small
        return (
            output, input_grad, pre[0], grad_in, dt, conv, shift[0], bias[0], log[0], skip[0], gate[0], grad_out
        )

    fill = jnp.zeros((rows_in, total - columns - heads), bf16)
    packed = jnp.concatenate([in_proj, dt_proj, fill], axis=1)
    tile = vector_tile(conv_weight, conv_bias, gate_gain, norm_gain)
    ph = jnp.pad(jnp.stack([dt_bias, a_log]).astype(f32), ((0, 6), (0, KEY - heads)))
    skip_wide = jnp.repeat(skip_gain.astype(f32), HD)[None]
    live = (jnp.arange(length) < lengths[0]).astype(f32)[:, None]
    rows_wide = hidden.astype(f32)
    cot_wide = cotangent.astype(f32)
    upstream = (cot_wide * live).astype(bf16)
    inverse_one = pre_norm_inverse(rows_wide)
    w_in, w_out = gather_rows(packed), gather_rows(out_proj)
    tiles = gather_rows(tile[None])
    whole = lambda rows, part: jnp.transpose(tiles[:, rows, :part], (1, 0, 2)).reshape(-1, parts * part)
    conv_all = whole(slice(0, 5), conv_part)
    gain_two = whole(slice(5, 6), gate_part)
    gain_one = whole(slice(6, 7), rows_in)[0]
    rest = jnp.concatenate([gain_two, skip_wide, jnp.zeros((1, wide), f32)], axis=0)
    pv = jnp.concatenate([conv_all, jnp.pad(rest, ((0, 0), (0, 2 * KEY)))], axis=0)
    normed = (rows_wide * inverse_one * gain_one[None, :]).astype(bf16)
    projected = mm(normed, w_in)
    mixed, product, states, inverse_two, *shared = mixer_forward(projected, pv, ph)
    inv = inverse_two[:, :1]
    gated = (product * inv * gain_two).astype(bf16)
    output = (rows_wide + live * mm(gated, w_out)).astype(bf16)
    grad_gated = mm_nt(upstream, w_out)
    pull = jnp.sum(grad_gated * gain_two * product, axis=1, keepdims=True)
    pull = jnp.broadcast_to(inv * inv * inv * pull / wide, inverse_two.shape)
    grad_out = mm_tn(gated, upstream)
    grad_proj, sums_v, sums_k, sums_h = mixer_backward(
        projected, pv, ph, mixed, grad_gated, states, inverse_two, pull, shared
    )
    skip_grad = jnp.pad(jnp.sum(sums_v[6].reshape(heads, HD), axis=1), (0, KEY - heads))[None]
    head_grads = jnp.concatenate([sums_h[:2], skip_grad, jnp.zeros((5, KEY), f32)], axis=0)

    grad_normed = mm_nt(grad_proj, w_in)
    scaled = grad_normed * gain_one[None, :]
    row_sums = jnp.sum(scaled * rows_wide, axis=1, keepdims=True) / width
    grad_rows = inverse_one * scaled - rows_wide * (inverse_one * inverse_one * inverse_one * row_sums)
    input_grad = cot_wide + grad_rows
    grad_gain_one = jnp.sum(grad_normed * rows_wide * inverse_one, axis=0, keepdims=True)

    conv_grad = jnp.concatenate([sums_v[:5], sums_k[:5]], axis=1)
    small = vector_tiles(conv_grad, sums_v[5:6], grad_gain_one, parts)
    grad_out = scatter_rows(grad_out.astype(bf16)).astype(f32)
    head_sums = lax.psum(head_grads, AXES)
    grad_all = scatter_rows(mm_tn(normed, grad_proj).astype(bf16)).astype(f32)
    grad_in, grad_dt = grad_all[:, :columns], grad_all[:, columns:]
    small_sum = scatter_rows(small)[0]
    return (
        output,
        input_grad,
        small_sum[6, :rows_in],
        grad_in,
        grad_dt[:, :heads],
        small_sum[:taps, :conv_part],
        small_sum[taps, :conv_part],
        head_sums[0, :heads],
        head_sums[1, :heads],
        head_sums[2, :heads],
        small_sum[5, :gate_part],
        grad_out,
    )


def solution(mesh):
    rows = P(AXES, None)
    vector = P(AXES)
    last = P(None, AXES)
    return jax.shard_map(
        partial(shards, mesh.shape["dp"] == 8 and mesh.shape["fsdp"] == 4),
        mesh=mesh,
        in_specs=(rows, rows, vector, vector, rows, rows, last, vector, P(), P(), P(), vector, rows),
        out_specs=(rows, rows, vector, rows, rows, last, vector, P(), P(), P(), vector, rows),
        check_vma=False,
    )
```

```python
from functools import partial

import jax
import jax.numpy as jnp
from jax import lax
from jax.experimental import pallas as pl
from jax.experimental.pallas import tpu as pltpu
from jax.sharding import PartitionSpec as P

f32 = jnp.float32
bf16 = jnp.bfloat16
epsilon = 1e-05
highest = lax.Precision.HIGHEST
BLK = 128
GH = 4
HD = 64
GC = GH * HD
KEY = 128
NEG = -1e30


def sigmoid(v):
    return 0.5 * jnp.tanh(0.5 * v) + 0.5


def mm(a, b):
    return lax.dot_general(a, b, (((1,), (0,)), ((), ())), preferred_element_type=f32)


def mm_nt(a, b):
    return lax.dot_general(a, b, (((1,), (1,)), ((), ())), preferred_element_type=f32)


def mm_tn(a, b):
    return lax.dot_general(a, b, (((0,), (0,)), ((), ())), preferred_element_type=f32)


def mm_hi(a, b, dims=((1,), (0,))):
    return lax.dot_general(a, b, (dims, ((), ())), preferred_element_type=f32, precision=highest)


def split(v):
    hi = v.astype(bf16)
    lo = (v - hi.astype(f32)).astype(bf16)
    return jnp.concatenate([hi, lo], axis=1)


def iota(shape, dim):
    return lax.broadcasted_iota(jnp.int32, shape, dim)


def expander(g):
    rows = iota((2 * KEY, GC), 0)
    cols = iota((2 * KEY, GC), 1)
    return jnp.where(lax.rem(rows, KEY) == cols // HD + g * GH, 1.0, 0.0).astype(bf16)


def reducer(g):
    rows = iota((GC, KEY), 0)
    cols = iota((GC, KEY), 1)
    return jnp.where(rows // HD + g * GH == cols, 1.0, 0.0).astype(bf16)


def taps_of(window, par):
    out = par[4:5] + par[3:4] * window[8:136]
    for k in range(3):
        out = out + par[k : k + 1] * window[5 + k : 133 + k]
    return out


def group_rows(st_ref, g, half, rows):
    tile = st_ref[pl.ds(pl.multiple_of(g // 2 * 8, 8), 8), rows]
    return jnp.where(half == 0, tile[:GH], tile[GH:])


def forward_shared(
    rawk_ref, dtr_ref, pv_ref, key_at, ph_ref, s_ref, st_ref, hl_ref, ehl_ref, kb_ref, kt_ref, sc_ref, padk
):
    blocks = rawk_ref.shape[0] // BLK
    dt = jax.nn.softplus(dtr_ref[...] + ph_ref[0:1, :])
    la = -dt * jnp.exp(ph_ref[1:2, :])
    tri = jnp.where(iota((BLK, BLK), 0) >= iota((BLK, BLK), 1), 1.0, 0.0).astype(f32)
    hl_ref[0] = split(dt)
    ehl_ref[...] = jnp.zeros_like(ehl_ref)
    padk[0:8] = jnp.zeros((8, 2 * KEY), f32)
    padk[8:] = rawk_ref[...]
    par = pv_ref[:, key_at : key_at + 2 * KEY]
    for k in range(blocks):
        rows = slice(k * BLK, (k + 1) * BLK)
        s = mm_hi(tri, la[rows])
        s_ref[rows] = s
        st_ref[:, rows] = s.T
        hl_ref[1, rows] = split(jnp.exp(s))
        hl_ref[2, rows] = split(jnp.exp(s[BLK - 1 :] - s))
        ehl_ref[k : k + 1] = split(jnp.exp(s[BLK - 1 :]))
        u = taps_of(padk[k * BLK : k * BLK + BLK + 8], par)
        v = u * sigmoid(u)
        kb_ref[rows] = v.astype(bf16)
        kt_ref[:, rows] = v.T.astype(bf16)
        sc_ref[k] = mm_hi(v[:, KEY:], v[:, :KEY], ((1,), (1,)))


def forward_group(
    g, gate_ref, rawv_ref, pv_ref, s_ref, st_ref, hl_ref, ehl_ref, kb_ref, kt_ref, sc_ref,
    y_ref, p_ref, hst_ref, pad, sg, hcar, ssq,
):
    blocks = gate_ref.shape[0] // BLK
    pad[8:] = rawv_ref[...]
    sg[...] = pltpu.roll(s_ref[...], lax.rem(KEY - g * GH, KEY), 1)
    ex = expander(g)
    bias = jnp.where(iota((BLK, BLK), 0) >= iota((BLK, BLK), 1), 0.0, NEG).astype(f32)
    low = iota((BLK, KEY), 1) < HD
    eend = mm(ehl_ref[...], ex)
    parg = pv_ref[:, pl.ds(pl.multiple_of(g * GC, GC), GC)]
    half = lax.rem(g, 8 // GH)
    hcar[...] = jnp.zeros_like(hcar)
    for k in range(blocks):
        rows = slice(k * BLK, (k + 1) * BLK)
        dtx = mm(hl_ref[0, rows], ex)
        exx = mm(hl_ref[1, rows], ex)
        txx = mm(hl_ref[2, rows], ex)
        hb = hcar[...].astype(bf16)
        hst_ref[k] = hb
        outer = mm(kb_ref[rows, KEY:], hb)
        across = group_rows(st_ref, g, half, rows)
        xts = []
        for q in range(GC // KEY):
            cols = slice(q * KEY, (q + 1) * KEY)
            par = parg[:, cols]
            u = taps_of(pad[k * BLK : k * BLK + BLK + 8, cols], par)
            v = u * sigmoid(u)
            x = v * dtx[:, cols]
            xts.append((x * txx[:, cols]).astype(bf16))
            xb = x.astype(bf16)
            zero = jnp.zeros_like(xb)
            x2 = jnp.concatenate([jnp.where(low, xb, zero), jnp.where(low, zero, xb)], axis=0)
            ms = []
            for side in range(2):
                j = 2 * q + side
                spread = sg[rows, j : j + 1] - across[j : j + 1]
                ms.append((jnp.exp(spread + bias) * sc_ref[k]).astype(bf16))
            y = mm(jnp.concatenate(ms, axis=1), x2)
            y = y + outer[:, cols] * exx[:, cols] + par[6:7] * v
            y_ref[rows, cols] = y
            gate = gate_ref[rows, cols]
            p = y * (gate * sigmoid(gate))
            p_ref[rows, pl.ds(pl.multiple_of(g * GC + q * KEY, KEY), KEY)] = p
            ssq[rows] += p * p
        if k + 1 < blocks:
            hcar[...] = eend[k : k + 1] * hcar[...] + mm(kt_ref[:KEY, rows], jnp.concatenate(xts, axis=1))


def fwd_kernel(
    gate_ref, rawv_ref, rawk_ref, dtr_ref, pv_ref, ph_ref,
    y_ref, p_ref, hst_ref, r_ref, s_ref, st_ref, hl_ref, ehl_ref, kb_ref, kt_ref, sc_ref,
    pad, padk, sg, hcar, ssq,
):
    g = pl.program_id(0)
    wide = p_ref.shape[1]
    shared = (s_ref, st_ref, hl_ref, ehl_ref, kb_ref, kt_ref, sc_ref)

    @pl.when(g == 0)
    def _():
        forward_shared(rawk_ref, dtr_ref, pv_ref, wide, ph_ref, *shared, padk)
        pad[0:8] = jnp.zeros((8, GC), f32)
        ssq[...] = jnp.zeros_like(ssq)

    forward_group(g, gate_ref, rawv_ref, pv_ref, *shared, y_ref, p_ref, hst_ref, pad, sg, hcar, ssq)

    @pl.when(g == pl.num_programs(0) - 1)
    def _():
        mean = jnp.sum(ssq[...], axis=1, keepdims=True) / wide
        r_ref[...] = jnp.broadcast_to(lax.rsqrt(mean + epsilon), r_ref.shape)


def backward_start(length, pad, dpad, dsc, dkb, dsrow, dscol, ddt):
    pad[0:8] = jnp.zeros((8, GC), f32)
    dpad[length:] = jnp.zeros((8, GC), f32)
    for ref in (dsc, dkb, dsrow, dscol, ddt):
        ref[...] = jnp.zeros_like(ref)


def backward_group(
    g, gate_ref, rawv_ref, y_ref, gg_ref, hst_ref, r_ref, c_ref, pv_ref, shared,
    dgate_ref, draw_ref, sv_ref, pad, dpad, sg, dhcar, dsc, dkb, dsrow, dscol, ddt,
):
    s_ref, st_ref, hl_ref, ehl_ref, kb_ref, kt_ref, sc_ref = shared
    blocks = gate_ref.shape[0] // BLK
    pad[8:] = rawv_ref[...]
    sg[...] = pltpu.roll(s_ref[...], lax.rem(KEY - g * GH, KEY), 1)
    ex = expander(g)
    red = reducer(g)
    row = iota((BLK, BLK), 0)
    col = iota((BLK, BLK), 1)
    bias = jnp.where(row >= col, 0.0, NEG).astype(f32)
    strict = row > col
    low = iota((BLK, KEY), 1) < HD
    eend = mm(ehl_ref[...], ex)
    parg = pv_ref[:, pl.ds(pl.multiple_of(g * GC, GC), GC)]
    half = lax.rem(g, 8 // GH)
    tile_at = pl.ds(pl.multiple_of(g // 2 * 8, 8), 8)
    mine = (iota((8, BLK), 0) < GH) == (half == 0)
    dhcar[...] = jnp.zeros_like(dhcar)
    sv_ref[...] = jnp.zeros_like(sv_ref)
    for k in range(blocks - 1, -1, -1):
        rows = slice(k * BLK, (k + 1) * BLK)
        dtx = mm(hl_ref[0, rows], ex)
        exx = mm(hl_ref[1, rows], ex)
        txx = mm(hl_ref[2, rows], ex)
        hb = hst_ref[k]
        dhb = dhcar[...].astype(bf16)
        ch = mm(kb_ref[rows, KEY:], hb)
        qq = mm(kb_ref[rows, :KEY], dhb)
        across = group_rows(st_ref, g, half, rows)
        dyes, xts, zs, oys, ddts, ecols = [], [], [], [], [], []
        dsrow_k = jnp.zeros((BLK, KEY), f32)
        for q in range(GC // KEY):
            cols = slice(q * KEY, (q + 1) * KEY)
            par = parg[:, cols]
            window = pad[k * BLK : k * BLK + BLK + 8, cols]
            u = taps_of(window, par)
            su = sigmoid(u)
            v = u * su
            x = v * dtx[:, cols]
            xb = x.astype(bf16)
            gate = gate_ref[rows, cols]
            y = y_ref[rows, cols]
            sgt = sigmoid(gate)
            silu_g = gate * sgt
            p = y * silu_g
            dgn = gg_ref[rows, cols] * r_ref[rows]
            sv_ref[5:6, cols] += jnp.sum(dgn * p, axis=0, keepdims=True)
            dp = dgn * par[5:6] - p * c_ref[rows]
            dgate_ref[rows, cols] = (dp * y * (sgt + silu_g * (1.0 - sgt))).astype(bf16)
            dy = dp * silu_g
            sv_ref[6:7, cols] += jnp.sum(dy * v, axis=0, keepdims=True)
            dyb = dy.astype(bf16)
            dye = dy * exx[:, cols]
            dyes.append(dye.astype(bf16))
            oys.append((dye * ch[:, cols]).astype(bf16))
            xt = x * txx[:, cols]
            xts.append(xt.astype(bf16))
            zs.append((xt * qq[:, cols]).astype(bf16))
            zero = jnp.zeros_like(dyb)
            dy2 = jnp.concatenate([jnp.where(low, dyb, zero), jnp.where(low, zero, dyb)], axis=0)
            dm2 = mm_nt(dy2, xb)
            ms, scored = [], []
            for side in range(2):
                j = 2 * q + side
                spread = sg[rows, j : j + 1] - across[j : j + 1]
                decay = jnp.exp(spread + bias)
                m = decay * sc_ref[k]
                ms.append(m.astype(bf16))
                dm = dm2[side * BLK : (side + 1) * BLK]
                part = decay * dm
                scored.append(part)
                e = jnp.where(strict, part * sc_ref[k], 0.0)
                dsrow_k = jnp.where(col == g * GH + j, jnp.sum(e, axis=1, keepdims=True), dsrow_k)
                ecols.append(jnp.sum(e, axis=0, keepdims=True))
            dsc[k] += scored[0] + scored[1]
            dx = mm_tn(jnp.concatenate(ms, axis=0), dy2) + qq[:, cols] * txx[:, cols]
            dv = dx * dtx[:, cols] + par[6:7] * dy
            ddts.append((dx * v).astype(bf16))
            du = dv * (su + v * (1.0 - su))
            dpad[rows, cols] = du
            sv_ref[4:5, cols] += jnp.sum(du, axis=0, keepdims=True)
            for t in range(4):
                sv_ref[t : t + 1, cols] += jnp.sum(du * window[5 + t : 133 + t], axis=0, keepdims=True)
        dscol[tile_at, rows] += jnp.where(mine, jnp.concatenate(ecols + ecols, axis=0), 0.0)
        dye = jnp.concatenate(dyes, axis=1)
        xt = jnp.concatenate(xts, axis=1)
        zsum = mm(jnp.concatenate(zs, axis=1), red)
        ddt[rows] += mm(jnp.concatenate(ddts, axis=1), red)
        hterm = eend[k : k + 1] * jnp.sum(dhcar[...] * hb.astype(f32), axis=0, keepdims=True)
        end = jnp.sum(zsum, axis=0, keepdims=True) + mm_hi(hterm, red.astype(f32))
        add = dsrow_k + mm(jnp.concatenate(oys, axis=1), red) - zsum
        dsrow[rows] += add + jnp.where(row == BLK - 1, end, 0.0)
        dkb[rows, KEY:] += mm_nt(dye, hb)
        dkb[rows, :KEY] += mm_nt(xt, dhb)
        if k:
            dhcar[...] = eend[k : k + 1] * dhcar[...] + mm(kt_ref[KEY:, rows], dye)

    for k in range(blocks):
        rows = slice(k * BLK, (k + 1) * BLK)
        for q in range(GC // KEY):
            cols = slice(q * KEY, (q + 1) * KEY)
            par = parg[:, cols]
            window = dpad[k * BLK : k * BLK + BLK + 8, cols]
            out = par[3:4] * window[0:BLK]
            for t in range(3):
                out = out + par[t : t + 1] * window[3 - t : 3 - t + BLK]
            draw_ref[rows, cols] = out.astype(bf16)


def backward_shared(
    rawk_ref, dtr_ref, pv_ref, key_at, ph_ref, kb_ref, dkeys_ref, ddt_ref, sk_ref, sh_ref,
    padk, dpadk, dsc, dkb, dsrow, dscol, ddt,
):
    length = rawk_ref.shape[0]
    blocks = length // BLK
    row = iota((BLK, BLK), 0)
    col = iota((BLK, BLK), 1)
    padk[0:8] = jnp.zeros((8, 2 * KEY), f32)
    padk[8:] = rawk_ref[...]
    dpadk[length:] = jnp.zeros((8, 2 * KEY), f32)
    sk_ref[...] = jnp.zeros_like(sk_ref)
    sh_ref[...] = jnp.zeros_like(sh_ref)
    upper = jnp.where(row <= col, 1.0, 0.0).astype(f32)
    par = pv_ref[:, key_at : key_at + 2 * KEY]
    for k in range(blocks):
        rows = slice(k * BLK, (k + 1) * BLK)
        window = padk[k * BLK : k * BLK + BLK + 8]
        u = taps_of(window, par)
        su = sigmoid(u)
        ds = dsc[k].astype(bf16)
        db = dkb[rows, :KEY] + mm_tn(ds, kb_ref[rows, KEY:])
        dc = dkb[rows, KEY:] + mm(ds, kb_ref[rows, :KEY])
        du = jnp.concatenate([db, dc], axis=1) * (su + u * su * (1.0 - su))
        dpadk[rows] = du
        sk_ref[4:5] += jnp.sum(du, axis=0, keepdims=True)
        for t in range(4):
            sk_ref[t : t + 1] += jnp.sum(du * window[5 + t : 133 + t], axis=0, keepdims=True)
        dla = mm_hi(upper, dsrow[rows] - dscol[:, rows].T)
        z = dtr_ref[rows] + ph_ref[0:1, :]
        rate = jnp.exp(ph_ref[1:2, :])
        dt = jax.nn.softplus(z)
        sh_ref[1:2] += jnp.sum(dla * (-dt * rate), axis=0, keepdims=True)
        dz = (ddt[rows] - dla * rate) * sigmoid(z)
        sh_ref[0:1] += jnp.sum(dz, axis=0, keepdims=True)
        ddt_ref[rows] = dz.astype(bf16)
    for k in range(blocks):
        rows = slice(k * BLK, (k + 1) * BLK)
        window = dpadk[k * BLK : k * BLK + BLK + 8]
        out = par[3:4] * window[0:BLK]
        for t in range(3):
            out = out + par[t : t + 1] * window[3 - t : 3 - t + BLK]
        dkeys_ref[rows] = out.astype(bf16)


def bwd_kernel(
    gate_ref, rawv_ref, rawk_ref, dtr_ref, pv_ref, ph_ref,
    y_ref, gg_ref, hst_ref, r_ref, c_ref, s_ref, st_ref, hl_ref, ehl_ref, kb_ref, kt_ref, sc_ref,
    dproj_ref, sv_ref, sk_ref, sh_ref,
    pad, padk, dpad, dpadk, sg, dhcar, dsc, dkb, dsrow, dscol, ddt,
):
    g = pl.program_id(0)
    length, total = dproj_ref.shape
    wide = GC * pl.num_programs(0)
    shared = (s_ref, st_ref, hl_ref, ehl_ref, kb_ref, kt_ref, sc_ref)

    @pl.when(g == 0)
    def _():
        backward_start(length, pad, dpad, dsc, dkb, dsrow, dscol, ddt)

    gate_at = pl.ds(pl.multiple_of(g * GC, GC), GC)
    draw_at = pl.ds(pl.multiple_of(wide + g * GC, GC), GC)
    backward_group(
        g, gate_ref, rawv_ref, y_ref, gg_ref, hst_ref, r_ref, c_ref, pv_ref, shared,
        dproj_ref.at[:, gate_at], dproj_ref.at[:, draw_at], sv_ref,
        pad, dpad, sg, dhcar, dsc, dkb, dsrow, dscol, ddt,
    )

    @pl.when(g == pl.num_programs(0) - 1)
    def _():
        keys = 2 * wide
        dproj_ref[:, keys + 3 * KEY :] = jnp.zeros((length, total - keys - 3 * KEY), bf16)
        backward_shared(
            rawk_ref, dtr_ref, pv_ref, wide, ph_ref, kb_ref,
            dproj_ref.at[:, keys : keys + 2 * KEY], dproj_ref.at[:, keys + 2 * KEY : keys + 3 * KEY],
            sk_ref, sh_ref, padk, dpadk, dsc, dkb, dsrow, dscol, ddt,
        )


def whole_spec(shape):
    return pl.BlockSpec(shape, lambda g: (0,) * len(shape))


def state_specs(length):
    return (
        ((length, KEY), f32),
        ((KEY, length), f32),
        ((3, length, 2 * KEY), bf16),
        ((8, 2 * KEY), bf16),
        ((length, 2 * KEY), bf16),
        ((2 * KEY, length), bf16),
        ((length // BLK, BLK, BLK), f32),
    )


def proj_specs(length, groups):
    wide = groups * GC
    return [
        pl.BlockSpec((length, GC), lambda g: (0, g)),
        pl.BlockSpec((length, GC), lambda g: (0, groups + g)),
        pl.BlockSpec((length, 2 * KEY), lambda g: (0, 2 * wide // (2 * KEY))),
        pl.BlockSpec((length, KEY), lambda g: (0, 2 * wide // KEY + 2)),
        whole_spec((8, wide + 2 * KEY)),
        whole_spec((8, KEY)),
    ]


def mixer_forward(projected, pv, ph):
    length = projected.shape[0]
    wide = pv.shape[1] - 2 * KEY
    groups = wide // GC
    blocks = length // BLK
    column = pl.BlockSpec((length, GC), lambda g: (0, g))
    shared = state_specs(length)
    return pl.pallas_call(
        fwd_kernel,
        grid=(groups,),
        in_specs=proj_specs(length, groups),
        out_specs=[
            column,
            whole_spec((length, wide)),
            pl.BlockSpec((blocks, KEY, GC), lambda g: (0, 0, g)),
            whole_spec((length, KEY)),
        ]
        + [whole_spec(shape) for shape, _ in shared],
        out_shape=[
            jax.ShapeDtypeStruct((length, wide), f32),
            jax.ShapeDtypeStruct((length, wide), f32),
            jax.ShapeDtypeStruct((blocks, KEY, wide), bf16),
            jax.ShapeDtypeStruct((length, KEY), f32),
        ]
        + [jax.ShapeDtypeStruct(shape, dtype) for shape, dtype in shared],
        scratch_shapes=[
            pltpu.VMEM((length + 8, GC), f32),
            pltpu.VMEM((length + 8, 2 * KEY), f32),
            pltpu.VMEM((length, KEY), f32),
            pltpu.VMEM((KEY, GC), f32),
            pltpu.VMEM((length, KEY), f32),
        ],
        name="mixer_forward",
    )(projected, projected, projected, projected, pv, ph)


def backward_scratch(length):
    return [
        pltpu.VMEM((length + 8, GC), f32),
        pltpu.VMEM((length + 8, 2 * KEY), f32),
        pltpu.VMEM((length + 8, GC), f32),
        pltpu.VMEM((length + 8, 2 * KEY), f32),
        pltpu.VMEM((length, KEY), f32),
        pltpu.VMEM((KEY, GC), f32),
        pltpu.VMEM((length // BLK, BLK, BLK), f32),
        pltpu.VMEM((length, 2 * KEY), f32),
        pltpu.VMEM((length, KEY), f32),
        pltpu.VMEM((KEY, length), f32),
        pltpu.VMEM((length, KEY), f32),
    ]


def mixer_backward(projected, pv, ph, mixed, grad_gated, states, inverse, pull, shared):
    length, total = projected.shape
    wide = pv.shape[1] - 2 * KEY
    groups = wide // GC
    blocks = length // BLK
    column = pl.BlockSpec((length, GC), lambda g: (0, g))
    return pl.pallas_call(
        bwd_kernel,
        grid=(groups,),
        in_specs=proj_specs(length, groups)
        + [
            column,
            column,
            pl.BlockSpec((blocks, KEY, GC), lambda g: (0, 0, g)),
            whole_spec((length, KEY)),
            whole_spec((length, KEY)),
        ]
        + [whole_spec(shape) for shape, _ in state_specs(length)],
        out_specs=[
            whole_spec((length, total)),
            pl.BlockSpec((8, GC), lambda g: (0, g)),
            whole_spec((8, 2 * KEY)),
            whole_spec((8, KEY)),
        ],
        out_shape=[
            jax.ShapeDtypeStruct((length, total), bf16),
            jax.ShapeDtypeStruct((8, wide), f32),
            jax.ShapeDtypeStruct((8, 2 * KEY), f32),
            jax.ShapeDtypeStruct((8, KEY), f32),
        ],
        scratch_shapes=backward_scratch(length),
        name="mixer_backward",
    )(projected, projected, projected, projected, pv, ph, mixed, grad_gated, states, inverse, pull, *shared)


MESH = pl.DeviceIdType.MESH
HALF = 256


ORDERS = ("xylh", "yxlh", "lhxy")
GATHER_WAITS = (3, 6, 10, 14, 16)
SCATTER_WAITS = (2, 6, 10, 14, 18)


def places():
    d, f = lax.axis_index("dp"), lax.axis_index("fsdp")
    bits = {"x": d % 2, "y": f // 2, "l": d // 2 % 2, "h": d // 4, "c": f % 2}
    far = {"x": (1, 0), "y": (0, 2), "l": (2, 0), "h": (4, 0), "c": (0, 1)}
    hops = {k: tuple(w * (1 - 2 * bits[k]) if w else 0 for w in far[k]) for k in far}
    return d, f, bits, hops


def kind_of(u):
    r = lax.rem(u, 9)
    along_y = (r == 1) | (r == 3) | (r == 6) | ((r == 7) & (lax.rem(u // 9, 2) == 1))
    return jnp.where((r == 4) | (r == 8), 2, jnp.where(along_y, 1, 0))


def pick(kind, values):
    if isinstance(kind, int):
        return values[kind]
    if all(v is values[0] for v in values):
        return values[0]
    return jnp.where(kind == 0, values[0], jnp.where(kind == 1, values[1], values[2]))


def exchange(place, kind, stage):
    d, f, bits, hops = place
    axes = "ccc" if stage == 0 else [order[stage - 1] for order in ORDERS]
    side = pick(kind, [bits[a] for a in axes])
    return side, (d + pick(kind, [hops[a][0] for a in axes]), f + pick(kind, [hops[a][1] for a in axes]))


def strides(kind):
    return {a: pick(kind, [8 >> order.index(a) for order in ORDERS]) for a in "xylh"}


def position(kind, bits):
    step = strides(kind)
    return sum(bits[a] * step[a] for a in "xylh")


def all_positions(kind):
    step = strides(kind)
    out = []
    for i in range(32):
        bits = {"x": i // 4 % 2, "y": i // 2 % 2, "l": i // 8 % 2, "h": i // 16}
        out.append((i % 2, sum(step[a] for a in "xylh" if bits[a])))
    return out


def greet(partners):
    barrier = pltpu.get_barrier_semaphore()
    for partner in partners:
        pl.semaphore_signal(barrier, inc=1, device_id=partner, device_id_type=MESH)
    pl.semaphore_wait(barrier, len(partners))


def spread_lanes(tiles, width, lane, count):
    out = [jnp.zeros(tiles[0].shape, f32) for _ in range(count)]
    for i, tile in enumerate(tiles):
        at, shift = divmod(i * width, KEY)
        turned = pltpu.roll(tile, shift, 1) if shift else tile
        end = shift + width
        out[at] = out[at] + jnp.where((lane >= shift) & (lane < end), turned, 0.0)
        if end > KEY:
            out[at + 1] = out[at + 1] + jnp.where(lane < end - KEY, turned, 0.0)
    return out


def forward_kernel(
    n_in, n_out, lengths_ref, hidden_ref, cot_ref, w_ref, wd_ref, wo_ref, conv_ref, shift_ref, gate_ref, pre_ref,
    dt_ref, log_ref, skip_ref,
    w_out, proj_out, mixed_out, states_out, flipped_gated_out, gg_out,
    out_ref, flipped_ref, live_ref, ph_ref, pv_ref, gain, r_ref, c_ref, s_ref, st_ref, hl_ref, ehl_ref, kb_ref, kt_ref, sc_ref,
    held, tiles, w_stage, wo_stage, proj_stage, mixed_stage, states_stage, flip_stage, normed, gated, big,
    pad, padk, sg, hcar, ssq, dots,
    send, recv, tile_sem, out_sem, gg_sem,
):
    rb = w_ref.shape[0]
    length, width = hidden_ref.shape
    wide = big.shape[1]
    n = n_in + n_out
    place = places()
    greet([exchange(place, 0, stage)[1] for stage in range(5)])
    count = (1, 2, 4, 8, 16)

    def columns(i, half):
        group = (i - 1) * HALF + half * wide
        return pl.ds(pl.multiple_of(jnp.where(i == 0, 2 * wide + half * HALF, group), HALF), HALF)

    def own_at(kind):
        return place[2]["c"] * 16 + position(kind, place[2])

    def copy(stage, u):
        kind = kind_of(u)
        start = own_at(kind) // count[stage] * count[stage]
        block = held.at[u, pl.ds(start, count[stage])]
        return pltpu.make_async_remote_copy(
            src_ref=block,
            dst_ref=block,
            send_sem=send.at[u, stage],
            recv_sem=recv.at[u, stage],
            device_id=exchange(place, kind, 4 - stage)[1],
            device_id_type=MESH,
        )

    def tile_copy(stage):
        block = tiles.at[pl.ds(own_at(0) // count[stage] * count[stage], count[stage])]
        return pltpu.make_async_remote_copy(
            src_ref=block,
            dst_ref=block,
            send_sem=tile_sem.at[0, stage],
            recv_sem=tile_sem.at[1, stage],
            device_id=exchange(place, 0, 4 - stage)[1],
            device_id_type=MESH,
        )

    def weight_stores(i):
        slot = lax.rem(i, 2)
        copies = []
        for half in range(2):
            cols = slice(half * HALF, (half + 1) * HALF)
            copies.append(
                pltpu.make_async_copy(
                    w_stage.at[slot, :, cols], w_out.at[:, columns(i, half)], out_sem.at[half, slot]
                )
            )
            copies.append(
                pltpu.make_async_copy(
                    proj_stage.at[slot, :, cols], proj_out.at[:, columns(i, half)], out_sem.at[2 + half, slot]
                )
            )
        return copies

    def group_stores(i):
        slot = lax.rem(i, 2)
        cols = pl.ds(pl.multiple_of((i - 1) * HALF, HALF), HALF)
        return (
            pltpu.make_async_copy(mixed_stage.at[slot], mixed_out.at[:, cols], out_sem.at[4, slot]),
            pltpu.make_async_copy(states_stage.at[slot], states_out.at[:, :, cols], out_sem.at[5, slot]),
        )

    def flip_store(k):
        return pltpu.make_async_copy(
            flip_stage.at[k % 2], flipped_gated_out.at[k * HALF : (k + 1) * HALF], out_sem.at[6, k % 2]
        )

    tile = tiles.at[own_at(0)]
    tile[...] = jnp.zeros((8, KEY), f32)
    tile[0:4, 0 : conv_ref.shape[1]] = conv_ref[...].astype(f32)
    tile[4:5, 0 : shift_ref.shape[1]] = shift_ref[...].astype(f32)
    tile[5:6, 0 : gate_ref.shape[1]] = gate_ref[...].astype(f32)
    tile[6:7, 0 : pre_ref.shape[1]] = pre_ref[...].astype(f32)
    tile_copy(0).start()
    heads = dt_ref.shape[1]
    ph_ref[...] = jnp.zeros_like(ph_ref)
    ph_ref[0:1, 0:heads] = dt_ref[...].astype(f32)
    ph_ref[1:2, 0:heads] = log_ref[...].astype(f32)
    ph_ref[2:3, 0:heads] = skip_ref[...].astype(f32)
    live_ref[...] = jnp.where(iota((length, KEY), 0) < lengths_ref[0], 1.0, 0.0).astype(f32)

    held[0, own_at(kind_of(0))] = w_ref[:, 2 * wide : 2 * wide + HALF]
    held[1, own_at(kind_of(1))] = jnp.zeros((rb, HALF), bf16)
    held[1, own_at(kind_of(1)), :, 0:heads] = wd_ref[...]

    def land(u, carry):
        group = pl.ds(pl.multiple_of((u // 2 - 1) * HALF + lax.rem(u, 2) * wide, HALF), HALF)
        held[u, own_at(kind_of(u))] = w_ref[:, group]
        return carry

    lax.fori_loop(2, 2 * n_in, land, 0)
    for u in range(2 * n_out):
        rows = slice(u % 2 * rb, (u % 2 + 1) * rb)
        held[2 * n_in + u, own_at(kind_of(2 * n_in + u))] = wo_ref[rows, u // 2 * HALF : (u // 2 + 1) * HALF]

    def first_chunk():
        lane = iota((8, KEY), 1)
        row = iota((8, KEY), 0)
        order = [tiles[c * 16 + at] for c, at in all_positions(0)]
        conv = spread_lanes(order, (wide + 2 * KEY) // 32, lane, wide // KEY + 2)
        gate = spread_lanes(order, wide // 32, lane, wide // KEY)
        pre = spread_lanes(order, width // 32, lane, width // KEY)
        skips = split(jnp.broadcast_to(ph_ref[2:3], (8, KEY)))
        for k, tile in enumerate(conv):
            cols = slice(k * KEY, (k + 1) * KEY)
            if k < wide // KEY:
                if k % 2 == 0:
                    skip = mm(skips, expander(k // 2))
                skip_part = skip[:, k % 2 * KEY : (k % 2 + 1) * KEY]
                tile = jnp.where(row == 5, gate[k], jnp.where(row == 6, skip_part, tile))
            pv_ref[:, cols] = tile
        for k, tile in enumerate(pre):
            gain[:, k * KEY : (k + 1) * KEY] = tile
        for k in range(0, length, KEY):
            values = hidden_ref[k : k + KEY].astype(f32)
            mean = jnp.mean(values * values, axis=1, keepdims=True)
            rows = (values * lax.rsqrt(mean + epsilon) * gain[6:7]).astype(bf16)
            normed[k : k + KEY] = rows
            flipped_ref[:, k : k + KEY] = rows.T

    def keys_chunk(slot):
        forward_shared(
            proj_stage.at[slot, :, 0:HALF], proj_stage.at[slot, :, HALF : HALF + KEY], pv_ref, wide, ph_ref,
            s_ref, st_ref, hl_ref, ehl_ref, kb_ref, kt_ref, sc_ref, padk,
        )
        pad[0:8] = jnp.zeros((8, GC), f32)
        ssq[...] = jnp.zeros_like(ssq)
        dots[...] = jnp.zeros_like(dots)

    def project(slot):
        for half in range(2):
            cols = slice(half * HALF, (half + 1) * HALF)
            proj_stage[slot, :, cols] = mm(normed[...], w_stage[slot, :, cols])

    def group_chunk(slot, g):
        forward_group(
            g, proj_stage.at[slot, :, 0:HALF], proj_stage.at[slot, :, HALF : 2 * HALF], pv_ref,
            s_ref, st_ref, hl_ref, ehl_ref, kb_ref, kt_ref, sc_ref,
            mixed_stage.at[slot], big, states_stage.at[slot], pad, sg, hcar, ssq,
        )

    def finish_groups():
        mean = jnp.sum(ssq[...], axis=1, keepdims=True) / wide
        r_ref[...] = jnp.broadcast_to(lax.rsqrt(mean + epsilon), r_ref.shape)
        for k in range(wide // HALF):
            if k >= 2:
                flip_store(k - 2).wait()
            for q in range(HALF // KEY):
                cols = slice(k * HALF + q * KEY, k * HALF + (q + 1) * KEY)
                part = (big[:, cols] * r_ref[...] * pv_ref[5:6, cols]).astype(bf16)
                gated[:, cols] = part
                flip_stage[k % 2, q * KEY : (q + 1) * KEY] = part.T
            flip_store(k).start()
        for k in range(wide // HALF - 2, wide // HALF):
            flip_store(k).wait()

    def out_chunk_first(i):
        j = i - n_in
        side = pl.ds(pl.multiple_of(lax.rem(j, 2) * HALF, HALF), HALF)
        for half in range(2):
            for b, (c, at) in enumerate(all_positions(kind_of(2 * i + half))):
                wo_stage[(2 * b + half) * rb : (2 * b + half + 1) * rb, side] = held[2 * i + half, c * 16 + at]
        cols = pl.ds(pl.multiple_of(j * HALF, HALF), HALF)
        branch = mm(gated[...], wo_stage[:, side])
        live = jnp.concatenate([live_ref[...]] * (HALF // KEY), axis=1)
        out_ref[:, cols] = (hidden_ref[:, cols].astype(f32) + live * branch).astype(bf16)
        upstream = (cot_ref[:, cols].astype(f32) * live).astype(bf16)
        pull = upstream.astype(f32) * branch
        dots[...] += pull[:, :KEY] + pull[:, KEY:]

    def gg_store(q):
        cols = slice(q, q + 2 * HALF)
        return pltpu.make_async_copy(big.at[:, cols], gg_out.at[:, cols], gg_sem.at[q // (2 * HALF)])

    def out_chunk_second(i):
        j = i - n_in

        @pl.when(lax.rem(j, 2) == 1)
        def _():
            cols = pl.ds(pl.multiple_of((j - 1) * HALF, 2 * HALF), 2 * HALF)
            live = jnp.concatenate([live_ref[...]] * (2 * HALF // KEY), axis=1)
            upstream = (cot_ref[:, cols].astype(f32) * live).astype(bf16)
            for q in range(0, wide, 2 * HALF):
                more = mm_nt(upstream, wo_stage[q : q + 2 * HALF])

                @pl.when(j == 1)
                def _():
                    big[:, q : q + 2 * HALF] = more

                @pl.when(j > 1)
                def _():
                    big[:, q : q + 2 * HALF] += more

                @pl.when(j == n_out - 1)
                def _():
                    gg_store(q).start()

    def consume_first(i):
        slot = lax.rem(i, 2)

        @pl.when(i < n_in)
        def _():
            @pl.when(i >= 2)
            def _():
                for store in weight_stores(i - 2):
                    store.wait()

            for half in range(2):
                for b, (c, at) in enumerate(all_positions(kind_of(2 * i + half))):
                    w_stage[slot, b * rb : (b + 1) * rb, half * HALF : (half + 1) * HALF] = held[
                        2 * i + half, c * 16 + at
                    ]

            @pl.when(i == 0)
            def _():
                first_chunk()

            project(slot)
            for store in weight_stores(i):
                store.start()

        @pl.when(i >= n_in)
        def _():
            out_chunk_first(i)

    def consume_second(i):
        slot = lax.rem(i, 2)

        @pl.when(i == 0)
        def _():
            keys_chunk(slot)

        @pl.when((i > 0) & (i < n_in))
        def _():
            @pl.when(i >= 3)
            def _():
                for store in group_stores(i - 2):
                    store.wait()

            group_chunk(slot, i - 1)
            for store in group_stores(i):
                store.start()

        @pl.when(i == n_in - 1)
        def _():
            finish_groups()

        @pl.when(i >= n_in)
        def _():
            out_chunk_second(i)

    def tick(t, carry):
        @pl.when(t < 2 * n)
        def _():
            copy(0, t).start()

        for stage in range(5):
            u = t - GATHER_WAITS[stage]

            @pl.when(u == 0)
            def _(stage=stage):
                tile_copy(stage).wait()
                if stage < 4:
                    tile_copy(stage + 1).start()

            @pl.when((u >= 0) & (u < 2 * n))
            def _(stage=stage, u=u):
                copy(stage, u).wait()
                if stage < 4:
                    copy(stage + 1, u).start()

        u = t - GATHER_WAITS[4]

        @pl.when((u >= 1) & (lax.rem(u, 2) == 1))
        def _():
            consume_first(u // 2)

        @pl.when((u >= 2) & (lax.rem(u, 2) == 0))
        def _():
            consume_second(u // 2 - 1)

        return carry

    lax.fori_loop(0, 2 * n + GATHER_WAITS[4] + 1, tick, 0)
    pull = jnp.sum(dots[...], axis=1, keepdims=True) / wide
    c_ref[...] = r_ref[...] * r_ref[...] * pull
    for i in (n_in - 2, n_in - 1):
        for store in weight_stores(i) + list(group_stores(i)):
            store.wait()
    for q in range(0, wide, 2 * HALF):
        gg_store(q).wait()


def gather_forward(lengths, hidden, cotangent, shard, dt_shard, out_shard, *vectors):
    length, width = hidden.shape
    rb = shard.shape[0]
    columns = shard.shape[1] + 2 * KEY
    wide = out_shard.shape[0] * 32
    n_in, n_out = columns // (2 * HALF), width // HALF
    blocks = length // BLK
    vmem = pl.BlockSpec(memory_space=pltpu.VMEM)
    anywhere = pl.BlockSpec(memory_space=pl.ANY)
    struct = jax.ShapeDtypeStruct
    shared = [struct(shape, dtype) for shape, dtype in state_specs(length)]
    return pl.pallas_call(
        partial(forward_kernel, n_in, n_out),
        out_shape=[
            struct((width, columns), bf16),
            struct((length, columns), f32),
            struct((length, wide), f32),
            struct((blocks, KEY, wide), bf16),
            struct((wide, length), bf16),
            struct((length, wide), f32),
            struct((length, width), bf16),
            struct((width, length), bf16),
            struct((length, KEY), f32),
            struct((8, KEY), f32),
            struct((8, wide + 2 * KEY), f32),
            struct((8, width), f32),
            struct((length, KEY), f32),
            struct((length, KEY), f32),
        ]
        + shared,
        in_specs=[pl.BlockSpec(memory_space=pltpu.SMEM)] + [vmem] * (5 + len(vectors)),
        out_specs=[anywhere] * 6 + [vmem] * (8 + len(shared)),
        scratch_shapes=[
            pltpu.VMEM((2 * (n_in + n_out), 32, rb, HALF), bf16),
            pltpu.VMEM((32, 8, KEY), f32),
            pltpu.VMEM((2, width, 2 * HALF), bf16),
            pltpu.VMEM((wide, 2 * HALF), bf16),
            pltpu.VMEM((2, length, 2 * HALF), f32),
            pltpu.VMEM((2, length, HALF), f32),
            pltpu.VMEM((2, blocks, KEY, HALF), bf16),
            pltpu.VMEM((2, HALF, length), bf16),
            pltpu.VMEM((length, width), bf16),
            pltpu.VMEM((length, wide), bf16),
            pltpu.VMEM((length, wide), f32),
            pltpu.VMEM((length + 8, GC), f32),
            pltpu.VMEM((length + 8, 2 * KEY), f32),
            pltpu.VMEM((length, KEY), f32),
            pltpu.VMEM((KEY, GC), f32),
            pltpu.VMEM((length, KEY), f32),
            pltpu.VMEM((length, KEY), f32),
            pltpu.SemaphoreType.DMA((2 * (n_in + n_out), 5)),
            pltpu.SemaphoreType.DMA((2 * (n_in + n_out), 5)),
            pltpu.SemaphoreType.DMA((2, 5)),
            pltpu.SemaphoreType.DMA((7, 2)),
            pltpu.SemaphoreType.DMA((wide // (2 * HALF),)),
        ],
        compiler_params=pltpu.CompilerParams(
            collective_id=2, has_side_effects=True, vmem_limit_bytes=67043328
        ),
        name="gather_forward",
    )(lengths, hidden, cotangent, shard, dt_shard, out_shard, *vectors)


EARLY = 7


def gather_lanes(row_tiles, width, lane, i):
    at, shift = divmod(i * width, KEY)
    if shift == 0:
        return row_tiles[at]
    first = pltpu.roll(row_tiles[at], KEY - shift, 1)
    if shift + width <= KEY:
        return first
    return jnp.where(lane < KEY - shift, first, pltpu.roll(row_tiles[at + 1], KEY - shift, 1))


def backward_kernel(
    n_in, n_out, hidden_ref, cot_ref, live_ref, flipped_ref, gated_ref, pv_ref, gain_ref, ph_ref, r_ref, c_ref,
    s_ref, st_ref, hl_ref, ehl_ref, kb_ref, kt_ref, sc_ref,
    proj_in, mixed_in, gg_in, states_in, w_in,
    rows_out, in_ref, dt_ref, out_ref, tile_out, sums_ref,
    parts, r0, r1, r2, r3, r4, tiles, t0, t1, t2, t3, t4, sums, sums_in,
    stage_in, states_stage, w_stage, keys_stage, dchunk, rows_grad, sv, sv_all, sk, sh, skip_sum, gain_sum,
    pad, padk, dpad, dpadk, sg, dhcar, dsc, dkb, dsrow, dscol, ddt,
    send, recv, tile_sem, sums_sem, in_sem, out_sem,
):
    length, width = hidden_ref.shape
    wide = mixed_in.shape[1]
    rb = in_ref.shape[0]
    n = n_in + n_out
    groups = n_in - 1
    keys_tick = n - 2
    shared = (s_ref, st_ref, hl_ref, ehl_ref, kb_ref, kt_ref, sc_ref)
    place = places()
    held = (r0, r1, r2, r3, r4)
    tile_source = (tiles, t0, t1, t2, t3, t4)
    greet([exchange(place, 0, stage)[1] for stage in range(5)])

    def is_out(t):
        return ((t < 3 * n_out - 3) & (lax.rem(t, 3) == 0)) | (t == n - 1)

    def out_index(t):
        return jnp.where(t == n - 1, n_out - 1, t // 3)

    def group_index(t):
        return jnp.where(t < 3 * n_out - 3, t // 3 * 2 + lax.rem(t, 3) - 1, t - n_out + 1)

    def loads(g):
        slot = lax.rem(g, 2)
        near = pl.ds(pl.multiple_of(g * HALF, HALF), HALF)
        far = pl.ds(pl.multiple_of(wide + g * HALF, HALF), HALF)
        pairs = (
            (proj_in.at[:, near], stage_in.at[slot, 0]),
            (proj_in.at[:, far], stage_in.at[slot, 1]),
            (mixed_in.at[:, near], stage_in.at[slot, 2]),
            (gg_in.at[:, near], stage_in.at[slot, 3]),
            (states_in.at[:, :, near], states_stage.at[slot]),
        )
        return [pltpu.make_async_copy(a, b, in_sem.at[k, slot]) for k, (a, b) in enumerate(pairs)]

    def weight_loads(g):
        slot = lax.rem(g, 2)
        first = jnp.where(g == groups, 2 * wide, g * HALF)
        second = jnp.where(g == groups, 2 * wide + HALF, wide + g * HALF)
        return [
            pltpu.make_async_copy(
                w_in.at[:, pl.ds(pl.multiple_of(at, HALF), HALF)],
                w_stage.at[slot, :, half * HALF : (half + 1) * HALF],
                in_sem.at[5 + half, slot],
            )
            for half, at in enumerate((first, second))
        ]

    keys_load = pltpu.make_async_copy(proj_in.at[:, 2 * wide : 2 * wide + 3 * KEY], keys_stage, in_sem.at[7, 0])
    for load in loads(0) + weight_loads(0) + [keys_load]:
        load.start()
    rows_store = pltpu.make_async_copy(rows_grad, rows_out, out_sem.at[0])

    def sums_copy(stage):
        return pltpu.make_async_remote_copy(
            src_ref=sums.at[stage],
            dst_ref=sums_in.at[stage],
            send_sem=sums_sem.at[0, stage],
            recv_sem=sums_sem.at[1, stage],
            device_id=exchange(place, 0, stage)[1],
            device_id_type=MESH,
        )

    def tile_copy(stage):
        count = 16 >> stage
        return pltpu.make_async_remote_copy(
            src_ref=tile_source[stage].at[pl.ds((1 - exchange(place, 0, stage)[0]) * count, count)],
            dst_ref=tile_source[stage + 1],
            send_sem=tile_sem.at[0, stage],
            recv_sem=tile_sem.at[1, stage],
            device_id=exchange(place, 0, stage)[1],
            device_id_type=MESH,
        )

    def spot(stage, u):
        return lax.rem(u, 2 * EARLY) if stage == 0 else u

    def copy(stage, u):
        count = 16 >> stage
        side, partner = exchange(place, kind_of(u), stage)
        if stage == 0:
            src = parts.at[lax.rem(u // 2, 2), 1 - side, lax.rem(u, 2)]
        else:
            src = held[stage - 1].at[spot(stage - 1, u), pl.ds((1 - side) * count, count)]
        return pltpu.make_async_remote_copy(
            src_ref=src,
            dst_ref=held[stage].at[spot(stage, u)],
            send_sem=send.at[u, stage],
            recv_sem=recv.at[u, stage],
            device_id=partner,
            device_id_type=MESH,
        )

    backward_start(length, pad, dpad, dsc, dkb, dsrow, dscol, ddt)
    skip_sum[...] = jnp.zeros_like(skip_sum)
    rows_grad[...] = jnp.zeros_like(rows_grad)

    def out_chunk(slot, t):
        j = out_index(t)
        where = [all_positions(kind_of(2 * t + half)) for half in range(2)]
        cols = pl.ds(pl.multiple_of(j * HALF, HALF), HALF)
        live = jnp.concatenate([live_ref[...]] * (HALF // KEY), axis=1)
        upstream = (cot_ref[:, cols].astype(f32) * live).astype(bf16)
        for z in range(4):
            res = mm(gated_ref[z * 16 * rb : (z + 1) * 16 * rb], upstream)
            for b in range(8):
                for half in range(2):
                    c, at = where[half][z * 8 + b]
                    at_row = (2 * b + half) * rb
                    parts[slot, c, half, at] = res[at_row : at_row + rb].astype(bf16)

    def weight_chunk(slot, t, g):
        for load in weight_loads(g):
            load.wait()
        at = lax.rem(g, 2)
        for half in range(2):
            right = dchunk[:, half * HALF : (half + 1) * HALF]
            where = all_positions(kind_of(2 * t + half))
            for z in range(4):
                res = mm(flipped_ref[z * 8 * rb : (z + 1) * 8 * rb], right)
                for b in range(8):
                    c, to = where[z * 8 + b]
                    parts[slot, c, half, to] = res[b * rb : (b + 1) * rb].astype(bf16)
        for k in range(0, width, 512):
            rows_grad[:, k : k + 512] += mm_nt(dchunk[...], w_stage[at, k : k + 512])

    def group_chunk(t):
        g = group_index(t)

        for load in weight_loads(g + 1):
            load.start()

        @pl.when(g + 1 < groups)
        def _():
            for load in loads(g + 1):
                load.start()

        for load in loads(g):
            load.wait()
        at = lax.rem(g, 2)
        backward_group(
            g, stage_in.at[at, 0], stage_in.at[at, 1], stage_in.at[at, 2], stage_in.at[at, 3], states_stage.at[at],
            r_ref, c_ref, pv_ref, shared, dchunk.at[:, 0:HALF], dchunk.at[:, HALF : 2 * HALF], sv,
            pad, dpad, sg, dhcar, dsc, dkb, dsrow, dscol, ddt,
        )

    def group_chunk_end(slot, t):
        g = group_index(t)
        sv_all[:, pl.ds(pl.multiple_of(g * HALF, HALF), HALF)] = sv[...]
        skip_sum[...] += mm_hi(sv[...], reducer(g).astype(f32))
        weight_chunk(slot, t, g)

    def keys_chunk():
        keys_load.wait()
        dchunk[:, 3 * KEY :] = jnp.zeros((length, KEY), bf16)
        backward_shared(
            keys_stage.at[:, 0:HALF], keys_stage.at[:, HALF : HALF + KEY], pv_ref, wide, ph_ref, kb_ref,
            dchunk.at[:, 0:HALF], dchunk.at[:, HALF : HALF + KEY], sk, sh,
            padk, dpadk, dsc, dkb, dsrow, dscol, ddt,
        )

    def keys_chunk_end(slot):
        weight_chunk(slot, keys_tick, groups)
        for half in range(2):
            copy(0, 2 * keys_tick + half).start()
        gain = gain_ref[6:7]
        gain_sum[...] = jnp.zeros_like(gain_sum)
        for k in range(0, length, KEY):
            values = hidden_ref[k : k + KEY].astype(f32)
            inverse = lax.rsqrt(jnp.mean(values * values, axis=1, keepdims=True) + epsilon)
            grads = rows_grad[k : k + KEY]
            gain_sum[0:1] += jnp.sum(grads * values * inverse, axis=0, keepdims=True)
            scaled = grads * gain
            pull = jnp.sum(scaled * values, axis=1, keepdims=True) / width
            back = inverse * scaled - values * (inverse * inverse * inverse * pull)
            rows_grad[k : k + KEY] = cot_ref[k : k + KEY].astype(f32) + back
        rows_store.start()
        row = iota((8, KEY), 0)
        lane = iota((8, KEY), 1)
        conv = [sv_all[:, k * KEY : (k + 1) * KEY] for k in range(wide // KEY)]
        gate = conv
        conv = conv + [sk[:, 0:KEY], sk[:, KEY : 2 * KEY]]
        pre = [jnp.broadcast_to(gain_sum[0:1, k * KEY : (k + 1) * KEY], (8, KEY)) for k in range(width // KEY)]
        for i, (c, at) in enumerate(all_positions(0)):
            tile = gather_lanes(conv, (wide + 2 * KEY) // 32, lane, i)
            tile = jnp.where(row == 5, gather_lanes(gate, wide // 32, lane, i), tile)
            tiles[c * 16 + at] = jnp.where(row == 6, gather_lanes(pre, width // 32, lane, i), tile)
        tile_copy(0).start()
        sums[0] = jnp.where(row == 2, skip_sum[6:7], sh[...])
        sums_copy(0).start()

    def write_out(u, value):
        i, half = u // 2, lax.rem(u, 2)

        @pl.when(is_out(i))
        def _():
            cols = pl.ds(pl.multiple_of(out_index(i) * HALF, HALF), HALF)
            out_ref[pl.ds(pl.multiple_of(half * rb, 16), rb), cols] = value

        @pl.when(jnp.logical_not(is_out(i)) & (i != keys_tick))
        def _():
            cols = pl.ds(pl.multiple_of(half * wide + group_index(i) * HALF, HALF), HALF)
            in_ref[:, cols] = value

        @pl.when(u == 2 * keys_tick)
        def _():
            in_ref[:, 2 * wide : 2 * wide + HALF] = value

        @pl.when(u == 2 * keys_tick + 1)
        def _():
            dt_ref[...] = value[:, :KEY]

    def first_step(t):
        @pl.when(jnp.logical_not(is_out(t)) & (t != keys_tick))
        def _():
            group_chunk(t)

        @pl.when(t == keys_tick)
        def _():
            keys_chunk()

    def second_step(t):
        slot = lax.rem(t, 2)

        @pl.when(t >= 2)
        def _():
            for half in range(2):
                copy(0, 2 * (t - 2) + half).wait_send()

        @pl.when(is_out(t))
        def _():
            out_chunk(slot, t)

        @pl.when(jnp.logical_not(is_out(t)) & (t != keys_tick))
        def _():
            group_chunk_end(slot, t)

        @pl.when(t == keys_tick)
        def _():
            keys_chunk_end(slot)

        @pl.when(t != keys_tick)
        def _():
            for half in range(2):
                copy(0, 2 * t + half).start()

    def tick(step, carry):
        t = step // 2

        @pl.when((t < n) & (lax.rem(step, 2) == 0))
        def _():
            first_step(t)

        @pl.when((t < n) & (lax.rem(step, 2) == 1))
        def _():
            second_step(t)

        for stage in range(5):
            u = step - SCATTER_WAITS[stage]
            count = 16 >> stage

            @pl.when(u == 2 * keys_tick)
            def _(stage=stage, count=count):
                sums_copy(stage).wait()
                tile_copy(stage).wait()
                total = tile_source[stage + 1][...] + tile_source[stage][
                    pl.ds(exchange(place, 0, stage)[0] * count, count)
                ]
                if stage < 4:
                    sums[stage + 1] = sums[stage] + sums_in[stage]
                    sums_copy(stage + 1).start()
                    tile_source[stage + 1][...] = total
                    tile_copy(stage + 1).start()
                else:
                    sums_ref[...] = sums[stage] + sums_in[stage]
                    tile_out[...] = total[0]

            @pl.when((u >= 0) & (u < 2 * n))
            def _(stage=stage, u=u, count=count):
                done = copy(stage, u)
                side, _ = exchange(place, kind_of(u), stage)
                if stage == 0:
                    done.wait_recv()
                    mine = parts[lax.rem(u // 2, 2), side, lax.rem(u, 2)]
                else:
                    done.wait()
                    mine = held[stage - 1][spot(stage - 1, u), pl.ds(side * count, count)]
                if stage < 4:
                    at = spot(stage, u)
                    held[stage][at] = (held[stage][at].astype(f32) + mine.astype(f32)).astype(bf16)
                    copy(stage + 1, u).start()
                else:
                    write_out(u, held[stage][u, 0].astype(f32) + mine[0].astype(f32))

        return carry

    lax.fori_loop(0, 2 * n + SCATTER_WAITS[4], tick, 0)
    for u in range(2 * n - 4, 2 * n):
        copy(0, u).wait_send()
    rows_store.wait()


def backward_scatter(
    hidden, cotangent, live, flipped, gated_flipped, pv, gains, ph, inverse, pull, shared,
    projected, mixed, grad_gated, states, w_in, rb,
):
    length, width = hidden.shape
    columns = projected.shape[1]
    wide = mixed.shape[1]
    n_in, n_out = columns // (2 * HALF), width // HALF
    n = n_in + n_out
    blocks = length // BLK
    vmem = pl.BlockSpec(memory_space=pltpu.VMEM)
    anywhere = pl.BlockSpec(memory_space=pl.ANY)
    struct = jax.ShapeDtypeStruct
    return pl.pallas_call(
        partial(backward_kernel, n_in, n_out),
        out_shape=[
            struct((length, width), f32),
            struct((rb, columns - 2 * KEY), f32),
            struct((rb, KEY), f32),
            struct((2 * rb, width), f32),
            struct((8, KEY), f32),
            struct((8, KEY), f32),
        ],
        in_specs=[vmem] * 17 + [anywhere] * 5,
        out_specs=[anywhere] + [vmem] * 5,
        scratch_shapes=[pltpu.VMEM((2, 2, 2, 16, rb, HALF), bf16)]
        + [pltpu.VMEM((2 * (n if stage else EARLY), 16 >> stage, rb, HALF), bf16) for stage in range(5)]
        + [pltpu.VMEM((32 >> stage, 8, KEY), f32) for stage in range(6)]
        + [pltpu.VMEM((5, 8, KEY), f32)] * 2
        + [
            pltpu.VMEM((2, 4, length, HALF), f32),
            pltpu.VMEM((2, blocks, KEY, HALF), bf16),
            pltpu.VMEM((2, width, 2 * HALF), bf16),
            pltpu.VMEM((length, 3 * KEY), f32),
            pltpu.VMEM((length, 2 * HALF), bf16),
            pltpu.VMEM((length, width), f32),
            pltpu.VMEM((8, HALF), f32),
            pltpu.VMEM((8, wide), f32),
            pltpu.VMEM((8, HALF), f32),
            pltpu.VMEM((8, KEY), f32),
            pltpu.VMEM((8, KEY), f32),
            pltpu.VMEM((8, width), f32),
        ]
        + backward_scratch(length)
        + [pltpu.SemaphoreType.DMA((2 * n, 5))] * 2
        + [pltpu.SemaphoreType.DMA((2, 5))] * 2
        + [pltpu.SemaphoreType.DMA((8, 2)), pltpu.SemaphoreType.DMA((1,))],
        compiler_params=pltpu.CompilerParams(
            collective_id=1, has_side_effects=True, vmem_limit_bytes=67043328
        ),
        name="backward_scatter",
    )(
        hidden, cotangent, live, flipped, gated_flipped, pv, gains, ph, inverse, pull, *shared,
        projected, mixed, grad_gated, states, w_in,
    )


PIECE = 128


def finish_kernel(tile_ref, sums_ref, dt_in, *refs):
    big_in, refs = refs[:4], refs[4:]
    big_out, (pre_ref, dt_ref, conv_ref, shift_ref, bias_ref, log_ref, skip_ref, gate_ref) = refs[:4], refs[4:12]
    stages, (sem,) = refs[12:16], refs[16:]
    reads, writes = [], []
    for a, s, b in zip(big_in, stages, big_out):
        for at in range(0, a.shape[0], PIECE):
            rows = slice(at, min(at + PIECE, a.shape[0]))
            k = len(reads)
            reads.append(pltpu.make_async_copy(a.at[rows], s.at[rows], sem.at[0, k]))
            writes.append(pltpu.make_async_copy(s.at[rows], b.at[rows], sem.at[1, k]))
    for read in reads:
        read.start()
    pre_ref[...] = tile_ref[6:7, 0 : pre_ref.shape[1]]
    dt_ref[...] = dt_in[:, 0 : dt_ref.shape[1]]
    conv_ref[...] = tile_ref[0:4, 0 : conv_ref.shape[1]]
    shift_ref[...] = tile_ref[4:5, 0 : shift_ref.shape[1]]
    gate_ref[...] = tile_ref[5:6, 0 : gate_ref.shape[1]]
    for k, ref in enumerate((bias_ref, log_ref, skip_ref)):
        ref[...] = sums_ref[k : k + 1, 0 : ref.shape[1]]
    for read, write in zip(reads, writes):
        read.wait()
        write.start()
    for write in writes:
        write.wait()


def finish(tile, sums, grad_dt, arrays, small_shapes):
    vmem = pl.BlockSpec(memory_space=pltpu.VMEM)
    anywhere = pl.BlockSpec(memory_space=pl.ANY)
    return pl.pallas_call(
        finish_kernel,
        out_shape=[jax.ShapeDtypeStruct(a.shape, a.dtype) for a in arrays]
        + [jax.ShapeDtypeStruct(shape, f32) for shape in small_shapes],
        in_specs=[vmem] * 3 + [anywhere] * 4,
        out_specs=[anywhere] * 4 + [vmem] * 8,
        scratch_shapes=[pltpu.VMEM(a.shape, a.dtype) for a in arrays] + [
            pltpu.SemaphoreType.DMA((2, sum(-(-a.shape[0] // PIECE) for a in arrays)))
        ],
        name="finish",
    )(tile, sums, grad_dt, *arrays)


def pre_norm_inverse(rows):
    return lax.rsqrt(jnp.mean(rows * rows, axis=1, keepdims=True) + epsilon)


AXES = ("dp", "fsdp")


def gather_rows(shard):
    return lax.all_gather(shard, AXES, axis=0, tiled=True)


def scatter_rows(whole):
    return lax.psum_scatter(whole, AXES, scatter_dimension=0, tiled=True)


def vector_tile(conv_weight, conv_bias, gate_gain, norm_gain):
    rows = [conv_weight, conv_bias[None], gate_gain[None], norm_gain[None]]
    rows = [jnp.pad(row.astype(f32), ((0, 0), (0, KEY - row.shape[1]))) for row in rows]
    return jnp.concatenate(rows + [jnp.zeros((1, KEY), f32)], axis=0)


def vector_tiles(conv, gate, pre, parts):
    rows = []
    for whole in (conv, gate, pre):
        part = whole.shape[1] // parts
        split_up = jnp.transpose(whole.reshape(-1, parts, part), (1, 0, 2))
        rows.append(jnp.pad(split_up, ((0, 0), (0, 0), (0, KEY - part))))
    return jnp.concatenate(rows + [jnp.zeros((parts, 1, KEY), f32)], axis=1)


def shards(
    kernels, hidden, cotangent, lengths, norm_gain, in_proj, dt_proj, conv_weight, conv_bias,
    dt_bias, a_log, skip_gain, gate_gain, out_proj,
):
    length, width = hidden.shape
    assert lengths.shape[0] == 1
    rows_in, columns = in_proj.shape
    heads = dt_bias.shape[0]
    parts = width // rows_in
    taps, conv_part = conv_weight.shape
    gate_part = gate_gain.shape[0]
    wide = gate_part * parts
    total = columns + 2 * KEY

    if kernels:
        rows = lambda *vectors: [v.reshape(1, -1) for v in vectors]
        (
            w_in, projected, mixed, states, gated_flipped, grad_gated, output, flipped, live, ph, pv, gains, inverse_two,
            pull, *shared,
        ) = gather_forward(
            lengths, hidden, cotangent, in_proj, dt_proj, out_proj, conv_weight,
            *rows(conv_bias, gate_gain, norm_gain, dt_bias, a_log, skip_gain),
        )
        input_grad, grad_in, grad_dt, grad_out, small_sum, head_sums = backward_scatter(
            hidden, cotangent, live, flipped, gated_flipped, pv, gains, ph,
            inverse_two, pull, shared, projected, mixed, grad_gated, states, w_in, rows_in,
        )
        output, input_grad, grad_in, grad_out, *small = finish(
            small_sum, head_sums, grad_dt, (output, input_grad, grad_in, grad_out),
            ((1, rows_in), (rows_in, heads), (taps, conv_part), (1, conv_part))
            + ((1, heads),) * 3 + ((1, gate_part),),
        )
        pre, dt, conv, shift, bias, log, skip, gate = small
        return (
            output, input_grad, pre[0], grad_in, dt, conv, shift[0], bias[0], log[0], skip[0], gate[0], grad_out
        )

    fill = jnp.zeros((rows_in, total - columns - heads), bf16)
    packed = jnp.concatenate([in_proj, dt_proj, fill], axis=1)
    tile = vector_tile(conv_weight, conv_bias, gate_gain, norm_gain)
    ph = jnp.pad(jnp.stack([dt_bias, a_log]).astype(f32), ((0, 6), (0, KEY - heads)))
    skip_wide = jnp.repeat(skip_gain.astype(f32), HD)[None]
    live = (jnp.arange(length) < lengths[0]).astype(f32)[:, None]
    rows_wide = hidden.astype(f32)
    cot_wide = cotangent.astype(f32)
    upstream = (cot_wide * live).astype(bf16)
    inverse_one = pre_norm_inverse(rows_wide)
    w_in, w_out = gather_rows(packed), gather_rows(out_proj)
    tiles = gather_rows(tile[None])
    whole = lambda rows, part: jnp.transpose(tiles[:, rows, :part], (1, 0, 2)).reshape(-1, parts * part)
    conv_all = whole(slice(0, 5), conv_part)
    gain_two = whole(slice(5, 6), gate_part)
    gain_one = whole(slice(6, 7), rows_in)[0]
    rest = jnp.concatenate([gain_two, skip_wide, jnp.zeros((1, wide), f32)], axis=0)
    pv = jnp.concatenate([conv_all, jnp.pad(rest, ((0, 0), (0, 2 * KEY)))], axis=0)
    normed = (rows_wide * inverse_one * gain_one[None, :]).astype(bf16)
    projected = mm(normed, w_in)
    mixed, product, states, inverse_two, *shared = mixer_forward(projected, pv, ph)
    inv = inverse_two[:, :1]
    gated = (product * inv * gain_two).astype(bf16)
    output = (rows_wide + live * mm(gated, w_out)).astype(bf16)
    grad_gated = mm_nt(upstream, w_out)
    pull = jnp.sum(grad_gated * gain_two * product, axis=1, keepdims=True)
    pull = jnp.broadcast_to(inv * inv * inv * pull / wide, inverse_two.shape)
    grad_out = mm_tn(gated, upstream)
    grad_proj, sums_v, sums_k, sums_h = mixer_backward(
        projected, pv, ph, mixed, grad_gated, states, inverse_two, pull, shared
    )
    skip_grad = jnp.pad(jnp.sum(sums_v[6].reshape(heads, HD), axis=1), (0, KEY - heads))[None]
    head_grads = jnp.concatenate([sums_h[:2], skip_grad, jnp.zeros((5, KEY), f32)], axis=0)

    grad_normed = mm_nt(grad_proj, w_in)
    scaled = grad_normed * gain_one[None, :]
    row_sums = jnp.sum(scaled * rows_wide, axis=1, keepdims=True) / width
    grad_rows = inverse_one * scaled - rows_wide * (inverse_one * inverse_one * inverse_one * row_sums)
    input_grad = cot_wide + grad_rows
    grad_gain_one = jnp.sum(grad_normed * rows_wide * inverse_one, axis=0, keepdims=True)

    conv_grad = jnp.concatenate([sums_v[:5], sums_k[:5]], axis=1)
    small = vector_tiles(conv_grad, sums_v[5:6], grad_gain_one, parts)
    grad_out = scatter_rows(grad_out.astype(bf16)).astype(f32)
    head_sums = lax.psum(head_grads, AXES)
    grad_all = scatter_rows(mm_tn(normed, grad_proj).astype(bf16)).astype(f32)
    grad_in, grad_dt = grad_all[:, :columns], grad_all[:, columns:]
    small_sum = scatter_rows(small)[0]
    return (
        output,
        input_grad,
        small_sum[6, :rows_in],
        grad_in,
        grad_dt[:, :heads],
        small_sum[:taps, :conv_part],
        small_sum[taps, :conv_part],
        head_sums[0, :heads],
        head_sums[1, :heads],
        head_sums[2, :heads],
        small_sum[5, :gate_part],
        grad_out,
    )


def solution(mesh):
    rows = P(AXES, None)
    vector = P(AXES)
    last = P(None, AXES)
    return jax.shard_map(
        partial(shards, mesh.shape["dp"] == 8 and mesh.shape["fsdp"] == 4),
        mesh=mesh,
        in_specs=(rows, rows, vector, vector, rows, rows, last, vector, P(), P(), P(), vector, rows),
        out_specs=(rows, rows, vector, rows, rows, last, vector, P(), P(), P(), vector, rows),
        check_vma=False,
    )
```

```python
from functools import partial

import jax
import jax.numpy as jnp
from jax import lax
from jax.experimental import pallas as pl
from jax.experimental.pallas import tpu as pltpu
from jax.sharding import PartitionSpec as P

f32 = jnp.float32
bf16 = jnp.bfloat16
epsilon = 1e-05
highest = lax.Precision.HIGHEST
BLK = 128
GH = 4
HD = 64
GC = GH * HD
KEY = 128
NEG = -1e30


def sigmoid(v):
    return 0.5 * jnp.tanh(0.5 * v) + 0.5


def mm(a, b):
    return lax.dot_general(a, b, (((1,), (0,)), ((), ())), preferred_element_type=f32)


def mm_nt(a, b):
    return lax.dot_general(a, b, (((1,), (1,)), ((), ())), preferred_element_type=f32)


def mm_tn(a, b):
    return lax.dot_general(a, b, (((0,), (0,)), ((), ())), preferred_element_type=f32)


def mm_hi(a, b, dims=((1,), (0,))):
    return lax.dot_general(a, b, (dims, ((), ())), preferred_element_type=f32, precision=highest)


def split(v):
    hi = v.astype(bf16)
    lo = (v - hi.astype(f32)).astype(bf16)
    return jnp.concatenate([hi, lo], axis=1)


def iota(shape, dim):
    return lax.broadcasted_iota(jnp.int32, shape, dim)


def expander(g):
    rows = iota((2 * KEY, GC), 0)
    cols = iota((2 * KEY, GC), 1)
    return jnp.where(lax.rem(rows, KEY) == cols // HD + g * GH, 1.0, 0.0).astype(bf16)


def reducer(g):
    rows = iota((GC, KEY), 0)
    cols = iota((GC, KEY), 1)
    return jnp.where(rows // HD + g * GH == cols, 1.0, 0.0).astype(bf16)


def taps_of(window, par):
    out = par[4:5] + par[3:4] * window[8:136]
    for k in range(3):
        out = out + par[k : k + 1] * window[5 + k : 133 + k]
    return out


def group_rows(st_ref, g, half, rows):
    tile = st_ref[pl.ds(pl.multiple_of(g // 2 * 8, 8), 8), rows]
    return jnp.where(half == 0, tile[:GH], tile[GH:])


def forward_shared(
    rawk_ref, dtr_ref, pv_ref, key_at, ph_ref, s_ref, st_ref, hl_ref, ehl_ref, kb_ref, kt_ref, sc_ref, padk
):
    blocks = rawk_ref.shape[0] // BLK
    dt = jax.nn.softplus(dtr_ref[...] + ph_ref[0:1, :])
    la = -dt * jnp.exp(ph_ref[1:2, :])
    tri = jnp.where(iota((BLK, BLK), 0) >= iota((BLK, BLK), 1), 1.0, 0.0).astype(f32)
    hl_ref[0] = split(dt)
    ehl_ref[...] = jnp.zeros_like(ehl_ref)
    padk[0:8] = jnp.zeros((8, 2 * KEY), f32)
    padk[8:] = rawk_ref[...]
    par = pv_ref[:, key_at : key_at + 2 * KEY]
    for k in range(blocks):
        rows = slice(k * BLK, (k + 1) * BLK)
        s = mm_hi(tri, la[rows])
        s_ref[rows] = s
        st_ref[:, rows] = s.T
        hl_ref[1, rows] = split(jnp.exp(s))
        hl_ref[2, rows] = split(jnp.exp(s[BLK - 1 :] - s))
        ehl_ref[k : k + 1] = split(jnp.exp(s[BLK - 1 :]))
        u = taps_of(padk[k * BLK : k * BLK + BLK + 8], par)
        v = u * sigmoid(u)
        kb_ref[rows] = v.astype(bf16)
        kt_ref[:, rows] = v.T.astype(bf16)
        sc_ref[k] = mm_hi(v[:, KEY:], v[:, :KEY], ((1,), (1,)))


def forward_group(
    g, gate_ref, rawv_ref, pv_ref, s_ref, st_ref, hl_ref, ehl_ref, kb_ref, kt_ref, sc_ref,
    y_ref, p_ref, hst_ref, pad, sg, hcar, ssq,
):
    blocks = gate_ref.shape[0] // BLK
    pad[8:] = rawv_ref[...]
    sg[...] = pltpu.roll(s_ref[...], lax.rem(KEY - g * GH, KEY), 1)
    ex = expander(g)
    bias = jnp.where(iota((BLK, BLK), 0) >= iota((BLK, BLK), 1), 0.0, NEG).astype(f32)
    low = iota((BLK, KEY), 1) < HD
    eend = mm(ehl_ref[...], ex)
    parg = pv_ref[:, pl.ds(pl.multiple_of(g * GC, GC), GC)]
    half = lax.rem(g, 8 // GH)
    hcar[...] = jnp.zeros_like(hcar)
    for k in range(blocks):
        rows = slice(k * BLK, (k + 1) * BLK)
        dtx = mm(hl_ref[0, rows], ex)
        exx = mm(hl_ref[1, rows], ex)
        txx = mm(hl_ref[2, rows], ex)
        hb = hcar[...].astype(bf16)
        hst_ref[k] = hb
        outer = mm(kb_ref[rows, KEY:], hb)
        across = group_rows(st_ref, g, half, rows)
        xts = []
        for q in range(GC // KEY):
            cols = slice(q * KEY, (q + 1) * KEY)
            par = parg[:, cols]
            u = taps_of(pad[k * BLK : k * BLK + BLK + 8, cols], par)
            v = u * sigmoid(u)
            x = v * dtx[:, cols]
            xts.append((x * txx[:, cols]).astype(bf16))
            xb = x.astype(bf16)
            zero = jnp.zeros_like(xb)
            x2 = jnp.concatenate([jnp.where(low, xb, zero), jnp.where(low, zero, xb)], axis=0)
            ms = []
            for side in range(2):
                j = 2 * q + side
                spread = sg[rows, j : j + 1] - across[j : j + 1]
                ms.append((jnp.exp(spread + bias) * sc_ref[k]).astype(bf16))
            y = mm(jnp.concatenate(ms, axis=1), x2)
            y = y + outer[:, cols] * exx[:, cols] + par[6:7] * v
            y_ref[rows, cols] = y
            gate = gate_ref[rows, cols]
            p = y * (gate * sigmoid(gate))
            p_ref[rows, pl.ds(pl.multiple_of(g * GC + q * KEY, KEY), KEY)] = p
            ssq[rows] += p * p
        if k + 1 < blocks:
            hcar[...] = eend[k : k + 1] * hcar[...] + mm(kt_ref[:KEY, rows], jnp.concatenate(xts, axis=1))


def fwd_kernel(
    gate_ref, rawv_ref, rawk_ref, dtr_ref, pv_ref, ph_ref,
    y_ref, p_ref, hst_ref, r_ref, s_ref, st_ref, hl_ref, ehl_ref, kb_ref, kt_ref, sc_ref,
    pad, padk, sg, hcar, ssq,
):
    g = pl.program_id(0)
    wide = p_ref.shape[1]
    shared = (s_ref, st_ref, hl_ref, ehl_ref, kb_ref, kt_ref, sc_ref)

    @pl.when(g == 0)
    def _():
        forward_shared(rawk_ref, dtr_ref, pv_ref, wide, ph_ref, *shared, padk)
        pad[0:8] = jnp.zeros((8, GC), f32)
        ssq[...] = jnp.zeros_like(ssq)

    forward_group(g, gate_ref, rawv_ref, pv_ref, *shared, y_ref, p_ref, hst_ref, pad, sg, hcar, ssq)

    @pl.when(g == pl.num_programs(0) - 1)
    def _():
        mean = jnp.sum(ssq[...], axis=1, keepdims=True) / wide
        r_ref[...] = jnp.broadcast_to(lax.rsqrt(mean + epsilon), r_ref.shape)


def backward_start(length, pad, dpad, dsc, dkb, dsrow, dscol, ddt):
    pad[0:8] = jnp.zeros((8, GC), f32)
    dpad[length:] = jnp.zeros((8, GC), f32)
    for ref in (dsc, dkb, dsrow, dscol, ddt):
        ref[...] = jnp.zeros_like(ref)


def backward_group(
    g, gate_ref, rawv_ref, y_ref, gg_ref, hst_ref, r_ref, c_ref, pv_ref, shared,
    dgate_ref, draw_ref, sv_ref, pad, dpad, sg, dhcar, dsc, dkb, dsrow, dscol, ddt,
):
    s_ref, st_ref, hl_ref, ehl_ref, kb_ref, kt_ref, sc_ref = shared
    blocks = gate_ref.shape[0] // BLK
    pad[8:] = rawv_ref[...]
    sg[...] = pltpu.roll(s_ref[...], lax.rem(KEY - g * GH, KEY), 1)
    ex = expander(g)
    red = reducer(g)
    row = iota((BLK, BLK), 0)
    col = iota((BLK, BLK), 1)
    bias = jnp.where(row >= col, 0.0, NEG).astype(f32)
    strict = row > col
    low = iota((BLK, KEY), 1) < HD
    eend = mm(ehl_ref[...], ex)
    parg = pv_ref[:, pl.ds(pl.multiple_of(g * GC, GC), GC)]
    half = lax.rem(g, 8 // GH)
    tile_at = pl.ds(pl.multiple_of(g // 2 * 8, 8), 8)
    mine = (iota((8, BLK), 0) < GH) == (half == 0)
    dhcar[...] = jnp.zeros_like(dhcar)
    sv_ref[...] = jnp.zeros_like(sv_ref)
    for k in range(blocks - 1, -1, -1):
        rows = slice(k * BLK, (k + 1) * BLK)
        dtx = mm(hl_ref[0, rows], ex)
        exx = mm(hl_ref[1, rows], ex)
        txx = mm(hl_ref[2, rows], ex)
        hb = hst_ref[k]
        dhb = dhcar[...].astype(bf16)
        ch = mm(kb_ref[rows, KEY:], hb)
        qq = mm(kb_ref[rows, :KEY], dhb)
        across = group_rows(st_ref, g, half, rows)
        dyes, xts, zs, oys, ddts, ecols = [], [], [], [], [], []
        dsrow_k = jnp.zeros((BLK, KEY), f32)
        for q in range(GC // KEY):
            cols = slice(q * KEY, (q + 1) * KEY)
            par = parg[:, cols]
            window = pad[k * BLK : k * BLK + BLK + 8, cols]
            u = taps_of(window, par)
            su = sigmoid(u)
            v = u * su
            x = v * dtx[:, cols]
            xb = x.astype(bf16)
            gate = gate_ref[rows, cols]
            y = y_ref[rows, cols]
            sgt = sigmoid(gate)
            silu_g = gate * sgt
            p = y * silu_g
            dgn = gg_ref[rows, cols] * r_ref[rows]
            sv_ref[5:6, cols] += jnp.sum(dgn * p, axis=0, keepdims=True)
            dp = dgn * par[5:6] - p * c_ref[rows]
            dgate_ref[rows, cols] = (dp * y * (sgt + silu_g * (1.0 - sgt))).astype(bf16)
            dy = dp * silu_g
            sv_ref[6:7, cols] += jnp.sum(dy * v, axis=0, keepdims=True)
            dyb = dy.astype(bf16)
            dye = dy * exx[:, cols]
            dyes.append(dye.astype(bf16))
            oys.append((dye * ch[:, cols]).astype(bf16))
            xt = x * txx[:, cols]
            xts.append(xt.astype(bf16))
            zs.append((xt * qq[:, cols]).astype(bf16))
            zero = jnp.zeros_like(dyb)
            dy2 = jnp.concatenate([jnp.where(low, dyb, zero), jnp.where(low, zero, dyb)], axis=0)
            dm2 = mm_nt(dy2, xb)
            ms, scored = [], []
            for side in range(2):
                j = 2 * q + side
                spread = sg[rows, j : j + 1] - across[j : j + 1]
                decay = jnp.exp(spread + bias)
                m = decay * sc_ref[k]
                ms.append(m.astype(bf16))
                dm = dm2[side * BLK : (side + 1) * BLK]
                part = decay * dm
                scored.append(part)
                e = jnp.where(strict, part * sc_ref[k], 0.0)
                dsrow_k = jnp.where(col == g * GH + j, jnp.sum(e, axis=1, keepdims=True), dsrow_k)
                ecols.append(jnp.sum(e, axis=0, keepdims=True))
            dsc[k] += scored[0] + scored[1]
            dx = mm_tn(jnp.concatenate(ms, axis=0), dy2) + qq[:, cols] * txx[:, cols]
            dv = dx * dtx[:, cols] + par[6:7] * dy
            ddts.append((dx * v).astype(bf16))
            du = dv * (su + v * (1.0 - su))
            dpad[rows, cols] = du
            sv_ref[4:5, cols] += jnp.sum(du, axis=0, keepdims=True)
            for t in range(4):
                sv_ref[t : t + 1, cols] += jnp.sum(du * window[5 + t : 133 + t], axis=0, keepdims=True)
        dscol[tile_at, rows] += jnp.where(mine, jnp.concatenate(ecols + ecols, axis=0), 0.0)
        dye = jnp.concatenate(dyes, axis=1)
        xt = jnp.concatenate(xts, axis=1)
        zsum = mm(jnp.concatenate(zs, axis=1), red)
        ddt[rows] += mm(jnp.concatenate(ddts, axis=1), red)
        hterm = eend[k : k + 1] * jnp.sum(dhcar[...] * hb.astype(f32), axis=0, keepdims=True)
        end = jnp.sum(zsum, axis=0, keepdims=True) + mm_hi(hterm, red.astype(f32))
        add = dsrow_k + mm(jnp.concatenate(oys, axis=1), red) - zsum
        dsrow[rows] += add + jnp.where(row == BLK - 1, end, 0.0)
        dkb[rows, KEY:] += mm_nt(dye, hb)
        dkb[rows, :KEY] += mm_nt(xt, dhb)
        if k:
            dhcar[...] = eend[k : k + 1] * dhcar[...] + mm(kt_ref[KEY:, rows], dye)

    for k in range(blocks):
        rows = slice(k * BLK, (k + 1) * BLK)
        for q in range(GC // KEY):
            cols = slice(q * KEY, (q + 1) * KEY)
            par = parg[:, cols]
            window = dpad[k * BLK : k * BLK + BLK + 8, cols]
            out = par[3:4] * window[0:BLK]
            for t in range(3):
                out = out + par[t : t + 1] * window[3 - t : 3 - t + BLK]
            draw_ref[rows, cols] = out.astype(bf16)


def backward_shared(
    rawk_ref, dtr_ref, pv_ref, key_at, ph_ref, kb_ref, dkeys_ref, ddt_ref, sk_ref, sh_ref,
    padk, dpadk, dsc, dkb, dsrow, dscol, ddt,
):
    length = rawk_ref.shape[0]
    blocks = length // BLK
    row = iota((BLK, BLK), 0)
    col = iota((BLK, BLK), 1)
    padk[0:8] = jnp.zeros((8, 2 * KEY), f32)
    padk[8:] = rawk_ref[...]
    dpadk[length:] = jnp.zeros((8, 2 * KEY), f32)
    sk_ref[...] = jnp.zeros_like(sk_ref)
    sh_ref[...] = jnp.zeros_like(sh_ref)
    upper = jnp.where(row <= col, 1.0, 0.0).astype(f32)
    par = pv_ref[:, key_at : key_at + 2 * KEY]
    for k in range(blocks):
        rows = slice(k * BLK, (k + 1) * BLK)
        window = padk[k * BLK : k * BLK + BLK + 8]
        u = taps_of(window, par)
        su = sigmoid(u)
        ds = dsc[k].astype(bf16)
        db = dkb[rows, :KEY] + mm_tn(ds, kb_ref[rows, KEY:])
        dc = dkb[rows, KEY:] + mm(ds, kb_ref[rows, :KEY])
        du = jnp.concatenate([db, dc], axis=1) * (su + u * su * (1.0 - su))
        dpadk[rows] = du
        sk_ref[4:5] += jnp.sum(du, axis=0, keepdims=True)
        for t in range(4):
            sk_ref[t : t + 1] += jnp.sum(du * window[5 + t : 133 + t], axis=0, keepdims=True)
        dla = mm_hi(upper, dsrow[rows] - dscol[:, rows].T)
        z = dtr_ref[rows] + ph_ref[0:1, :]
        rate = jnp.exp(ph_ref[1:2, :])
        dt = jax.nn.softplus(z)
        sh_ref[1:2] += jnp.sum(dla * (-dt * rate), axis=0, keepdims=True)
        dz = (ddt[rows] - dla * rate) * sigmoid(z)
        sh_ref[0:1] += jnp.sum(dz, axis=0, keepdims=True)
        ddt_ref[rows] = dz.astype(bf16)
    for k in range(blocks):
        rows = slice(k * BLK, (k + 1) * BLK)
        window = dpadk[k * BLK : k * BLK + BLK + 8]
        out = par[3:4] * window[0:BLK]
        for t in range(3):
            out = out + par[t : t + 1] * window[3 - t : 3 - t + BLK]
        dkeys_ref[rows] = out.astype(bf16)


def bwd_kernel(
    gate_ref, rawv_ref, rawk_ref, dtr_ref, pv_ref, ph_ref,
    y_ref, gg_ref, hst_ref, r_ref, c_ref, s_ref, st_ref, hl_ref, ehl_ref, kb_ref, kt_ref, sc_ref,
    dproj_ref, sv_ref, sk_ref, sh_ref,
    pad, padk, dpad, dpadk, sg, dhcar, dsc, dkb, dsrow, dscol, ddt,
):
    g = pl.program_id(0)
    length, total = dproj_ref.shape
    wide = GC * pl.num_programs(0)
    shared = (s_ref, st_ref, hl_ref, ehl_ref, kb_ref, kt_ref, sc_ref)

    @pl.when(g == 0)
    def _():
        backward_start(length, pad, dpad, dsc, dkb, dsrow, dscol, ddt)

    gate_at = pl.ds(pl.multiple_of(g * GC, GC), GC)
    draw_at = pl.ds(pl.multiple_of(wide + g * GC, GC), GC)
    backward_group(
        g, gate_ref, rawv_ref, y_ref, gg_ref, hst_ref, r_ref, c_ref, pv_ref, shared,
        dproj_ref.at[:, gate_at], dproj_ref.at[:, draw_at], sv_ref,
        pad, dpad, sg, dhcar, dsc, dkb, dsrow, dscol, ddt,
    )

    @pl.when(g == pl.num_programs(0) - 1)
    def _():
        keys = 2 * wide
        dproj_ref[:, keys + 3 * KEY :] = jnp.zeros((length, total - keys - 3 * KEY), bf16)
        backward_shared(
            rawk_ref, dtr_ref, pv_ref, wide, ph_ref, kb_ref,
            dproj_ref.at[:, keys : keys + 2 * KEY], dproj_ref.at[:, keys + 2 * KEY : keys + 3 * KEY],
            sk_ref, sh_ref, padk, dpadk, dsc, dkb, dsrow, dscol, ddt,
        )


def whole_spec(shape):
    return pl.BlockSpec(shape, lambda g: (0,) * len(shape))


def state_specs(length):
    return (
        ((length, KEY), f32),
        ((KEY, length), f32),
        ((3, length, 2 * KEY), bf16),
        ((8, 2 * KEY), bf16),
        ((length, 2 * KEY), bf16),
        ((2 * KEY, length), bf16),
        ((length // BLK, BLK, BLK), f32),
    )


def proj_specs(length, groups):
    wide = groups * GC
    return [
        pl.BlockSpec((length, GC), lambda g: (0, g)),
        pl.BlockSpec((length, GC), lambda g: (0, groups + g)),
        pl.BlockSpec((length, 2 * KEY), lambda g: (0, 2 * wide // (2 * KEY))),
        pl.BlockSpec((length, KEY), lambda g: (0, 2 * wide // KEY + 2)),
        whole_spec((8, wide + 2 * KEY)),
        whole_spec((8, KEY)),
    ]


def mixer_forward(projected, pv, ph):
    length = projected.shape[0]
    wide = pv.shape[1] - 2 * KEY
    groups = wide // GC
    blocks = length // BLK
    column = pl.BlockSpec((length, GC), lambda g: (0, g))
    shared = state_specs(length)
    return pl.pallas_call(
        fwd_kernel,
        grid=(groups,),
        in_specs=proj_specs(length, groups),
        out_specs=[
            column,
            whole_spec((length, wide)),
            pl.BlockSpec((blocks, KEY, GC), lambda g: (0, 0, g)),
            whole_spec((length, KEY)),
        ]
        + [whole_spec(shape) for shape, _ in shared],
        out_shape=[
            jax.ShapeDtypeStruct((length, wide), f32),
            jax.ShapeDtypeStruct((length, wide), f32),
            jax.ShapeDtypeStruct((blocks, KEY, wide), bf16),
            jax.ShapeDtypeStruct((length, KEY), f32),
        ]
        + [jax.ShapeDtypeStruct(shape, dtype) for shape, dtype in shared],
        scratch_shapes=[
            pltpu.VMEM((length + 8, GC), f32),
            pltpu.VMEM((length + 8, 2 * KEY), f32),
            pltpu.VMEM((length, KEY), f32),
            pltpu.VMEM((KEY, GC), f32),
            pltpu.VMEM((length, KEY), f32),
        ],
        name="mixer_forward",
    )(projected, projected, projected, projected, pv, ph)


def backward_scratch(length):
    return [
        pltpu.VMEM((length + 8, GC), f32),
        pltpu.VMEM((length + 8, 2 * KEY), f32),
        pltpu.VMEM((length + 8, GC), f32),
        pltpu.VMEM((length + 8, 2 * KEY), f32),
        pltpu.VMEM((length, KEY), f32),
        pltpu.VMEM((KEY, GC), f32),
        pltpu.VMEM((length // BLK, BLK, BLK), f32),
        pltpu.VMEM((length, 2 * KEY), f32),
        pltpu.VMEM((length, KEY), f32),
        pltpu.VMEM((KEY, length), f32),
        pltpu.VMEM((length, KEY), f32),
    ]


def mixer_backward(projected, pv, ph, mixed, grad_gated, states, inverse, pull, shared):
    length, total = projected.shape
    wide = pv.shape[1] - 2 * KEY
    groups = wide // GC
    blocks = length // BLK
    column = pl.BlockSpec((length, GC), lambda g: (0, g))
    return pl.pallas_call(
        bwd_kernel,
        grid=(groups,),
        in_specs=proj_specs(length, groups)
        + [
            column,
            column,
            pl.BlockSpec((blocks, KEY, GC), lambda g: (0, 0, g)),
            whole_spec((length, KEY)),
            whole_spec((length, KEY)),
        ]
        + [whole_spec(shape) for shape, _ in state_specs(length)],
        out_specs=[
            whole_spec((length, total)),
            pl.BlockSpec((8, GC), lambda g: (0, g)),
            whole_spec((8, 2 * KEY)),
            whole_spec((8, KEY)),
        ],
        out_shape=[
            jax.ShapeDtypeStruct((length, total), bf16),
            jax.ShapeDtypeStruct((8, wide), f32),
            jax.ShapeDtypeStruct((8, 2 * KEY), f32),
            jax.ShapeDtypeStruct((8, KEY), f32),
        ],
        scratch_shapes=backward_scratch(length),
        name="mixer_backward",
    )(projected, projected, projected, projected, pv, ph, mixed, grad_gated, states, inverse, pull, *shared)


MESH = pl.DeviceIdType.MESH
HALF = 256


ORDERS = ("xylh", "yxlh", "lhxy")
GATHER_WAITS = (3, 6, 10, 14, 16)
SCATTER_WAITS = (2, 6, 10, 14, 18)


def places():
    d, f = lax.axis_index("dp"), lax.axis_index("fsdp")
    bits = {"x": d % 2, "y": f // 2, "l": d // 2 % 2, "h": d // 4, "c": f % 2}
    far = {"x": (1, 0), "y": (0, 2), "l": (2, 0), "h": (4, 0), "c": (0, 1)}
    hops = {k: tuple(w * (1 - 2 * bits[k]) if w else 0 for w in far[k]) for k in far}
    return d, f, bits, hops


def kind_of(u):
    r = lax.rem(u, 9)
    along_y = (r == 1) | (r == 3) | (r == 6) | ((r == 7) & (lax.rem(u // 9, 2) == 1))
    return jnp.where((r == 4) | (r == 8), 2, jnp.where(along_y, 1, 0))


def pick(kind, values):
    if isinstance(kind, int):
        return values[kind]
    if all(v is values[0] for v in values):
        return values[0]
    return jnp.where(kind == 0, values[0], jnp.where(kind == 1, values[1], values[2]))


def exchange(place, kind, stage):
    d, f, bits, hops = place
    axes = "ccc" if stage == 0 else [order[stage - 1] for order in ORDERS]
    side = pick(kind, [bits[a] for a in axes])
    return side, (d + pick(kind, [hops[a][0] for a in axes]), f + pick(kind, [hops[a][1] for a in axes]))


def strides(kind):
    return {a: pick(kind, [8 >> order.index(a) for order in ORDERS]) for a in "xylh"}


def position(kind, bits):
    step = strides(kind)
    return sum(bits[a] * step[a] for a in "xylh")


def all_positions(kind):
    step = strides(kind)
    out = []
    for i in range(32):
        bits = {"x": i // 4 % 2, "y": i // 2 % 2, "l": i // 8 % 2, "h": i // 16}
        out.append((i % 2, sum(step[a] for a in "xylh" if bits[a])))
    return out


def greet(partners):
    barrier = pltpu.get_barrier_semaphore()
    for partner in partners:
        pl.semaphore_signal(barrier, inc=1, device_id=partner, device_id_type=MESH)
    pl.semaphore_wait(barrier, len(partners))


def spread_lanes(tiles, width, lane, count):
    out = [jnp.zeros(tiles[0].shape, f32) for _ in range(count)]
    for i, tile in enumerate(tiles):
        at, shift = divmod(i * width, KEY)
        turned = pltpu.roll(tile, shift, 1) if shift else tile
        end = shift + width
        out[at] = out[at] + jnp.where((lane >= shift) & (lane < end), turned, 0.0)
        if end > KEY:
            out[at + 1] = out[at + 1] + jnp.where(lane < end - KEY, turned, 0.0)
    return out


def forward_kernel(
    n_in, n_out, lengths_ref, hidden_in, cot_in, w_ref, wd_ref, wo_ref, conv_ref, shift_ref, gate_ref, pre_ref,
    dt_ref, log_ref, skip_ref,
    w_out, proj_out, mixed_out, states_out, flipped_gated_out, gg_out, out_out, flipped_out,
    live_ref, ph_ref, pv_ref, gain, r_ref, c_ref, s_ref, st_ref, hl_ref, ehl_ref, kb_ref, kt_ref, sc_ref,
    held, tiles, w_stage, wo_stage, proj_stage, mixed_stage, states_stage, flip_stage, normed, gated, big,
    pad, padk, sg, hcar, ssq, dots, hidden_ref, cot_ref, out_ref, flipped_ref,
    send, recv, tile_sem, out_sem, gg_sem, row_sem,
):
    rb = w_ref.shape[0]
    length, width = hidden_ref.shape
    wide = big.shape[1]
    n = n_in + n_out
    hidden_load = pltpu.make_async_copy(hidden_in, hidden_ref, row_sem.at[0])
    cot_load = pltpu.make_async_copy(cot_in, cot_ref, row_sem.at[1])
    flipped_store = pltpu.make_async_copy(flipped_ref, flipped_out, row_sem.at[2])
    hidden_load.start()
    cot_load.start()
    place = places()
    greet([exchange(place, 0, stage)[1] for stage in range(5)])
    count = (1, 2, 4, 8, 16)

    def columns(i, half):
        group = (i - 1) * HALF + half * wide
        return pl.ds(pl.multiple_of(jnp.where(i == 0, 2 * wide + half * HALF, group), HALF), HALF)

    def own_at(kind):
        return place[2]["c"] * 16 + position(kind, place[2])

    def copy(stage, u):
        kind = kind_of(u)
        start = own_at(kind) // count[stage] * count[stage]
        block = held.at[u, pl.ds(start, count[stage])]
        return pltpu.make_async_remote_copy(
            src_ref=block,
            dst_ref=block,
            send_sem=send.at[u, stage],
            recv_sem=recv.at[u, stage],
            device_id=exchange(place, kind, 4 - stage)[1],
            device_id_type=MESH,
        )

    def tile_copy(stage):
        block = tiles.at[pl.ds(own_at(0) // count[stage] * count[stage], count[stage])]
        return pltpu.make_async_remote_copy(
            src_ref=block,
            dst_ref=block,
            send_sem=tile_sem.at[0, stage],
            recv_sem=tile_sem.at[1, stage],
            device_id=exchange(place, 0, 4 - stage)[1],
            device_id_type=MESH,
        )

    def weight_stores(i):
        slot = lax.rem(i, 2)
        copies = []
        for half in range(2):
            cols = slice(half * HALF, (half + 1) * HALF)
            copies.append(
                pltpu.make_async_copy(
                    w_stage.at[slot, :, cols], w_out.at[:, columns(i, half)], out_sem.at[half, slot]
                )
            )
            copies.append(
                pltpu.make_async_copy(
                    proj_stage.at[slot, :, cols], proj_out.at[:, columns(i, half)], out_sem.at[2 + half, slot]
                )
            )
        return copies

    def group_stores(i):
        slot = lax.rem(i, 2)
        cols = pl.ds(pl.multiple_of((i - 1) * HALF, HALF), HALF)
        return (
            pltpu.make_async_copy(mixed_stage.at[slot], mixed_out.at[:, cols], out_sem.at[4, slot]),
            pltpu.make_async_copy(states_stage.at[slot], states_out.at[:, :, cols], out_sem.at[5, slot]),
        )

    def flip_store(k):
        return pltpu.make_async_copy(
            flip_stage.at[k % 2], flipped_gated_out.at[k * HALF : (k + 1) * HALF], out_sem.at[6, k % 2]
        )

    tile = tiles.at[own_at(0)]
    tile[...] = jnp.zeros((8, KEY), f32)
    tile[0:4, 0 : conv_ref.shape[1]] = conv_ref[...].astype(f32)
    tile[4:5, 0 : shift_ref.shape[1]] = shift_ref[...].astype(f32)
    tile[5:6, 0 : gate_ref.shape[1]] = gate_ref[...].astype(f32)
    tile[6:7, 0 : pre_ref.shape[1]] = pre_ref[...].astype(f32)
    tile_copy(0).start()
    heads = dt_ref.shape[1]
    ph_ref[...] = jnp.zeros_like(ph_ref)
    ph_ref[0:1, 0:heads] = dt_ref[...].astype(f32)
    ph_ref[1:2, 0:heads] = log_ref[...].astype(f32)
    ph_ref[2:3, 0:heads] = skip_ref[...].astype(f32)
    live_ref[...] = jnp.where(iota((length, KEY), 0) < lengths_ref[0], 1.0, 0.0).astype(f32)

    held[0, own_at(kind_of(0))] = w_ref[:, 2 * wide : 2 * wide + HALF]
    held[1, own_at(kind_of(1))] = jnp.zeros((rb, HALF), bf16)
    held[1, own_at(kind_of(1)), :, 0:heads] = wd_ref[...]

    def land(u, carry):
        group = pl.ds(pl.multiple_of((u // 2 - 1) * HALF + lax.rem(u, 2) * wide, HALF), HALF)
        held[u, own_at(kind_of(u))] = w_ref[:, group]
        return carry

    lax.fori_loop(2, 2 * n_in, land, 0)
    for u in range(2 * n_out):
        rows = slice(u % 2 * rb, (u % 2 + 1) * rb)
        held[2 * n_in + u, own_at(kind_of(2 * n_in + u))] = wo_ref[rows, u // 2 * HALF : (u // 2 + 1) * HALF]

    def first_chunk():
        lane = iota((8, KEY), 1)
        row = iota((8, KEY), 0)
        order = [tiles[c * 16 + at] for c, at in all_positions(0)]
        conv = spread_lanes(order, (wide + 2 * KEY) // 32, lane, wide // KEY + 2)
        gate = spread_lanes(order, wide // 32, lane, wide // KEY)
        pre = spread_lanes(order, width // 32, lane, width // KEY)
        skips = split(jnp.broadcast_to(ph_ref[2:3], (8, KEY)))
        for k, tile in enumerate(conv):
            cols = slice(k * KEY, (k + 1) * KEY)
            if k < wide // KEY:
                if k % 2 == 0:
                    skip = mm(skips, expander(k // 2))
                skip_part = skip[:, k % 2 * KEY : (k % 2 + 1) * KEY]
                tile = jnp.where(row == 5, gate[k], jnp.where(row == 6, skip_part, tile))
            pv_ref[:, cols] = tile
        for k, tile in enumerate(pre):
            gain[:, k * KEY : (k + 1) * KEY] = tile
        hidden_load.wait()
        for k in range(0, length, KEY):
            values = hidden_ref[k : k + KEY].astype(f32)
            mean = jnp.mean(values * values, axis=1, keepdims=True)
            rows = (values * lax.rsqrt(mean + epsilon) * gain[6:7]).astype(bf16)
            normed[k : k + KEY] = rows
            flipped_ref[:, k : k + KEY] = rows.T
        flipped_store.start()

    def keys_chunk(slot):
        forward_shared(
            proj_stage.at[slot, :, 0:HALF], proj_stage.at[slot, :, HALF : HALF + KEY], pv_ref, wide, ph_ref,
            s_ref, st_ref, hl_ref, ehl_ref, kb_ref, kt_ref, sc_ref, padk,
        )
        pad[0:8] = jnp.zeros((8, GC), f32)
        ssq[...] = jnp.zeros_like(ssq)
        dots[...] = jnp.zeros_like(dots)

    def project(slot):
        for half in range(2):
            cols = slice(half * HALF, (half + 1) * HALF)
            proj_stage[slot, :, cols] = mm(normed[...], w_stage[slot, :, cols])

    def group_chunk(slot, g):
        forward_group(
            g, proj_stage.at[slot, :, 0:HALF], proj_stage.at[slot, :, HALF : 2 * HALF], pv_ref,
            s_ref, st_ref, hl_ref, ehl_ref, kb_ref, kt_ref, sc_ref,
            mixed_stage.at[slot], big, states_stage.at[slot], pad, sg, hcar, ssq,
        )

    def finish_groups():
        mean = jnp.sum(ssq[...], axis=1, keepdims=True) / wide
        r_ref[...] = jnp.broadcast_to(lax.rsqrt(mean + epsilon), r_ref.shape)
        for k in range(wide // HALF):
            if k >= 2:
                flip_store(k - 2).wait()
            for q in range(HALF // KEY):
                cols = slice(k * HALF + q * KEY, k * HALF + (q + 1) * KEY)
                part = (big[:, cols] * r_ref[...] * pv_ref[5:6, cols]).astype(bf16)
                gated[:, cols] = part
                flip_stage[k % 2, q * KEY : (q + 1) * KEY] = part.T
            flip_store(k).start()
        for k in range(wide // HALF - 2, wide // HALF):
            flip_store(k).wait()

    def out_store(j):
        cols = pl.ds(pl.multiple_of(j * HALF, HALF), HALF)
        return pltpu.make_async_copy(out_ref.at[:, cols], out_out.at[:, cols], row_sem.at[3 + j])

    def out_chunk_first(i):
        j = i - n_in

        @pl.when(j == 0)
        def _():
            cot_load.wait()

        side = pl.ds(pl.multiple_of(lax.rem(j, 2) * HALF, HALF), HALF)
        for half in range(2):
            for b, (c, at) in enumerate(all_positions(kind_of(2 * i + half))):
                wo_stage[(2 * b + half) * rb : (2 * b + half + 1) * rb, side] = held[2 * i + half, c * 16 + at]
        cols = pl.ds(pl.multiple_of(j * HALF, HALF), HALF)
        branch = mm(gated[...], wo_stage[:, side])
        live = jnp.concatenate([live_ref[...]] * (HALF // KEY), axis=1)
        out_ref[:, cols] = (hidden_ref[:, cols].astype(f32) + live * branch).astype(bf16)
        out_store(j).start()
        upstream = (cot_ref[:, cols].astype(f32) * live).astype(bf16)
        pull = upstream.astype(f32) * branch
        dots[...] += pull[:, :KEY] + pull[:, KEY:]

    def gg_store(q):
        cols = slice(q, q + 2 * HALF)
        return pltpu.make_async_copy(big.at[:, cols], gg_out.at[:, cols], gg_sem.at[q // (2 * HALF)])

    def out_chunk_second(i):
        j = i - n_in

        @pl.when(lax.rem(j, 2) == 1)
        def _():
            cols = pl.ds(pl.multiple_of((j - 1) * HALF, 2 * HALF), 2 * HALF)
            live = jnp.concatenate([live_ref[...]] * (2 * HALF // KEY), axis=1)
            upstream = (cot_ref[:, cols].astype(f32) * live).astype(bf16)
            for q in range(0, wide, 2 * HALF):
                more = mm_nt(upstream, wo_stage[q : q + 2 * HALF])

                @pl.when(j == 1)
                def _():
                    big[:, q : q + 2 * HALF] = more

                @pl.when(j > 1)
                def _():
                    big[:, q : q + 2 * HALF] += more

                @pl.when(j == n_out - 1)
                def _():
                    gg_store(q).start()

    def consume_first(i):
        slot = lax.rem(i, 2)

        @pl.when(i < n_in)
        def _():
            @pl.when(i >= 2)
            def _():
                for store in weight_stores(i - 2):
                    store.wait()

            for half in range(2):
                for b, (c, at) in enumerate(all_positions(kind_of(2 * i + half))):
                    w_stage[slot, b * rb : (b + 1) * rb, half * HALF : (half + 1) * HALF] = held[
                        2 * i + half, c * 16 + at
                    ]

            @pl.when(i == 0)
            def _():
                first_chunk()

            project(slot)
            for store in weight_stores(i):
                store.start()

        @pl.when(i >= n_in)
        def _():
            out_chunk_first(i)

    def consume_second(i):
        slot = lax.rem(i, 2)

        @pl.when(i == 0)
        def _():
            keys_chunk(slot)

        @pl.when((i > 0) & (i < n_in))
        def _():
            @pl.when(i >= 3)
            def _():
                for store in group_stores(i - 2):
                    store.wait()

            group_chunk(slot, i - 1)
            for store in group_stores(i):
                store.start()

        @pl.when(i == n_in - 1)
        def _():
            finish_groups()

        @pl.when(i >= n_in)
        def _():
            out_chunk_second(i)

    def tick(t, carry):
        @pl.when(t < 2 * n)
        def _():
            copy(0, t).start()

        for stage in range(5):
            u = t - GATHER_WAITS[stage]

            @pl.when(u == 0)
            def _(stage=stage):
                tile_copy(stage).wait()
                if stage < 4:
                    tile_copy(stage + 1).start()

            @pl.when((u >= 0) & (u < 2 * n))
            def _(stage=stage, u=u):
                copy(stage, u).wait()
                if stage < 4:
                    copy(stage + 1, u).start()

        u = t - GATHER_WAITS[4]

        @pl.when((u >= 1) & (lax.rem(u, 2) == 1))
        def _():
            consume_first(u // 2)

        @pl.when((u >= 2) & (lax.rem(u, 2) == 0))
        def _():
            consume_second(u // 2 - 1)

        return carry

    lax.fori_loop(0, 2 * n + GATHER_WAITS[4] + 1, tick, 0)
    pull = jnp.sum(dots[...], axis=1, keepdims=True) / wide
    c_ref[...] = r_ref[...] * r_ref[...] * pull
    for i in (n_in - 2, n_in - 1):
        for store in weight_stores(i) + list(group_stores(i)):
            store.wait()
    for q in range(0, wide, 2 * HALF):
        gg_store(q).wait()
    flipped_store.wait()
    for j in range(n_out):
        out_store(j).wait()


def gather_forward(lengths, hidden, cotangent, shard, dt_shard, out_shard, *vectors):
    length, width = hidden.shape
    rb = shard.shape[0]
    columns = shard.shape[1] + 2 * KEY
    wide = out_shard.shape[0] * 32
    n_in, n_out = columns // (2 * HALF), width // HALF
    blocks = length // BLK
    vmem = pl.BlockSpec(memory_space=pltpu.VMEM)
    anywhere = pl.BlockSpec(memory_space=pl.ANY)
    struct = jax.ShapeDtypeStruct
    shared = [struct(shape, dtype) for shape, dtype in state_specs(length)]
    return pl.pallas_call(
        partial(forward_kernel, n_in, n_out),
        out_shape=[
            struct((width, columns), bf16),
            struct((length, columns), f32),
            struct((length, wide), f32),
            struct((blocks, KEY, wide), bf16),
            struct((wide, length), bf16),
            struct((length, wide), f32),
            struct((length, width), bf16),
            struct((width, length), bf16),
            struct((length, KEY), f32),
            struct((8, KEY), f32),
            struct((8, wide + 2 * KEY), f32),
            struct((8, width), f32),
            struct((length, KEY), f32),
            struct((length, KEY), f32),
        ]
        + shared,
        in_specs=[pl.BlockSpec(memory_space=pltpu.SMEM)] + [anywhere] * 2 + [vmem] * (3 + len(vectors)),
        out_specs=[anywhere] * 8 + [vmem] * (6 + len(shared)),
        scratch_shapes=[
            pltpu.VMEM((2 * (n_in + n_out), 32, rb, HALF), bf16),
            pltpu.VMEM((32, 8, KEY), f32),
            pltpu.VMEM((2, width, 2 * HALF), bf16),
            pltpu.VMEM((wide, 2 * HALF), bf16),
            pltpu.VMEM((2, length, 2 * HALF), f32),
            pltpu.VMEM((2, length, HALF), f32),
            pltpu.VMEM((2, blocks, KEY, HALF), bf16),
            pltpu.VMEM((2, HALF, length), bf16),
            pltpu.VMEM((length, width), bf16),
            pltpu.VMEM((length, wide), bf16),
            pltpu.VMEM((length, wide), f32),
            pltpu.VMEM((length + 8, GC), f32),
            pltpu.VMEM((length + 8, 2 * KEY), f32),
            pltpu.VMEM((length, KEY), f32),
            pltpu.VMEM((KEY, GC), f32),
            pltpu.VMEM((length, KEY), f32),
            pltpu.VMEM((length, KEY), f32),
            pltpu.VMEM((length, width), bf16),
            pltpu.VMEM((length, width), bf16),
            pltpu.VMEM((length, width), bf16),
            pltpu.VMEM((width, length), bf16),
            pltpu.SemaphoreType.DMA((2 * (n_in + n_out), 5)),
            pltpu.SemaphoreType.DMA((2 * (n_in + n_out), 5)),
            pltpu.SemaphoreType.DMA((2, 5)),
            pltpu.SemaphoreType.DMA((7, 2)),
            pltpu.SemaphoreType.DMA((wide // (2 * HALF),)),
            pltpu.SemaphoreType.DMA((3 + n_out,)),
        ],
        compiler_params=pltpu.CompilerParams(
            collective_id=2, has_side_effects=True, vmem_limit_bytes=67043328
        ),
        name="gather_forward",
    )(lengths, hidden, cotangent, shard, dt_shard, out_shard, *vectors)


EARLY = 7


def gather_lanes(row_tiles, width, lane, i):
    at, shift = divmod(i * width, KEY)
    if shift == 0:
        return row_tiles[at]
    first = pltpu.roll(row_tiles[at], KEY - shift, 1)
    if shift + width <= KEY:
        return first
    return jnp.where(lane < KEY - shift, first, pltpu.roll(row_tiles[at + 1], KEY - shift, 1))


def backward_kernel(
    n_in, n_out, live_ref, pv_ref, gain_ref, ph_ref, r_ref, c_ref,
    s_ref, st_ref, hl_ref, ehl_ref, kb_ref, kt_ref, sc_ref,
    hidden_in, cot_in, flipped_in, gated_in, proj_in, mixed_in, gg_in, states_in, w_in,
    rows_out, in_ref, dt_ref, out_ref, tile_out, sums_ref,
    parts, r0, r1, r2, r3, r4, tiles, t0, t1, t2, t3, t4, sums, sums_in,
    stage_in, states_stage, w_stage, keys_stage, dchunk, rows_grad, sv, sv_all, sk, sh, skip_sum, gain_sum,
    pad, padk, dpad, dpadk, sg, dhcar, dsc, dkb, dsrow, dscol, ddt,
    hidden_ref, cot_ref, flipped_ref, gated_ref,
    send, recv, tile_sem, sums_sem, in_sem, out_sem, row_sem,
):
    length, width = hidden_ref.shape
    wide = mixed_in.shape[1]
    rb = in_ref.shape[0]
    n = n_in + n_out
    groups = n_in - 1
    keys_tick = n - 2
    shared = (s_ref, st_ref, hl_ref, ehl_ref, kb_ref, kt_ref, sc_ref)
    gated_load = pltpu.make_async_copy(gated_in, gated_ref, row_sem.at[0])
    cot_load = pltpu.make_async_copy(cot_in, cot_ref, row_sem.at[1])
    flipped_load = pltpu.make_async_copy(flipped_in, flipped_ref, row_sem.at[2])
    hidden_load = pltpu.make_async_copy(hidden_in, hidden_ref, row_sem.at[3])
    for load in (gated_load, cot_load, flipped_load, hidden_load):
        load.start()
    place = places()
    held = (r0, r1, r2, r3, r4)
    tile_source = (tiles, t0, t1, t2, t3, t4)
    greet([exchange(place, 0, stage)[1] for stage in range(5)])

    def is_out(t):
        return ((t < 3 * n_out - 3) & (lax.rem(t, 3) == 0)) | (t == n - 1)

    def out_index(t):
        return jnp.where(t == n - 1, n_out - 1, t // 3)

    def group_index(t):
        return jnp.where(t < 3 * n_out - 3, t // 3 * 2 + lax.rem(t, 3) - 1, t - n_out + 1)

    def loads(g):
        slot = lax.rem(g, 2)
        near = pl.ds(pl.multiple_of(g * HALF, HALF), HALF)
        far = pl.ds(pl.multiple_of(wide + g * HALF, HALF), HALF)
        pairs = (
            (proj_in.at[:, near], stage_in.at[slot, 0]),
            (proj_in.at[:, far], stage_in.at[slot, 1]),
            (mixed_in.at[:, near], stage_in.at[slot, 2]),
            (gg_in.at[:, near], stage_in.at[slot, 3]),
            (states_in.at[:, :, near], states_stage.at[slot]),
        )
        return [pltpu.make_async_copy(a, b, in_sem.at[k, slot]) for k, (a, b) in enumerate(pairs)]

    def weight_loads(g):
        slot = lax.rem(g, 2)
        first = jnp.where(g == groups, 2 * wide, g * HALF)
        second = jnp.where(g == groups, 2 * wide + HALF, wide + g * HALF)
        return [
            pltpu.make_async_copy(
                w_in.at[:, pl.ds(pl.multiple_of(at, HALF), HALF)],
                w_stage.at[slot, :, half * HALF : (half + 1) * HALF],
                in_sem.at[5 + half, slot],
            )
            for half, at in enumerate((first, second))
        ]

    keys_load = pltpu.make_async_copy(proj_in.at[:, 2 * wide : 2 * wide + 3 * KEY], keys_stage, in_sem.at[7, 0])
    for load in loads(0) + weight_loads(0) + [keys_load]:
        load.start()
    rows_store = pltpu.make_async_copy(rows_grad, rows_out, out_sem.at[0])

    def sums_copy(stage):
        return pltpu.make_async_remote_copy(
            src_ref=sums.at[stage],
            dst_ref=sums_in.at[stage],
            send_sem=sums_sem.at[0, stage],
            recv_sem=sums_sem.at[1, stage],
            device_id=exchange(place, 0, stage)[1],
            device_id_type=MESH,
        )

    def tile_copy(stage):
        count = 16 >> stage
        return pltpu.make_async_remote_copy(
            src_ref=tile_source[stage].at[pl.ds((1 - exchange(place, 0, stage)[0]) * count, count)],
            dst_ref=tile_source[stage + 1],
            send_sem=tile_sem.at[0, stage],
            recv_sem=tile_sem.at[1, stage],
            device_id=exchange(place, 0, stage)[1],
            device_id_type=MESH,
        )

    def spot(stage, u):
        return lax.rem(u, 2 * EARLY) if stage == 0 else u

    def copy(stage, u):
        count = 16 >> stage
        side, partner = exchange(place, kind_of(u), stage)
        if stage == 0:
            src = parts.at[lax.rem(u // 2, 2), 1 - side, lax.rem(u, 2)]
        else:
            src = held[stage - 1].at[spot(stage - 1, u), pl.ds((1 - side) * count, count)]
        return pltpu.make_async_remote_copy(
            src_ref=src,
            dst_ref=held[stage].at[spot(stage, u)],
            send_sem=send.at[u, stage],
            recv_sem=recv.at[u, stage],
            device_id=partner,
            device_id_type=MESH,
        )

    backward_start(length, pad, dpad, dsc, dkb, dsrow, dscol, ddt)
    skip_sum[...] = jnp.zeros_like(skip_sum)
    rows_grad[...] = jnp.zeros_like(rows_grad)

    def out_chunk(slot, t):
        j = out_index(t)
        where = [all_positions(kind_of(2 * t + half)) for half in range(2)]
        cols = pl.ds(pl.multiple_of(j * HALF, HALF), HALF)
        live = jnp.concatenate([live_ref[...]] * (HALF // KEY), axis=1)
        upstream = (cot_ref[:, cols].astype(f32) * live).astype(bf16)
        for z in range(4):
            res = mm(gated_ref[z * 16 * rb : (z + 1) * 16 * rb], upstream)
            for b in range(8):
                for half in range(2):
                    c, at = where[half][z * 8 + b]
                    at_row = (2 * b + half) * rb
                    parts[slot, c, half, at] = res[at_row : at_row + rb].astype(bf16)

    def weight_chunk(slot, t, g):
        for load in weight_loads(g):
            load.wait()
        at = lax.rem(g, 2)
        for half in range(2):
            right = dchunk[:, half * HALF : (half + 1) * HALF]
            where = all_positions(kind_of(2 * t + half))
            for z in range(4):
                res = mm(flipped_ref[z * 8 * rb : (z + 1) * 8 * rb], right)
                for b in range(8):
                    c, to = where[z * 8 + b]
                    parts[slot, c, half, to] = res[b * rb : (b + 1) * rb].astype(bf16)
        for k in range(0, width, 512):
            rows_grad[:, k : k + 512] += mm_nt(dchunk[...], w_stage[at, k : k + 512])

    def group_chunk(t):
        g = group_index(t)

        for load in weight_loads(g + 1):
            load.start()

        @pl.when(g + 1 < groups)
        def _():
            for load in loads(g + 1):
                load.start()

        for load in loads(g):
            load.wait()
        at = lax.rem(g, 2)
        backward_group(
            g, stage_in.at[at, 0], stage_in.at[at, 1], stage_in.at[at, 2], stage_in.at[at, 3], states_stage.at[at],
            r_ref, c_ref, pv_ref, shared, dchunk.at[:, 0:HALF], dchunk.at[:, HALF : 2 * HALF], sv,
            pad, dpad, sg, dhcar, dsc, dkb, dsrow, dscol, ddt,
        )

    def group_chunk_end(slot, t):
        g = group_index(t)
        sv_all[:, pl.ds(pl.multiple_of(g * HALF, HALF), HALF)] = sv[...]
        skip_sum[...] += mm_hi(sv[...], reducer(g).astype(f32))
        weight_chunk(slot, t, g)

    def keys_chunk():
        keys_load.wait()
        dchunk[:, 3 * KEY :] = jnp.zeros((length, KEY), bf16)
        backward_shared(
            keys_stage.at[:, 0:HALF], keys_stage.at[:, HALF : HALF + KEY], pv_ref, wide, ph_ref, kb_ref,
            dchunk.at[:, 0:HALF], dchunk.at[:, HALF : HALF + KEY], sk, sh,
            padk, dpadk, dsc, dkb, dsrow, dscol, ddt,
        )

    def keys_chunk_end(slot):
        weight_chunk(slot, keys_tick, groups)
        for half in range(2):
            copy(0, 2 * keys_tick + half).start()
        hidden_load.wait()
        gain = gain_ref[6:7]
        gain_sum[...] = jnp.zeros_like(gain_sum)
        for k in range(0, length, KEY):
            values = hidden_ref[k : k + KEY].astype(f32)
            inverse = lax.rsqrt(jnp.mean(values * values, axis=1, keepdims=True) + epsilon)
            grads = rows_grad[k : k + KEY]
            gain_sum[0:1] += jnp.sum(grads * values * inverse, axis=0, keepdims=True)
            scaled = grads * gain
            pull = jnp.sum(scaled * values, axis=1, keepdims=True) / width
            back = inverse * scaled - values * (inverse * inverse * inverse * pull)
            rows_grad[k : k + KEY] = cot_ref[k : k + KEY].astype(f32) + back
        rows_store.start()
        row = iota((8, KEY), 0)
        lane = iota((8, KEY), 1)
        conv = [sv_all[:, k * KEY : (k + 1) * KEY] for k in range(wide // KEY)]
        gate = conv
        conv = conv + [sk[:, 0:KEY], sk[:, KEY : 2 * KEY]]
        pre = [jnp.broadcast_to(gain_sum[0:1, k * KEY : (k + 1) * KEY], (8, KEY)) for k in range(width // KEY)]
        for i, (c, at) in enumerate(all_positions(0)):
            tile = gather_lanes(conv, (wide + 2 * KEY) // 32, lane, i)
            tile = jnp.where(row == 5, gather_lanes(gate, wide // 32, lane, i), tile)
            tiles[c * 16 + at] = jnp.where(row == 6, gather_lanes(pre, width // 32, lane, i), tile)
        tile_copy(0).start()
        sums[0] = jnp.where(row == 2, skip_sum[6:7], sh[...])
        sums_copy(0).start()

    def write_out(u, value):
        i, half = u // 2, lax.rem(u, 2)

        @pl.when(is_out(i))
        def _():
            cols = pl.ds(pl.multiple_of(out_index(i) * HALF, HALF), HALF)
            out_ref[pl.ds(pl.multiple_of(half * rb, 16), rb), cols] = value

        @pl.when(jnp.logical_not(is_out(i)) & (i != keys_tick))
        def _():
            cols = pl.ds(pl.multiple_of(half * wide + group_index(i) * HALF, HALF), HALF)
            in_ref[:, cols] = value

        @pl.when(u == 2 * keys_tick)
        def _():
            in_ref[:, 2 * wide : 2 * wide + HALF] = value

        @pl.when(u == 2 * keys_tick + 1)
        def _():
            dt_ref[...] = value[:, :KEY]

    def first_step(t):
        @pl.when(jnp.logical_not(is_out(t)) & (t != keys_tick))
        def _():
            group_chunk(t)

        @pl.when(t == keys_tick)
        def _():
            keys_chunk()

    def second_step(t):
        slot = lax.rem(t, 2)

        @pl.when(t >= 2)
        def _():
            for half in range(2):
                copy(0, 2 * (t - 2) + half).wait_send()

        @pl.when(t == 0)
        def _():
            gated_load.wait()
            cot_load.wait()

        @pl.when(t == 1)
        def _():
            flipped_load.wait()

        @pl.when(is_out(t))
        def _():
            out_chunk(slot, t)

        @pl.when(jnp.logical_not(is_out(t)) & (t != keys_tick))
        def _():
            group_chunk_end(slot, t)

        @pl.when(t == keys_tick)
        def _():
            keys_chunk_end(slot)

        @pl.when(t != keys_tick)
        def _():
            for half in range(2):
                copy(0, 2 * t + half).start()

    def tick(step, carry):
        t = step // 2

        @pl.when((t < n) & (lax.rem(step, 2) == 0))
        def _():
            first_step(t)

        @pl.when((t < n) & (lax.rem(step, 2) == 1))
        def _():
            second_step(t)

        for stage in range(5):
            u = step - SCATTER_WAITS[stage]
            count = 16 >> stage

            @pl.when(u == 2 * keys_tick)
            def _(stage=stage, count=count):
                sums_copy(stage).wait()
                tile_copy(stage).wait()
                total = tile_source[stage + 1][...] + tile_source[stage][
                    pl.ds(exchange(place, 0, stage)[0] * count, count)
                ]
                if stage < 4:
                    sums[stage + 1] = sums[stage] + sums_in[stage]
                    sums_copy(stage + 1).start()
                    tile_source[stage + 1][...] = total
                    tile_copy(stage + 1).start()
                else:
                    sums_ref[...] = sums[stage] + sums_in[stage]
                    tile_out[...] = total[0]

            @pl.when((u >= 0) & (u < 2 * n))
            def _(stage=stage, u=u, count=count):
                done = copy(stage, u)
                side, _ = exchange(place, kind_of(u), stage)
                if stage == 0:
                    done.wait_recv()
                    mine = parts[lax.rem(u // 2, 2), side, lax.rem(u, 2)]
                else:
                    done.wait()
                    mine = held[stage - 1][spot(stage - 1, u), pl.ds(side * count, count)]
                if stage < 4:
                    at = spot(stage, u)
                    held[stage][at] = (held[stage][at].astype(f32) + mine.astype(f32)).astype(bf16)
                    copy(stage + 1, u).start()
                else:
                    write_out(u, held[stage][u, 0].astype(f32) + mine[0].astype(f32))

        return carry

    lax.fori_loop(0, 2 * n + SCATTER_WAITS[4], tick, 0)
    for u in range(2 * n - 4, 2 * n):
        copy(0, u).wait_send()
    rows_store.wait()


def backward_scatter(
    hidden, cotangent, live, flipped, gated_flipped, pv, gains, ph, inverse, pull, shared,
    projected, mixed, grad_gated, states, w_in, rb,
):
    length, width = hidden.shape
    columns = projected.shape[1]
    wide = mixed.shape[1]
    n_in, n_out = columns // (2 * HALF), width // HALF
    n = n_in + n_out
    blocks = length // BLK
    vmem = pl.BlockSpec(memory_space=pltpu.VMEM)
    anywhere = pl.BlockSpec(memory_space=pl.ANY)
    struct = jax.ShapeDtypeStruct
    return pl.pallas_call(
        partial(backward_kernel, n_in, n_out),
        out_shape=[
            struct((length, width), f32),
            struct((rb, columns - 2 * KEY), f32),
            struct((rb, KEY), f32),
            struct((2 * rb, width), f32),
            struct((8, KEY), f32),
            struct((8, KEY), f32),
        ],
        in_specs=[vmem] * 13 + [anywhere] * 9,
        out_specs=[anywhere] + [vmem] * 5,
        scratch_shapes=[pltpu.VMEM((2, 2, 2, 16, rb, HALF), bf16)]
        + [pltpu.VMEM((2 * (n if stage else EARLY), 16 >> stage, rb, HALF), bf16) for stage in range(5)]
        + [pltpu.VMEM((32 >> stage, 8, KEY), f32) for stage in range(6)]
        + [pltpu.VMEM((5, 8, KEY), f32)] * 2
        + [
            pltpu.VMEM((2, 4, length, HALF), f32),
            pltpu.VMEM((2, blocks, KEY, HALF), bf16),
            pltpu.VMEM((2, width, 2 * HALF), bf16),
            pltpu.VMEM((length, 3 * KEY), f32),
            pltpu.VMEM((length, 2 * HALF), bf16),
            pltpu.VMEM((length, width), f32),
            pltpu.VMEM((8, HALF), f32),
            pltpu.VMEM((8, wide), f32),
            pltpu.VMEM((8, HALF), f32),
            pltpu.VMEM((8, KEY), f32),
            pltpu.VMEM((8, KEY), f32),
            pltpu.VMEM((8, width), f32),
        ]
        + backward_scratch(length)
        + [
            pltpu.VMEM((length, width), bf16),
            pltpu.VMEM((length, width), bf16),
            pltpu.VMEM((width, length), bf16),
            pltpu.VMEM((wide, length), bf16),
        ]
        + [pltpu.SemaphoreType.DMA((2 * n, 5))] * 2
        + [pltpu.SemaphoreType.DMA((2, 5))] * 2
        + [pltpu.SemaphoreType.DMA((8, 2)), pltpu.SemaphoreType.DMA((1,)), pltpu.SemaphoreType.DMA((4,))],
        compiler_params=pltpu.CompilerParams(
            collective_id=1, has_side_effects=True, vmem_limit_bytes=67043328
        ),
        name="backward_scatter",
    )(
        live, pv, gains, ph, inverse, pull, *shared,
        hidden, cotangent, flipped, gated_flipped, projected, mixed, grad_gated, states, w_in,
    )


PIECE = 512


def finish_kernel(tile_ref, sums_ref, dt_in, *refs):
    big_in, refs = refs[:4], refs[4:]
    big_out, (pre_ref, dt_ref, conv_ref, shift_ref, bias_ref, log_ref, skip_ref, gate_ref) = refs[:4], refs[4:12]
    stages, (sem,) = refs[12:16], refs[16:]
    reads, writes = [], []
    for a, s, b in zip(big_in, stages, big_out):
        for at in range(0, a.shape[0], PIECE):
            rows = slice(at, min(at + PIECE, a.shape[0]))
            k = len(reads)
            reads.append(pltpu.make_async_copy(a.at[rows], s.at[rows], sem.at[0, k]))
            writes.append(pltpu.make_async_copy(s.at[rows], b.at[rows], sem.at[1, k]))
    for read in reads:
        read.start()
    pre_ref[...] = tile_ref[6:7, 0 : pre_ref.shape[1]]
    dt_ref[...] = dt_in[:, 0 : dt_ref.shape[1]]
    conv_ref[...] = tile_ref[0:4, 0 : conv_ref.shape[1]]
    shift_ref[...] = tile_ref[4:5, 0 : shift_ref.shape[1]]
    gate_ref[...] = tile_ref[5:6, 0 : gate_ref.shape[1]]
    for k, ref in enumerate((bias_ref, log_ref, skip_ref)):
        ref[...] = sums_ref[k : k + 1, 0 : ref.shape[1]]
    for read, write in zip(reads, writes):
        read.wait()
        write.start()
    for write in writes:
        write.wait()


def finish(tile, sums, grad_dt, arrays, small_shapes):
    vmem = pl.BlockSpec(memory_space=pltpu.VMEM)
    anywhere = pl.BlockSpec(memory_space=pl.ANY)
    return pl.pallas_call(
        finish_kernel,
        out_shape=[jax.ShapeDtypeStruct(a.shape, a.dtype) for a in arrays]
        + [jax.ShapeDtypeStruct(shape, f32) for shape in small_shapes],
        in_specs=[vmem] * 3 + [anywhere] * 4,
        out_specs=[anywhere] * 4 + [vmem] * 8,
        scratch_shapes=[pltpu.VMEM(a.shape, a.dtype) for a in arrays] + [
            pltpu.SemaphoreType.DMA((2, sum(-(-a.shape[0] // PIECE) for a in arrays)))
        ],
        name="finish",
    )(tile, sums, grad_dt, *arrays)


def pre_norm_inverse(rows):
    return lax.rsqrt(jnp.mean(rows * rows, axis=1, keepdims=True) + epsilon)


AXES = ("dp", "fsdp")


def gather_rows(shard):
    return lax.all_gather(shard, AXES, axis=0, tiled=True)


def scatter_rows(whole):
    return lax.psum_scatter(whole, AXES, scatter_dimension=0, tiled=True)


def vector_tile(conv_weight, conv_bias, gate_gain, norm_gain):
    rows = [conv_weight, conv_bias[None], gate_gain[None], norm_gain[None]]
    rows = [jnp.pad(row.astype(f32), ((0, 0), (0, KEY - row.shape[1]))) for row in rows]
    return jnp.concatenate(rows + [jnp.zeros((1, KEY), f32)], axis=0)


def vector_tiles(conv, gate, pre, parts):
    rows = []
    for whole in (conv, gate, pre):
        part = whole.shape[1] // parts
        split_up = jnp.transpose(whole.reshape(-1, parts, part), (1, 0, 2))
        rows.append(jnp.pad(split_up, ((0, 0), (0, 0), (0, KEY - part))))
    return jnp.concatenate(rows + [jnp.zeros((parts, 1, KEY), f32)], axis=1)


def shards(
    kernels, hidden, cotangent, lengths, norm_gain, in_proj, dt_proj, conv_weight, conv_bias,
    dt_bias, a_log, skip_gain, gate_gain, out_proj,
):
    length, width = hidden.shape
    assert lengths.shape[0] == 1
    rows_in, columns = in_proj.shape
    heads = dt_bias.shape[0]
    parts = width // rows_in
    taps, conv_part = conv_weight.shape
    gate_part = gate_gain.shape[0]
    wide = gate_part * parts
    total = columns + 2 * KEY

    if kernels:
        rows = lambda *vectors: [v.reshape(1, -1) for v in vectors]
        (
            w_in, projected, mixed, states, gated_flipped, grad_gated, output, flipped, live, ph, pv, gains, inverse_two,
            pull, *shared,
        ) = gather_forward(
            lengths, hidden, cotangent, in_proj, dt_proj, out_proj, conv_weight,
            *rows(conv_bias, gate_gain, norm_gain, dt_bias, a_log, skip_gain),
        )
        input_grad, grad_in, grad_dt, grad_out, small_sum, head_sums = backward_scatter(
            hidden, cotangent, live, flipped, gated_flipped, pv, gains, ph,
            inverse_two, pull, shared, projected, mixed, grad_gated, states, w_in, rows_in,
        )
        output, input_grad, grad_in, grad_out, *small = finish(
            small_sum, head_sums, grad_dt, (output, input_grad, grad_in, grad_out),
            ((1, rows_in), (rows_in, heads), (taps, conv_part), (1, conv_part))
            + ((1, heads),) * 3 + ((1, gate_part),),
        )
        pre, dt, conv, shift, bias, log, skip, gate = small
        return (
            output, input_grad, pre[0], grad_in, dt, conv, shift[0], bias[0], log[0], skip[0], gate[0], grad_out
        )

    fill = jnp.zeros((rows_in, total - columns - heads), bf16)
    packed = jnp.concatenate([in_proj, dt_proj, fill], axis=1)
    tile = vector_tile(conv_weight, conv_bias, gate_gain, norm_gain)
    ph = jnp.pad(jnp.stack([dt_bias, a_log]).astype(f32), ((0, 6), (0, KEY - heads)))
    skip_wide = jnp.repeat(skip_gain.astype(f32), HD)[None]
    live = (jnp.arange(length) < lengths[0]).astype(f32)[:, None]
    rows_wide = hidden.astype(f32)
    cot_wide = cotangent.astype(f32)
    upstream = (cot_wide * live).astype(bf16)
    inverse_one = pre_norm_inverse(rows_wide)
    w_in, w_out = gather_rows(packed), gather_rows(out_proj)
    tiles = gather_rows(tile[None])
    whole = lambda rows, part: jnp.transpose(tiles[:, rows, :part], (1, 0, 2)).reshape(-1, parts * part)
    conv_all = whole(slice(0, 5), conv_part)
    gain_two = whole(slice(5, 6), gate_part)
    gain_one = whole(slice(6, 7), rows_in)[0]
    rest = jnp.concatenate([gain_two, skip_wide, jnp.zeros((1, wide), f32)], axis=0)
    pv = jnp.concatenate([conv_all, jnp.pad(rest, ((0, 0), (0, 2 * KEY)))], axis=0)
    normed = (rows_wide * inverse_one * gain_one[None, :]).astype(bf16)
    projected = mm(normed, w_in)
    mixed, product, states, inverse_two, *shared = mixer_forward(projected, pv, ph)
    inv = inverse_two[:, :1]
    gated = (product * inv * gain_two).astype(bf16)
    output = (rows_wide + live * mm(gated, w_out)).astype(bf16)
    grad_gated = mm_nt(upstream, w_out)
    pull = jnp.sum(grad_gated * gain_two * product, axis=1, keepdims=True)
    pull = jnp.broadcast_to(inv * inv * inv * pull / wide, inverse_two.shape)
    grad_out = mm_tn(gated, upstream)
    grad_proj, sums_v, sums_k, sums_h = mixer_backward(
        projected, pv, ph, mixed, grad_gated, states, inverse_two, pull, shared
    )
    skip_grad = jnp.pad(jnp.sum(sums_v[6].reshape(heads, HD), axis=1), (0, KEY - heads))[None]
    head_grads = jnp.concatenate([sums_h[:2], skip_grad, jnp.zeros((5, KEY), f32)], axis=0)

    grad_normed = mm_nt(grad_proj, w_in)
    scaled = grad_normed * gain_one[None, :]
    row_sums = jnp.sum(scaled * rows_wide, axis=1, keepdims=True) / width
    grad_rows = inverse_one * scaled - rows_wide * (inverse_one * inverse_one * inverse_one * row_sums)
    input_grad = cot_wide + grad_rows
    grad_gain_one = jnp.sum(grad_normed * rows_wide * inverse_one, axis=0, keepdims=True)

    conv_grad = jnp.concatenate([sums_v[:5], sums_k[:5]], axis=1)
    small = vector_tiles(conv_grad, sums_v[5:6], grad_gain_one, parts)
    grad_out = scatter_rows(grad_out.astype(bf16)).astype(f32)
    head_sums = lax.psum(head_grads, AXES)
    grad_all = scatter_rows(mm_tn(normed, grad_proj).astype(bf16)).astype(f32)
    grad_in, grad_dt = grad_all[:, :columns], grad_all[:, columns:]
    small_sum = scatter_rows(small)[0]
    return (
        output,
        input_grad,
        small_sum[6, :rows_in],
        grad_in,
        grad_dt[:, :heads],
        small_sum[:taps, :conv_part],
        small_sum[taps, :conv_part],
        head_sums[0, :heads],
        head_sums[1, :heads],
        head_sums[2, :heads],
        small_sum[5, :gate_part],
        grad_out,
    )


def solution(mesh):
    rows = P(AXES, None)
    vector = P(AXES)
    last = P(None, AXES)
    return jax.shard_map(
        partial(shards, mesh.shape["dp"] == 8 and mesh.shape["fsdp"] == 4),
        mesh=mesh,
        in_specs=(rows, rows, vector, vector, rows, rows, last, vector, P(), P(), P(), vector, rows),
        out_specs=(rows, rows, vector, rows, rows, last, vector, P(), P(), P(), vector, rows),
        check_vma=False,
    )
```
